128 devices in a mesh: row: 16 (over z, x), col: 8 (over y, core).
Axes of the slice: x: 4, y: 4, z: 4, core: 2. Of those that a mesh axis runs over, the one named last changes fastest.
Arguments:
- src_points: float32 [64, 16384], P(None, ('row', 'col')), as said below
- tgt_points: float32 [64, 32768], P(None, ('col', 'row')), as said below
- log_a: float32 [16384], P('row'), may hold values from -5 to 5
- log_b: float32 [32768], P('col'), may hold values from -5 to 5
- g_current: float32 [32768], P(('col', 'row')), may hold values from -4 to 4
- hist_g: float32 [4, 32768], P(None, ('col', 'row')), may hold values from -4 to 4
- hist_maps: float32 [4, 32768], P(None, ('col', 'row')), may hold values from -4 to 4
Outputs:
- f_out: float32 [16384], P('row')
- g_out: float32 [32768], P(('col', 'row'))
The draws below stay inside these ranges and needn't reach their ends.
Inputs may be any that keep to these rules, and one draw needn't show every extreme that they name: `src_points`: coordinates of the source points. `tgt_points`: coordinates of the target points.
All inputs are finite; a program needn't handle non-finite values.
Results may differ from the reference program's by a relative error of at most 0.0003.
Values sent between devices are 32-bit elements; how exact they have to be, the bound alone decides.
A program may use at most 64 MiB of HBM per device.

```python
import math
import jax
import jax.numpy as jnp
from jax import lax

D = 64
HIST = 5
ITERS = 2
N = 16384
M = 32768


def target_cloud(key):
    base = jax.random.normal(jax.random.fold_in(key, 7), (D, M), jnp.float32)
    return base * 0.15


def draw_tgt_points(key, part):
    return target_cloud(key)


def draw_src_points(key, part):
    base = jax.random.normal(jax.random.fold_in(key, 3), (D, N), jnp.float32)
    return base * 0.15


def level_of(rng, dims, pieces, smallest, top_value):
    factor_of = 1.0
    for axis_at, shards_of in pieces:
        draws = jax.random.uniform(jax.random.fold_in(jax.random.fold_in(rng, 6), axis_at), (shards_of,), jnp.float32, smallest / len(pieces), top_value / len(pieces))
        factor_of = factor_of * jnp.repeat(jnp.exp(draws), dims[axis_at] // shards_of).reshape((-1,) + (1,) * (len(dims) - 1 - axis_at))
    return factor_of


def bell_draw(own_key, shape, width, limit, cuts=(), kind=jnp.bfloat16):
    values = width * jax.random.normal(own_key, shape, jnp.float32)
    if cuts:
        values = values * level_of(own_key, shape, cuts, -0.22, 0.18)
    return jnp.clip(values, -limit, limit).astype(kind)


def setup_inputs(seed: int = 0) -> dict:
    keys = jax.random.split(jax.random.key(seed), 8)
    src_points = draw_src_points(jax.random.fold_in(keys[7], 71), 0)
    tgt_points = draw_tgt_points(jax.random.fold_in(keys[7], 71), 0)
    log_a = bell_draw(keys[2], (N,), 1.0, 5.0, ((0, 16),), jnp.float32)
    log_b = bell_draw(keys[3], (M,), 1.0, 5.0, ((0, 8),), jnp.float32)
    g_current = bell_draw(keys[4], (M,), 0.3, 4.0, ((0, 128),), jnp.float32)
    hist_g = bell_draw(keys[5], (HIST - 1, M), 0.3, 4.0, ((1, 128),), jnp.float32)
    hist_maps = bell_draw(keys[6], (HIST - 1, M), 0.3, 4.0, ((1, 128),), jnp.float32)
    return dict(src_points=src_points, tgt_points=tgt_points, log_a=log_a, log_b=log_b, g_current=g_current, hist_g=hist_g, hist_maps=hist_maps)


EPS = 0.1


def cost_of(source, source_sq, target, target_sq):
    cross = lax.dot_general(source, target, (((0,), (0,)), ((), ())), precision=lax.Precision.HIGHEST, preferred_element_type=jnp.float32)
    return source_sq[:, None] + target_sq[None, :] - 2.0 * cross


def solve_small(matrix, rhs):
    extent = matrix.shape[0]
    rows_list = [matrix[k] for k in range(extent)]
    values = [rhs[k] for k in range(extent)]
    for pivot_index in range(extent):
        for lower_row in range(pivot_index + 1, extent):
            factor = rows_list[lower_row][pivot_index] / rows_list[pivot_index][pivot_index]
            rows_list[lower_row] = rows_list[lower_row] - factor * rows_list[pivot_index]
            values[lower_row] = values[lower_row] - factor * values[pivot_index]
    answer = [None] * extent
    for pivot_index in reversed(range(extent)):
        running = values[pivot_index]
        for upper_col in range(pivot_index + 1, extent):
            running = running - rows_list[pivot_index][upper_col] * answer[upper_col]
        answer[pivot_index] = running / rows_list[pivot_index][pivot_index]
    return jnp.stack(answer)


def mix_weights(gram):
    extent = gram.shape[0]
    shift = 0.001 * jnp.trace(gram) / extent + 1e-6
    system = gram + shift * jnp.eye(extent, dtype=jnp.float32)
    weights = solve_small(system, jnp.ones((extent,), jnp.float32))
    return weights / jnp.sum(weights)


def reference(src_points, tgt_points, log_a, log_b, g_current, hist_g, hist_maps):
    source_sq = jnp.sum(src_points * src_points, axis=0)
    target_sq = jnp.sum(tgt_points * tgt_points, axis=0)
    total_rows = src_points.shape[1]
    total_cols = tgt_points.shape[1]
    row_block = math.gcd(total_rows, 1024)
    col_block = math.gcd(total_cols, 1024)

    def row_potential(g_whole):
        column_term = g_whole / EPS + log_b

        def one_block(index):
            start = (index * row_block).astype(jnp.int32)
            source = lax.dynamic_slice_in_dim(src_points, start, row_block, 1)
            sq_piece = lax.dynamic_slice_in_dim(source_sq, start, row_block, 0)
            scores = column_term[None, :] - cost_of(source, sq_piece, tgt_points, target_sq) / EPS
            top = jnp.max(scores, axis=1)
            return -EPS * (top + jnp.log(jnp.sum(jnp.exp(scores - top[:, None]), axis=1)))

        return lax.map(one_block, jnp.arange(total_rows // row_block, dtype=jnp.int32)).reshape(-1)

    def column_potential(f_whole):
        row_term = f_whole / EPS + log_a

        def one_block(index):
            start = (index * col_block).astype(jnp.int32)
            target = lax.dynamic_slice_in_dim(tgt_points, start, col_block, 1)
            sq_piece = lax.dynamic_slice_in_dim(target_sq, start, col_block, 0)
            scores = row_term[:, None] - cost_of(src_points, source_sq, target, sq_piece) / EPS
            top = jnp.max(scores, axis=0)
            return -EPS * (top + jnp.log(jnp.sum(jnp.exp(scores - top[None, :]), axis=0)))

        return lax.map(one_block, jnp.arange(total_cols // col_block, dtype=jnp.int32)).reshape(-1)

    potentials = [hist_g[k] for k in range(hist_g.shape[0])]
    images = [hist_maps[k] for k in range(hist_maps.shape[0])]
    g_whole = g_current
    f_whole = None
    for turn_index in range(ITERS):
        f_whole = row_potential(g_whole)
        mapped = column_potential(f_whole)
        potentials = (potentials + [g_whole])[-HIST:]
        images = (images + [mapped])[-HIST:]
        image_stack = jnp.stack(images)
        resid = image_stack - jnp.stack(potentials)
        gram = jnp.dot(resid, resid.T, precision=lax.Precision.HIGHEST, preferred_element_type=jnp.float32)
        mix = mix_weights(gram)
        g_whole = jnp.dot(mix, image_stack, precision=lax.Precision.HIGHEST, preferred_element_type=jnp.float32)
    return f_whole, g_whole
```

```python
import functools

import jax
import jax.numpy as jnp
from jax import lax
from jax.experimental import pallas as pl
from jax.experimental.pallas import tpu as pltpu
from jax.sharding import Mesh
from jax.sharding import PartitionSpec as P

HIST = 5
ITERS = 2
EPS = 0.1
LOG2E = 1.4426950408889634
BITS = LOG2E / EPS
NATS = EPS / LOG2E
MESH = pl.DeviceIdType.MESH
AXES = ("z", "x", "y", "core")


def split2(v):
    hi = v.astype(jnp.bfloat16).astype(jnp.float32)
    return hi, v - hi


def split3(v):
    hi = v.astype(jnp.bfloat16).astype(jnp.float32)
    rest = v - hi
    mid = rest.astype(jnp.bfloat16).astype(jnp.float32)
    return hi, mid, rest - mid


def placed(rows, values, width):
    at = lax.broadcasted_iota(jnp.int32, (rows, width), 0)
    out = jnp.zeros((rows, width), jnp.float32)
    for k, v in enumerate(values):
        out = jnp.where(at == k, v, out)
    return out


def gray(k):
    return k + (k // 2) * (5 - 2 * k)


def solve(gram):
    n = HIST
    trace = gram[0, 0]
    for k in range(1, n):
        trace = trace + gram[k, k]
    shift = 0.001 * trace / n + 1e-6
    a = [[gram[min(p, q), max(p, q)] + (shift if p == q else 0.0) for q in range(n)] for p in range(n)]
    rhs = [jnp.ones((1, 1), jnp.float32) for _ in range(n)]
    for p in range(n):
        for low in range(p + 1, n):
            factor = a[low][p] / a[p][p]
            for q in range(p + 1, n):
                a[low][q] = a[low][q] - factor * a[p][q]
            rhs[low] = rhs[low] - factor * rhs[p]
    out = [None] * n
    for p in reversed(range(n)):
        acc = rhs[p]
        for q in range(p + 1, n):
            acc = acc - a[p][q] * out[q]
        out[p] = acc / a[p][p]
    total = out[0]
    for k in range(1, n):
        total = total + out[k]
    return [o / total for o in out]


def kernel(
    dims,
    src_ref, tgt_ref, loga_ref, logb_ref, g_ref, hg_ref, hm_ref,
    f_ref, gout_ref,
    tgt_all, src_all, lhs, zs, mrep, sacc, bias, delta,
    f_buf, c_send, c_buf, m_buf, r_buf,
    tgt_send, tgt_recv, src_send, src_recv, f_sems, c_sems, m_sems, r_sems,
):
    NZ, NX, NY, NC = dims
    NR, NK = NZ * NX, NY * NC
    D, SW = src_ref.shape
    TW = tgt_ref.shape[1]
    ROWS = NK * SW
    z, x = lax.axis_index("z"), lax.axis_index("x")
    y, core = lax.axis_index("y"), lax.axis_index("core")
    row, col = z * NX + x, y * NC + core

    def row_peer(k):
        p = lax.rem(row + k, NR)
        return {"z": p // NX, "x": lax.rem(p, NX)}

    def col_peer(k):
        p = lax.rem(col + k, NK)
        return {"y": p // NC, "core": lax.rem(p, NC)}

    def to_all(peer, count, src, dst, ssem, rsem):
        def one(k, carry):
            pltpu.make_async_remote_copy(
                src_ref=src(k), dst_ref=dst, send_sem=ssem, recv_sem=rsem,
                device_id=peer(k), device_id_type=MESH,
            ).start()
            return carry
        lax.fori_loop(1, count, one, 0)

    def wait_bytes(buf, count, sem):
        part = buf.at[pl.ds(0, count)]
        pltpu.make_async_copy(part, part, sem).wait()

    mine = tgt_all.at[row]
    mine[0:D, :] = tgt_ref[...]
    mine[D:D + 8, :] = placed(8, [g_ref[...]] + [hm_ref[k:k + 1, :] for k in range(HIST - 1)], TW)
    src_all[col] = src_ref[...]

    barrier = pltpu.get_barrier_semaphore()

    def greet(peer):
        def one(k, carry):
            pl.semaphore_signal(barrier, inc=1, device_id=peer(k), device_id_type=MESH)
            return carry
        return one
    lax.fori_loop(1, NR, greet(row_peer), 0)
    lax.fori_loop(1, NK, greet(col_peer), 0)
    pl.semaphore_wait(barrier, NR + NK - 2)

    to_all(col_peer, NK, lambda k: src_all.at[col], src_all.at[col], src_send, src_recv)
    to_all(row_peer, NR, lambda k: tgt_all.at[row], tgt_all.at[row], tgt_send, tgt_recv.at[row])

    wait_bytes(src_all, NK - 1, src_recv)

    def left(b, carry):
        v = src_all[b]
        norm = jnp.sum(v * v, axis=0, keepdims=True) * (-BITS)
        hi, lo = split2(v * (2.0 * BITS))
        one = jnp.ones((1, SW), jnp.float32)
        tail = placed(D, list(split3(norm)) + [one] * 6, SW)
        full = jnp.concatenate([hi, hi, lo, tail], axis=0)
        lhs[pl.ds(pl.multiple_of(b * SW, SW), SW), :] = full.T.astype(jnp.bfloat16)
        return carry
    lax.fori_loop(0, NK, left, 0)

    mrep[...] = jnp.full(mrep.shape, -jnp.inf, jnp.float32)

    def chunk(k, carry):
        pz = lax.rem(z + gray(k // NX), NZ) if NZ == 4 else lax.rem(z + k // NX, NZ)
        px = lax.rem(x + gray(lax.rem(k, NX)), NX) if NX == 4 else lax.rem(x + lax.rem(k, NX), NX)
        r = pz * NX + px

        @pl.when(k > 0)
        def _():
            part = tgt_all.at[r]
            pltpu.make_async_copy(part, part, tgt_recv.at[r]).wait()
        v = tgt_all[r, 0:D, :]
        norm = jnp.sum(v * v, axis=0, keepdims=True) * (-BITS)
        b = tgt_all[r, D:D + 1, :] * BITS + logb_ref[r] * LOG2E
        bias[r] = b
        hi, lo = split2(v)
        one = jnp.ones((1, TW), jnp.float32)
        tail = placed(D, [one] * 3 + list(split3(norm)) + list(split3(b)), TW)
        rhs = jnp.concatenate([hi, lo, hi, tail], axis=0).astype(jnp.bfloat16)

        def rows_of(i, c2):
            rows = pl.ds(pl.multiple_of(i * 128, 128), 128)
            t = jnp.dot(lhs[rows, :], rhs, preferred_element_type=jnp.float32)
            zs[r, rows, :] = t
            top = mrep[rows, :]
            for q in range(0, TW, 128):
                top = jnp.maximum(top, t[:, q:q + 128])
            mrep[rows, :] = top
            return c2
        lax.fori_loop(0, ROWS // 128, rows_of, 0)
        return carry
    lax.fori_loop(0, NR, chunk, 0)

    RB = 32
    diag = (lax.broadcasted_iota(jnp.int32, (128, 128), 0) == lax.broadcasted_iota(jnp.int32, (128, 128), 1))

    for it in range(ITERS):
        last = it == ITERS - 1

        def term(r):
            return delta[r] if it else None

        if it:
            def top_of(i, carry):
                rows = pl.ds(pl.multiple_of(i * RB, RB), RB)
                top = jnp.full((RB, 128), -jnp.inf, jnp.float32)
                for r in range(NR):
                    v = zs[r, rows, :] + delta[r]
                    for q in range(0, TW, 128):
                        top = jnp.maximum(top, v[:, q:q + 128])
                mrep[rows, :] = top
                return carry
            lax.fori_loop(0, ROWS // RB, top_of, 0)

        def sum_of(i, carry):
            rows = pl.ds(pl.multiple_of(i * RB, RB), RB)
            top = jnp.max(mrep[rows, :], axis=1, keepdims=True)
            acc = jnp.zeros((RB, 128), jnp.float32)
            for r in range(NR):
                v = zs[r, rows, :]
                if it:
                    v = v + delta[r]
                e = jnp.exp2(v - top)
                for q in range(0, TW, 128):
                    acc = acc + e[:, q:q + 128]
            mrep[rows, :] = jnp.broadcast_to(top, (RB, 128))
            sacc[rows, :] = acc
            return carry
        lax.fori_loop(0, ROWS // RB, sum_of, 0)

        packed = []
        for t in range(ROWS // 128):
            rows = slice(t * 128, (t + 1) * 128)
            s = jnp.sum(sacc[rows, :], axis=1, keepdims=True)
            part = mrep[rows, :] + jnp.log2(s)
            packed.append(jnp.sum(jnp.where(diag, part, 0.0), axis=0, keepdims=True))
        f_buf[it, col] = jnp.concatenate(packed, axis=0)
        to_all(col_peer, NK, lambda k: f_buf.at[it, col], f_buf.at[it, col], f_sems.at[it, 0], f_sems.at[it, 1])
        wait_bytes(f_buf.at[it], NK - 1, f_sems.at[it, 1])
        parts = f_buf[it]
        top = jnp.max(parts, axis=0)
        whole = top + jnp.log2(jnp.sum(jnp.exp2(parts - top[None]), axis=0))
        if last:
            f_ref[...] = whole * (-NATS)
        term_rows = loga_ref[...] * LOG2E - whole
        for t in range(ROWS // 128):
            v = jnp.where(diag, term_rows[t:t + 1, :], 0.0)
            s = jnp.sum(v, axis=1, keepdims=True)
            mrep[t * 128:(t + 1) * 128, :] = jnp.broadcast_to(s, (128, 128))

        def column(r, carry):
            def tops(i, acc):
                rows = pl.ds(pl.multiple_of(i * 128, 128), 128)
                f = mrep[rows, :]
                out = []
                for n, q in enumerate(range(0, TW, 128)):
                    v = zs[r, rows, q:q + 128] + f
                    out.append(jnp.maximum(acc[n], jnp.max(v.reshape(16, 8, 128), axis=0)))
                return tuple(out)
            low = tuple(jnp.full((8, 128), -jnp.inf, jnp.float32) for _ in range(0, TW, 128))
            tops_ = lax.fori_loop(0, ROWS // 128, tops, low)
            tops_ = [jnp.max(t, axis=0, keepdims=True) for t in tops_]

            def sums(i, acc):
                rows = pl.ds(pl.multiple_of(i * 128, 128), 128)
                f = mrep[rows, :]
                out = []
                for n, q in enumerate(range(0, TW, 128)):
                    v = jnp.exp2((zs[r, rows, q:q + 128] + f) - tops_[n])
                    out.append(acc[n] + jnp.sum(v.reshape(16, 8, 128), axis=0))
                return tuple(out)
            none = tuple(jnp.zeros((8, 128), jnp.float32) for _ in range(0, TW, 128))
            sums_ = lax.fori_loop(0, ROWS // 128, sums, none)
            sums_ = [jnp.sum(s, axis=0, keepdims=True) for s in sums_]
            val = jnp.concatenate([t + jnp.log2(s) for t, s in zip(tops_, sums_)], axis=1)
            c_send[it, r] = val - bias[r]
            return carry
        lax.fori_loop(0, NR, column, 0)
        c_buf[it, row] = c_send[it, row]
        to_all(
            row_peer, NR, lambda k: c_send.at[it, lax.rem(row + k, NR)], c_buf.at[it, row],
            c_sems.at[it, 0], c_sems.at[it, 1],
        )
        wait_bytes(c_buf.at[it], NR - 1, c_sems.at[it, 1])
        top = c_buf[it, 0]
        for r in range(1, NR):
            top = jnp.maximum(top, c_buf[it, r])
        tot = jnp.exp2(c_buf[it, 0] - top)
        for r in range(1, NR):
            tot = tot + jnp.exp2(c_buf[it, r] - top)
        mapped = (top + jnp.log2(tot)) * (-NATS)

        if it == 0:
            images = [hm_ref[k:k + 1, :] for k in range(HIST - 1)] + [mapped]
            base = [hg_ref[k:k + 1, :] for k in range(HIST - 1)] + [g_ref[...]]
        else:
            images = images[1:] + [mapped]
            base = base[1:] + [g_own]
        resid = placed(8, [p - q for p, q in zip(images, base)], TW)
        lane = lax.broadcasted_iota(jnp.int32, (8, 128), 1)
        sub = lax.broadcasted_iota(jnp.int32, (8, 128), 0)
        flat = jnp.zeros((8, 128), jnp.float32)
        for b in range(HIST):
            prod = jnp.sum(resid * resid[b:b + 1, :], axis=1, keepdims=True)
            flat = jnp.where(lane == sub * 8 + b, prod, flat)
        flat = jnp.sum(flat, axis=0, keepdims=True)
        m_buf[it, row, :, 0:TW] = mapped
        m_buf[it, row, :, TW:TW + 128] = flat
        to_all(row_peer, NR, lambda k: m_buf.at[it, row], m_buf.at[it, row], m_sems.at[it, 0], m_sems.at[it, 1])
        wait_bytes(m_buf.at[it], NR - 1, m_sems.at[it, 1])
        flat = m_buf[it, 0, :, TW:TW + 128]
        for r in range(1, NR):
            flat = flat + m_buf[it, r, :, TW:TW + 128]
        r_buf[it, col] = flat
        to_all(col_peer, NK, lambda k: r_buf.at[it, col], r_buf.at[it, col], r_sems.at[it, 0], r_sems.at[it, 1])
        wait_bytes(r_buf.at[it], NK - 1, r_sems.at[it, 1])
        flat = r_buf[it, 0]
        for b in range(1, NK):
            flat = flat + r_buf[it, b]
        line = lax.broadcasted_iota(jnp.int32, (1, 128), 1)
        gram = {
            (a, b): jnp.sum(jnp.where(line == a * 8 + b, flat, 0.0), axis=1, keepdims=True)
            for a in range(HIST) for b in range(a, HIST)
        }
        mix = solve(gram)
        g_own = images[0] * mix[0]
        for k in range(1, HIST):
            g_own = g_own + images[k] * mix[k]
        if last:
            gout_ref[...] = g_own
        else:
            def renew(r, carry):
                acc = m_buf[it, r, :, 0:TW] * mix[HIST - 1]
                for k in range(HIST - 1):
                    acc = acc + tgt_all[r, D + 1 + k:D + 2 + k, :] * mix[k]
                b = acc * BITS + logb_ref[r] * LOG2E
                delta[r] = b - bias[r]
                return carry
            lax.fori_loop(0, NR, renew, 0)

    wait_bytes(src_all, NK - 1, src_send)
    wait_bytes(tgt_all, NR - 1, tgt_send)
    for it in range(ITERS):
        wait_bytes(f_buf.at[it], NK - 1, f_sems.at[it, 0])
        wait_bytes(c_buf.at[it], NR - 1, c_sems.at[it, 0])
        wait_bytes(m_buf.at[it], NR - 1, m_sems.at[it, 0])
        wait_bytes(r_buf.at[it], NK - 1, r_sems.at[it, 0])


def shards(dims, src, tgt, log_a, log_b, g, hist_g, hist_maps):
    NZ, NX, NY, NC = dims
    NR, NK = NZ * NX, NY * NC
    D, SW = src.shape
    TW = tgt.shape[1]
    ROWS = NK * SW
    f32 = jnp.float32
    vmem = pl.BlockSpec(memory_space=pltpu.VMEM)
    dma = pltpu.SemaphoreType.DMA
    f, gout = pl.pallas_call(
        functools.partial(kernel, dims),
        out_shape=(
            jax.ShapeDtypeStruct((ROWS // 128, 128), f32),
            jax.ShapeDtypeStruct((1, TW), f32),
        ),
        in_specs=[vmem] * 7,
        out_specs=(vmem, vmem),
        scratch_shapes=[
            pltpu.VMEM((NR, D + 8, TW), f32),
            pltpu.VMEM((NK, D, SW), f32),
            pltpu.VMEM((ROWS, 4 * D), jnp.bfloat16),
            pltpu.VMEM((NR, ROWS, TW), f32),
            pltpu.VMEM((ROWS, 128), f32),
            pltpu.VMEM((ROWS, 128), f32),
            pltpu.VMEM((NR, 1, TW), f32),
            pltpu.VMEM((NR, 1, TW), f32),
            pltpu.VMEM((ITERS, NK, ROWS // 128, 128), f32),
            pltpu.VMEM((ITERS, NR, 1, TW), f32),
            pltpu.VMEM((ITERS, NR, 1, TW), f32),
            pltpu.VMEM((ITERS, NR, 1, TW + 128), f32),
            pltpu.VMEM((ITERS, NK, 1, 128), f32),
            dma, dma((NR,)), dma, dma,
            dma((ITERS, 2)), dma((ITERS, 2)), dma((ITERS, 2)), dma((ITERS, 2)),
        ],
        compiler_params=pltpu.CompilerParams(
            collective_id=0, has_side_effects=True, vmem_limit_bytes=48 * 1024 * 1024
        ),
        name="sinkhorn",
    )(src, tgt, log_a.reshape(ROWS // 128, 128), log_b.reshape(NR, 1, TW), g.reshape(1, TW), hist_g, hist_maps)
    return f.reshape(-1), gout.reshape(-1)


def solution(mesh, dims=(4, 4, 4, 2)):
    grid = Mesh(mesh.devices.reshape(dims), AXES)
    in_specs = (
        P(None, AXES),
        P(None, ("y", "core", "z", "x")),
        P(("z", "x")),
        P(("y", "core")),
        P(("y", "core", "z", "x")),
        P(None, ("y", "core", "z", "x")),
        P(None, ("y", "core", "z", "x")),
    )
    out_specs = (P(("z", "x")), P(("y", "core", "z", "x")))
    return jax.shard_map(
        functools.partial(shards, dims), mesh=grid, in_specs=in_specs, out_specs=out_specs, check_vma=False
    )
```

```python
import functools

import jax
import jax.numpy as jnp
from jax import lax
from jax.experimental import pallas as pl
from jax.experimental.pallas import tpu as pltpu
from jax.sharding import Mesh
from jax.sharding import PartitionSpec as P

HIST = 5
ITERS = 2
EPS = 0.1
LOG2E = 1.4426950408889634
BITS = LOG2E / EPS
NATS = EPS / LOG2E
MESH = pl.DeviceIdType.MESH
AXES = ("z", "x", "y", "core")


def split2(v):
    hi = v.astype(jnp.bfloat16).astype(jnp.float32)
    return hi, v - hi


def split3(v):
    hi = v.astype(jnp.bfloat16).astype(jnp.float32)
    rest = v - hi
    mid = rest.astype(jnp.bfloat16).astype(jnp.float32)
    return hi, mid, rest - mid


def placed(rows, values, width):
    at = lax.broadcasted_iota(jnp.int32, (rows, width), 0)
    out = jnp.zeros((rows, width), jnp.float32)
    for k, v in enumerate(values):
        out = jnp.where(at == k, v, out)
    return out


def gray(k):
    return k + (k // 2) * (5 - 2 * k)


def solve(gram):
    n = HIST
    trace = gram[0, 0]
    for k in range(1, n):
        trace = trace + gram[k, k]
    shift = 0.001 * trace / n + 1e-6
    a = [[gram[min(p, q), max(p, q)] + (shift if p == q else 0.0) for q in range(n)] for p in range(n)]
    rhs = [jnp.ones((1, 1), jnp.float32) for _ in range(n)]
    for p in range(n):
        for low in range(p + 1, n):
            factor = a[low][p] / a[p][p]
            for q in range(p + 1, n):
                a[low][q] = a[low][q] - factor * a[p][q]
            rhs[low] = rhs[low] - factor * rhs[p]
    out = [None] * n
    for p in reversed(range(n)):
        acc = rhs[p]
        for q in range(p + 1, n):
            acc = acc - a[p][q] * out[q]
        out[p] = acc / a[p][p]
    total = out[0]
    for k in range(1, n):
        total = total + out[k]
    return [o / total for o in out]


def kernel(
    dims,
    src_hbm, tgt_hbm, loga_hbm, logb_hbm, g_hbm, hg_hbm, hm_hbm,
    f_ref, gout_ref,
    tgt_all, src_all, g_in, hm_in, loga_ref, logb_ref, hg_ref,
    lhs, zs, mrep, sacc, bias, delta,
    f_buf, c_send, c_buf, m_buf, r_buf,
    in_sems, tgt_send, tgt_recv, src_send, src_recv, f_sems, c_sems, m_sems, r_sems,
):
    NZ, NX, NY, NC = dims
    SIZE = dict(zip(AXES, dims))
    NR, NK = NZ * NX, NY * NC
    D, SW = src_hbm.shape
    TW = tgt_hbm.shape[1]
    ROWS = NK * SW
    at = {name: lax.axis_index(name) for name in AXES}
    z, x, y, core = (at[name] for name in AXES)
    row, col = z * NX + x, y * NC + core

    def row_peer(k):
        p = lax.rem(row + k, NR)
        return {"z": p // NX, "x": lax.rem(p, NX)}

    def col_peer(k):
        p = lax.rem(col + k, NK)
        return {"y": p // NC, "core": lax.rem(p, NC)}

    def near(axis, d):
        return {axis: lax.rem(at[axis] + d + SIZE[axis], SIZE[axis])}

    def remote(src, dst, ssem, rsem, peer):
        pltpu.make_async_remote_copy(
            src_ref=src, dst_ref=dst, send_sem=ssem, recv_sem=rsem, device_id=peer, device_id_type=MESH
        ).start()

    def to_all(peer, count, src, dst, ssem, rsem):
        def one(k, carry):
            remote(src(k), dst, ssem, rsem, peer(k))
            return carry
        lax.fori_loop(1, count, one, 0)

    def wait_bytes(buf, count, sem):
        if count:
            part = buf.at[pl.ds(0, count)]
            pltpu.make_async_copy(part, part, sem).wait()

    def wait_for(part, sem):
        pltpu.make_async_copy(part, part, sem).wait()

    barrier = pltpu.get_barrier_semaphore()
    around = [(name, d) for name in ("x", "z", "y") if SIZE[name] > 1 for d in (1, -1)]
    if NC > 1:
        around.append(("core", 1))
    for name, d in around:
        pl.semaphore_signal(barrier, inc=1, device_id=near(name, d), device_id_type=MESH)

    moves = [
        (tgt_hbm, tgt_all.at[row, pl.ds(0, D)]), (src_hbm, src_all.at[col]), (g_hbm, g_in), (logb_hbm, logb_ref),
        (loga_hbm, loga_ref), (hm_hbm, hm_in), (hg_hbm, hg_ref),
    ]
    moves = [pltpu.make_async_copy(s, d, in_sems.at[k]) for k, (s, d) in enumerate(moves)]
    for m in moves:
        m.start()
    mrep[...] = jnp.full(mrep.shape, -jnp.inf, jnp.float32)
    for m in moves:
        m.wait()
    tgt_all[row, D:D + 8, :] = placed(8, [g_in[...]] + [hm_in[k:k + 1, :] for k in range(HIST - 1)], TW)
    pl.semaphore_wait(barrier, len(around))

    HALF = D // 2
    QUART = D // 4
    EXTRA = 8
    PIECES = {
        (0, None): (0, HALF), (0, 0): (0, QUART), (0, 1): (QUART, QUART),
        (1, None): (HALF, HALF + EXTRA), (1, 0): (HALF, QUART + EXTRA), (1, 1): (HALF + QUART + EXTRA, QUART),
    }
    ORDER = (("x", "z"), ("z", "x"))

    def slot(h, da, db):
        a, b = ORDER[h]
        d = {a: da, b: db}
        return lax.rem(z + d["z"] + NZ, NZ) * NX + lax.rem(x + d["x"] + NX, NX)

    def piece(r, h, sub=None):
        start, count = PIECES[h, sub]
        return tgt_all.at[r, pl.ds(start, count)]

    def pass_on(r, h, sub, axis, d):
        part = piece(r, h, sub)
        remote(part, part, tgt_send, tgt_recv.at[h, r], near(axis, d))

    def arrived(h, da, db):
        a, b = ORDER[h]
        if (da and SIZE[a] == 1) or (db and SIZE[b] == 1):
            return
        r = slot(h, da, db)
        if da or db:
            wait_for(piece(r, h), tgt_recv.at[h, r])
        if db == 0:
            if da == 0 and SIZE[a] > 1:
                for d in (1, -1):
                    pass_on(r, h, None, a, d)
            elif da in (1, -1):
                pass_on(r, h, 0 if da < 0 else 1, a, -da)
            if SIZE[b] > 1:
                for d in (1, -1):
                    pass_on(r, h, None, b, d)
        elif db in (1, -1):
            pass_on(r, h, 0 if db < 0 else 1, b, -db)

    def source(c, sub=None):
        if sub is None:
            return src_all.at[c]
        return src_all.at[c, pl.ds(sub * HALF, HALF)]

    def src_slot(dy, other=0):
        return lax.rem(y + dy + NY, NY) * NC + lax.rem(core + other, NC)

    def src_pass(c, sub, axis, d):
        part = source(c, sub)
        remote(part, part, src_send, src_recv.at[c], near(axis, d))

    def src_arrived(dy):
        if dy and NY == 1:
            return
        c = src_slot(dy)
        if dy:
            wait_for(source(c), src_recv.at[c])
        if dy == 0 and NY > 1:
            for d in (1, -1):
                src_pass(c, None, "y", d)
        elif dy in (1, -1):
            src_pass(c, 0 if dy < 0 else 1, "y", -dy)
        if NC > 1:
            src_pass(c, None, "core", 1)

    def left(b):
        v = src_all[b]
        norm = jnp.sum(v * v, axis=0, keepdims=True) * (-BITS)
        hi, lo = split2(v * (2.0 * BITS))
        one = jnp.ones((1, SW), jnp.float32)
        tail = placed(D, list(split3(norm)) + [one] * 6, SW)
        full = jnp.concatenate([hi, hi, lo, tail], axis=0)
        lhs[pl.ds(pl.multiple_of(b * SW, SW), SW), :] = full.T.astype(jnp.bfloat16)

    MB = min(256, ROWS)

    def chunk(r):
        v = tgt_all[r, 0:D, :]
        norm = jnp.sum(v * v, axis=0, keepdims=True) * (-BITS)
        b = tgt_all[r, D:D + 1, :] * BITS + logb_ref[r] * LOG2E
        bias[r] = b
        hi, lo = split2(v)
        one = jnp.ones((1, TW), jnp.float32)
        tail = placed(D, [one] * 3 + list(split3(norm)) + list(split3(b)), TW)
        rhs = jnp.concatenate([hi, lo, hi, tail], axis=0).astype(jnp.bfloat16)

        def rows_of(i, c2):
            rows = pl.ds(pl.multiple_of(i * MB, MB), MB)
            t = jnp.dot(lhs[rows, :], rhs, preferred_element_type=jnp.float32)
            zs[r, rows, :] = t
            top = mrep[rows, :]
            for q in range(0, TW, 128):
                top = jnp.maximum(top, t[:, q:q + 128])
            mrep[rows, :] = top
            return c2
        lax.fori_loop(0, ROWS // MB, rows_of, 0)

    def chunks(count, offset):
        def one(k, carry):
            dz, dx = offset(k)
            chunk(lax.rem(z + dz + NZ, NZ) * NX + lax.rem(x + dx + NX, NX))
            return carry
        lax.fori_loop(0, count, one, 0)

    both = NZ > 1 and NX > 1
    for h in (0, 1):
        arrived(h, 0, 0)
    src_arrived(0)
    left(col)
    for dy in (1, -1):
        src_arrived(dy)
    for h in (0, 1):
        for da in (1, -1):
            arrived(h, da, 0)
    for h in (0, 1):
        for db in (1, -1):
            arrived(h, 0, db)
    src_arrived(2)
    if NY > 1:
        for dy in (1, -1, 2):
            left(src_slot(dy))
    for h in (0, 1):
        arrived(h, 2, 0)
        for da in (1, -1):
            for db in (1, -1):
                arrived(h, da, db)
    if NC > 1:
        for dy in ((0, 1, -1, 2) if NY > 1 else (0,)):
            c = src_slot(dy, 1)
            wait_for(source(c), src_recv.at[c])
            left(c)

    def first(k):
        i = jnp.maximum(k - 1, 0)
        s = (1 - 2 * lax.rem(i, 2)) * jnp.minimum(k, 1)
        return s * (i // 2), s * (1 - i // 2)
    if both:
        chunks(5, first)
    elif NZ > 1:
        chunks(3, lambda k: (lax.rem(k + 1, 3) - 1, 0))
    elif NX > 1:
        chunks(3, lambda k: (0, lax.rem(k + 1, 3) - 1))
    else:
        chunks(1, lambda k: (0, 0))
    for h in (0, 1):
        for db in (1, -1):
            arrived(h, 2, db)
        arrived(h, 0, 2)
    if both:
        chunks(4, lambda k: (1 - 2 * (k // 2), 1 - 2 * lax.rem(k, 2)))
        chunks(2, lambda k: (2 * k, 2 - 2 * k))
    elif NZ > 1:
        chunks(1, lambda k: (2, 0))
    elif NX > 1:
        chunks(1, lambda k: (0, 2))
    for h in (0, 1):
        for da in (1, -1, 2):
            arrived(h, da, 2)
    if both:
        chunks(2, lambda k: (2, 1 - 2 * k))
        chunks(2, lambda k: (1 - 2 * k, 2))
        chunks(1, lambda k: (2, 2))

    def lane_tops():
        for t in range(ROWS // 128):
            rows = slice(t * 128, (t + 1) * 128)
            mrep[rows, :] = jnp.broadcast_to(jnp.max(mrep[rows, :], axis=1, keepdims=True), (128, 128))

    RB = 32
    diag = (lax.broadcasted_iota(jnp.int32, (128, 128), 0) == lax.broadcasted_iota(jnp.int32, (128, 128), 1))

    for it in range(ITERS):
        last = it == ITERS - 1

        def term(r):
            return delta[r] if it else None

        if it:
            def top_of(i, carry):
                rows = pl.ds(pl.multiple_of(i * RB, RB), RB)
                top = jnp.full((RB, 128), -jnp.inf, jnp.float32)
                for r in range(NR):
                    v = zs[r, rows, :] + delta[r]
                    for q in range(0, TW, 128):
                        top = jnp.maximum(top, v[:, q:q + 128])
                mrep[rows, :] = top
                return carry
            lax.fori_loop(0, ROWS // RB, top_of, 0)
        lane_tops()

        def sum_of(i, carry):
            rows = pl.ds(pl.multiple_of(i * RB, RB), RB)
            top = mrep[rows, :]
            acc = jnp.zeros((RB, 128), jnp.float32)
            for r in range(NR):
                v = zs[r, rows, :]
                if it:
                    v = v + delta[r]
                for q in range(0, TW, 128):
                    acc = acc + jnp.exp2(v[:, q:q + 128] - top)
            sacc[rows, :] = acc
            return carry
        lax.fori_loop(0, ROWS // RB, sum_of, 0)

        packed = []
        for t in range(ROWS // 128):
            rows = slice(t * 128, (t + 1) * 128)
            s = jnp.sum(sacc[rows, :], axis=1, keepdims=True)
            part = mrep[rows, :] + jnp.log2(s)
            packed.append(jnp.sum(jnp.where(diag, part, 0.0), axis=0, keepdims=True))
        f_buf[it, col] = jnp.concatenate(packed, axis=0)
        to_all(col_peer, NK, lambda k: f_buf.at[it, col], f_buf.at[it, col], f_sems.at[it, 0], f_sems.at[it, 1])
        wait_bytes(f_buf.at[it], NK - 1, f_sems.at[it, 1])
        parts = f_buf[it]
        top = jnp.max(parts, axis=0)
        whole = top + jnp.log2(jnp.sum(jnp.exp2(parts - top[None]), axis=0))
        if last:
            f_ref[...] = whole * (-NATS)
        term_rows = loga_ref[...] * LOG2E - whole
        for t in range(ROWS // 128):
            v = jnp.where(diag, term_rows[t:t + 1, :], 0.0)
            s = jnp.sum(v, axis=1, keepdims=True)
            mrep[t * 128:(t + 1) * 128, :] = jnp.broadcast_to(s, (128, 128))

        def column(r, carry):
            def tops(i, acc):
                rows = pl.ds(pl.multiple_of(i * 128, 128), 128)
                f = mrep[rows, :]
                out = []
                for n, q in enumerate(range(0, TW, 128)):
                    v = zs[r, rows, q:q + 128] + f
                    out.append(jnp.maximum(acc[n], jnp.max(v.reshape(16, 8, 128), axis=0)))
                return tuple(out)
            low = tuple(jnp.full((8, 128), -jnp.inf, jnp.float32) for _ in range(0, TW, 128))
            tops_ = lax.fori_loop(0, ROWS // 128, tops, low)
            tops_ = [jnp.max(t, axis=0, keepdims=True) for t in tops_]

            def sums(i, acc):
                rows = pl.ds(pl.multiple_of(i * 128, 128), 128)
                f = mrep[rows, :]
                out = []
                for n, q in enumerate(range(0, TW, 128)):
                    v = jnp.exp2((zs[r, rows, q:q + 128] + f) - tops_[n])
                    out.append(acc[n] + jnp.sum(v.reshape(16, 8, 128), axis=0))
                return tuple(out)
            none = tuple(jnp.zeros((8, 128), jnp.float32) for _ in range(0, TW, 128))
            sums_ = lax.fori_loop(0, ROWS // 128, sums, none)
            sums_ = [jnp.sum(s, axis=0, keepdims=True) for s in sums_]
            val = jnp.concatenate([t + jnp.log2(s) for t, s in zip(tops_, sums_)], axis=1)
            c_send[it, r] = val - bias[r]
            return carry
        lax.fori_loop(0, NR, column, 0)
        c_buf[it, row] = c_send[it, row]
        to_all(
            row_peer, NR, lambda k: c_send.at[it, lax.rem(row + k, NR)], c_buf.at[it, row],
            c_sems.at[it, 0], c_sems.at[it, 1],
        )
        wait_bytes(c_buf.at[it], NR - 1, c_sems.at[it, 1])
        top = c_buf[it, 0]
        for r in range(1, NR):
            top = jnp.maximum(top, c_buf[it, r])
        tot = jnp.exp2(c_buf[it, 0] - top)
        for r in range(1, NR):
            tot = tot + jnp.exp2(c_buf[it, r] - top)
        mapped = (top + jnp.log2(tot)) * (-NATS)

        if it == 0:
            images = [hm_in[k:k + 1, :] for k in range(HIST - 1)] + [mapped]
            base = [hg_ref[k:k + 1, :] for k in range(HIST - 1)] + [g_in[...]]
        else:
            images = images[1:] + [mapped]
            base = base[1:] + [g_own]
        resid = placed(8, [p - q for p, q in zip(images, base)], TW)
        lane = lax.broadcasted_iota(jnp.int32, (8, 128), 1)
        sub = lax.broadcasted_iota(jnp.int32, (8, 128), 0)
        flat = jnp.zeros((8, 128), jnp.float32)
        for b in range(HIST):
            prod = jnp.sum(resid * resid[b:b + 1, :], axis=1, keepdims=True)
            flat = jnp.where(lane == sub * 8 + b, prod, flat)
        flat = jnp.sum(flat, axis=0, keepdims=True)
        m_buf[it, row, :, 0:TW] = mapped
        m_buf[it, row, :, TW:TW + 128] = flat
        to_all(row_peer, NR, lambda k: m_buf.at[it, row], m_buf.at[it, row], m_sems.at[it, 0], m_sems.at[it, 1])
        wait_bytes(m_buf.at[it], NR - 1, m_sems.at[it, 1])
        flat = m_buf[it, 0, :, TW:TW + 128]
        for r in range(1, NR):
            flat = flat + m_buf[it, r, :, TW:TW + 128]
        r_buf[it, col] = flat
        to_all(col_peer, NK, lambda k: r_buf.at[it, col], r_buf.at[it, col], r_sems.at[it, 0], r_sems.at[it, 1])
        wait_bytes(r_buf.at[it], NK - 1, r_sems.at[it, 1])
        flat = r_buf[it, 0]
        for b in range(1, NK):
            flat = flat + r_buf[it, b]
        line = lax.broadcasted_iota(jnp.int32, (1, 128), 1)
        gram = {
            (a, b): jnp.sum(jnp.where(line == a * 8 + b, flat, 0.0), axis=1, keepdims=True)
            for a in range(HIST) for b in range(a, HIST)
        }
        mix = solve(gram)
        g_own = images[0] * mix[0]
        for k in range(1, HIST):
            g_own = g_own + images[k] * mix[k]
        if last:
            gout_ref[...] = g_own
        else:
            def renew(r, carry):
                acc = m_buf[it, r, :, 0:TW] * mix[HIST - 1]
                for k in range(HIST - 1):
                    acc = acc + tgt_all[r, D + 1 + k:D + 2 + k, :] * mix[k]
                b = acc * BITS + logb_ref[r] * LOG2E
                delta[r] = b - bias[r]
                return carry
            lax.fori_loop(0, NR, renew, 0)

    wait_bytes(src_all, NK - 1, src_send)
    wait_bytes(tgt_all, NR - 1, tgt_send)
    for it in range(ITERS):
        wait_bytes(f_buf.at[it], NK - 1, f_sems.at[it, 0])
        wait_bytes(c_buf.at[it], NR - 1, c_sems.at[it, 0])
        wait_bytes(m_buf.at[it], NR - 1, m_sems.at[it, 0])
        wait_bytes(r_buf.at[it], NK - 1, r_sems.at[it, 0])


def shards(dims, src, tgt, log_a, log_b, g, hist_g, hist_maps):
    NZ, NX, NY, NC = dims
    NR, NK = NZ * NX, NY * NC
    D, SW = src.shape
    TW = tgt.shape[1]
    ROWS = NK * SW
    f32 = jnp.float32
    vmem = pl.BlockSpec(memory_space=pltpu.VMEM)
    dma = pltpu.SemaphoreType.DMA
    f, gout = pl.pallas_call(
        functools.partial(kernel, dims),
        out_shape=(
            jax.ShapeDtypeStruct((ROWS // 128, 128), f32),
            jax.ShapeDtypeStruct((1, TW), f32),
        ),
        in_specs=[pl.BlockSpec(memory_space=pltpu.HBM)] * 7,
        out_specs=(vmem, vmem),
        scratch_shapes=[
            pltpu.VMEM((NR, D + 8, TW), f32),
            pltpu.VMEM((NK, D, SW), f32),
            pltpu.VMEM((1, TW), f32),
            pltpu.VMEM((HIST - 1, TW), f32),
            pltpu.VMEM((ROWS // 128, 128), f32),
            pltpu.VMEM((NR, 1, TW), f32),
            pltpu.VMEM((HIST - 1, TW), f32),
            pltpu.VMEM((ROWS, 4 * D), jnp.bfloat16),
            pltpu.VMEM((NR, ROWS, TW), f32),
            pltpu.VMEM((ROWS, 128), f32),
            pltpu.VMEM((ROWS, 128), f32),
            pltpu.VMEM((NR, 1, TW), f32),
            pltpu.VMEM((NR, 1, TW), f32),
            pltpu.VMEM((ITERS, NK, ROWS // 128, 128), f32),
            pltpu.VMEM((ITERS, NR, 1, TW), f32),
            pltpu.VMEM((ITERS, NR, 1, TW), f32),
            pltpu.VMEM((ITERS, NR, 1, TW + 128), f32),
            pltpu.VMEM((ITERS, NK, 1, 128), f32),
            dma((7,)), dma, dma((2, NR)), dma, dma((NK,)),
            dma((ITERS, 2)), dma((ITERS, 2)), dma((ITERS, 2)), dma((ITERS, 2)),
        ],
        compiler_params=pltpu.CompilerParams(
            collective_id=0, has_side_effects=True, vmem_limit_bytes=48 * 1024 * 1024
        ),
        name="sinkhorn",
    )(src, tgt, log_a.reshape(ROWS // 128, 128), log_b.reshape(NR, 1, TW), g.reshape(1, TW), hist_g, hist_maps)
    return f.reshape(-1), gout.reshape(-1)


def solution(mesh, dims=(4, 4, 4, 2)):
    grid = Mesh(mesh.devices.reshape(dims), AXES)
    in_specs = (
        P(None, AXES),
        P(None, ("y", "core", "z", "x")),
        P(("z", "x")),
        P(("y", "core")),
        P(("y", "core", "z", "x")),
        P(None, ("y", "core", "z", "x")),
        P(None, ("y", "core", "z", "x")),
    )
    out_specs = (P(("z", "x")), P(("y", "core", "z", "x")))
    return jax.shard_map(
        functools.partial(shards, dims), mesh=grid, in_specs=in_specs, out_specs=out_specs, check_vma=False
    )
```

```python
import functools

import jax
import jax.numpy as jnp
from jax import lax
from jax.experimental import pallas as pl
from jax.experimental.pallas import tpu as pltpu
from jax.sharding import Mesh
from jax.sharding import PartitionSpec as P

HIST = 5
ITERS = 2
EPS = 0.1
LOG2E = 1.4426950408889634
BITS = LOG2E / EPS
NATS = EPS / LOG2E
FLAG_LANE = 63
LEAST_BITS = -88.0
SMALLEST = 2.0**LEAST_BITS
MESH = pl.DeviceIdType.MESH
AXES = ("z", "x", "y", "core")


def split2(v):
    hi = v.astype(jnp.bfloat16).astype(jnp.float32)
    return hi, v - hi


def split3(v):
    hi = v.astype(jnp.bfloat16).astype(jnp.float32)
    rest = v - hi
    mid = rest.astype(jnp.bfloat16).astype(jnp.float32)
    return hi, mid, rest - mid


def placed(rows, values, width):
    at = lax.broadcasted_iota(jnp.int32, (rows, width), 0)
    out = jnp.zeros((rows, width), jnp.float32)
    for k, v in enumerate(values):
        out = jnp.where(at == k, v, out)
    return out


def gray(k):
    return k + (k // 2) * (5 - 2 * k)


def solve(gram):
    n = HIST
    trace = gram[0, 0]
    for k in range(1, n):
        trace = trace + gram[k, k]
    shift = 0.001 * trace / n + 1e-6
    a = [[gram[min(p, q), max(p, q)] + (shift if p == q else 0.0) for q in range(n)] for p in range(n)]
    rhs = [jnp.ones((1, 1), jnp.float32) for _ in range(n)]
    for p in range(n):
        for low in range(p + 1, n):
            factor = a[low][p] / a[p][p]
            for q in range(p + 1, n):
                a[low][q] = a[low][q] - factor * a[p][q]
            rhs[low] = rhs[low] - factor * rhs[p]
    out = [None] * n
    for p in reversed(range(n)):
        acc = rhs[p]
        for q in range(p + 1, n):
            acc = acc - a[p][q] * out[q]
        out[p] = acc / a[p][p]
    total = out[0]
    for k in range(1, n):
        total = total + out[k]
    return [o / total for o in out]


def kernel(
    fast, dims,
    src_hbm, tgt_hbm, loga_hbm, logb_hbm, g_hbm, hg_hbm, hm_hbm,
    f_ref, gout_ref, flag_ref,
    tgt_all, src_all, g_in, hm_in, loga_ref, logb_ref, hg_ref,
    lhs, zs, mrep, sacc, m_rows, bias, delta,
    f_buf, c_send, c_buf, m_buf, r_buf,
    in_sems, tgt_send, tgt_recv, src_send, src_recv, f_sems, c_sems, m_sems, r_sems,
):
    NZ, NX, NY, NC = dims
    SIZE = dict(zip(AXES, dims))
    NR, NK = NZ * NX, NY * NC
    D, SW = src_hbm.shape
    TW = tgt_hbm.shape[1]
    ROWS = NK * SW
    at = {name: lax.axis_index(name) for name in AXES}
    z, x, y, core = (at[name] for name in AXES)
    row, col = z * NX + x, y * NC + core

    def row_peer(k):
        p = lax.rem(row + k, NR)
        return {"z": p // NX, "x": lax.rem(p, NX)}

    def col_peer(k):
        p = lax.rem(col + k, NK)
        return {"y": p // NC, "core": lax.rem(p, NC)}

    def near(axis, d):
        return {axis: lax.rem(at[axis] + d + SIZE[axis], SIZE[axis])}

    def remote(src, dst, ssem, rsem, peer):
        pltpu.make_async_remote_copy(
            src_ref=src, dst_ref=dst, send_sem=ssem, recv_sem=rsem, device_id=peer, device_id_type=MESH
        ).start()

    def to_all(peer, count, src, dst, ssem, rsem):
        def one(k, carry):
            remote(src(k), dst, ssem, rsem, peer(k))
            return carry
        lax.fori_loop(1, count, one, 0)

    def wait_bytes(buf, count, sem):
        if count:
            part = buf.at[pl.ds(0, count)]
            pltpu.make_async_copy(part, part, sem).wait()

    def wait_for(part, sem):
        pltpu.make_async_copy(part, part, sem).wait()

    barrier = pltpu.get_barrier_semaphore()
    around = [(name, d) for name in ("x", "z", "y") if SIZE[name] > 1 for d in (1, -1)]
    if NC > 1:
        around.append(("core", 1))
    for name, d in around:
        pl.semaphore_signal(barrier, inc=1, device_id=near(name, d), device_id_type=MESH)

    moves = [
        (tgt_hbm, tgt_all.at[row, pl.ds(0, D)]), (src_hbm, src_all.at[col]), (g_hbm, g_in), (logb_hbm, logb_ref),
        (loga_hbm, loga_ref), (hm_hbm, hm_in), (hg_hbm, hg_ref),
    ]
    moves = [pltpu.make_async_copy(s, d, in_sems.at[k]) for k, (s, d) in enumerate(moves)]
    for m in moves:
        m.start()
    mrep[...] = jnp.full(mrep.shape, -jnp.inf, jnp.float32)
    for m in moves:
        m.wait()
    tgt_all[row, D:D + 8, :] = placed(8, [g_in[...]] + [hm_in[k:k + 1, :] for k in range(HIST - 1)], TW)
    pl.semaphore_wait(barrier, len(around))

    HALF = D // 2
    QUART = D // 4
    EXTRA = 8
    PIECES = {
        (0, None): (0, HALF), (0, 0): (0, QUART), (0, 1): (QUART, QUART),
        (1, None): (HALF, HALF + EXTRA), (1, 0): (HALF, QUART + EXTRA), (1, 1): (HALF + QUART + EXTRA, QUART),
    }
    ORDER = (("x", "z"), ("z", "x"))

    def slot(h, da, db):
        a, b = ORDER[h]
        d = {a: da, b: db}
        return lax.rem(z + d["z"] + NZ, NZ) * NX + lax.rem(x + d["x"] + NX, NX)

    def piece(r, h, sub=None):
        start, count = PIECES[h, sub]
        return tgt_all.at[r, pl.ds(start, count)]

    def pass_on(r, h, sub, axis, d):
        part = piece(r, h, sub)
        remote(part, part, tgt_send, tgt_recv.at[h, r], near(axis, d))

    def arrived(h, da, db):
        a, b = ORDER[h]
        if (da and SIZE[a] == 1) or (db and SIZE[b] == 1):
            return
        r = slot(h, da, db)
        if da or db:
            wait_for(piece(r, h), tgt_recv.at[h, r])
        if db == 0:
            if da == 0 and SIZE[a] > 1:
                for d in (1, -1):
                    pass_on(r, h, None, a, d)
            elif da in (1, -1):
                pass_on(r, h, 0 if da < 0 else 1, a, -da)
            if SIZE[b] > 1:
                for d in (1, -1):
                    pass_on(r, h, None, b, d)
        elif db in (1, -1):
            pass_on(r, h, 0 if db < 0 else 1, b, -db)

    def source(c, sub=None):
        if sub is None:
            return src_all.at[c]
        return src_all.at[c, pl.ds(sub * HALF, HALF)]

    def src_slot(dy, other=0):
        return lax.rem(y + dy + NY, NY) * NC + lax.rem(core + other, NC)

    def src_pass(c, sub, axis, d):
        part = source(c, sub)
        remote(part, part, src_send, src_recv.at[c], near(axis, d))

    def src_arrived(dy):
        if dy and NY == 1:
            return
        c = src_slot(dy)
        if dy:
            wait_for(source(c), src_recv.at[c])
        if dy == 0 and NY > 1:
            for d in (1, -1):
                src_pass(c, None, "y", d)
        elif dy in (1, -1):
            src_pass(c, 0 if dy < 0 else 1, "y", -dy)
        if NC > 1:
            src_pass(c, None, "core", 1)

    def left(b):
        v = src_all[b]
        norm = jnp.sum(v * v, axis=0, keepdims=True) * (-BITS)
        hi, lo = split2(v * (2.0 * BITS))
        one = jnp.ones((1, SW), jnp.float32)
        tail = placed(D, list(split3(norm)) + [one] * 6, SW)
        full = jnp.concatenate([hi, hi, lo, tail], axis=0)
        lhs[pl.ds(pl.multiple_of(b * SW, SW), SW), :] = full.T.astype(jnp.bfloat16)

    def right(r):
        v = tgt_all[r, 0:D, :]
        norm = jnp.sum(v * v, axis=0, keepdims=True) * (-BITS)
        b = tgt_all[r, D:D + 1, :] * BITS + logb_ref[r] * LOG2E
        bias[r] = b
        hi, lo = split2(v)
        one = jnp.ones((1, TW), jnp.float32)
        tail = placed(D, [one] * 3 + list(split3(norm)) + list(split3(b)), TW)
        return jnp.concatenate([hi, lo, hi, tail], axis=0).astype(jnp.bfloat16)

    def chunk(slots):
        t = jnp.dot(
            lhs[...], jnp.concatenate([right(r) for r in slots], axis=1), preferred_element_type=jnp.float32
        )
        top = mrep[...]
        for n, r in enumerate(slots):
            zs[r] = t[:, n * TW:(n + 1) * TW]
        for q in range(0, len(slots) * TW, 128):
            top = jnp.maximum(top, t[:, q:q + 128])
        mrep[...] = top

    def chunks(count, offsets):
        def one(k, carry):
            chunk([
                lax.rem(z + dz + NZ, NZ) * NX + lax.rem(x + dx + NX, NX) for dz, dx in offsets(k)
            ])
            return carry
        lax.fori_loop(0, count, one, 0)

    both = NZ > 1 and NX > 1
    for h in (0, 1):
        arrived(h, 0, 0)
    src_arrived(0)
    left(col)
    for dy in (1, -1):
        src_arrived(dy)
    for h in (0, 1):
        for da in (1, -1):
            arrived(h, da, 0)
    for h in (0, 1):
        for db in (1, -1):
            arrived(h, 0, db)
    src_arrived(2)
    if NY > 1:
        for dy in (1, -1, 2):
            left(src_slot(dy))
    for h in (0, 1):
        arrived(h, 2, 0)
        for da in (1, -1):
            for db in (1, -1):
                arrived(h, da, db)
    if NC > 1:
        for dy in ((0, 1, -1, 2) if NY > 1 else (0,)):
            c = src_slot(dy, 1)
            wait_for(source(c), src_recv.at[c])
            left(c)

    if both:
        chunks(2, lambda k: ((k, 1 - k), (-k, k - 1)))
    elif NZ > 1:
        chunks(1, lambda k: ((1, 0), (-1, 0)))
    elif NX > 1:
        chunks(1, lambda k: ((0, 1), (0, -1)))
    else:
        chunks(1, lambda k: ((0, 0),))
    for h in (0, 1):
        for db in (1, -1):
            arrived(h, 2, db)
        arrived(h, 0, 2)
    if both:
        chunks(2, lambda k: ((1, 1 - 2 * k), (-1, 1 - 2 * k)))
        chunks(1, lambda k: ((2, 0), (0, 2)))
    elif NZ > 1:
        chunks(1, lambda k: ((0, 0), (2, 0)))
    elif NX > 1:
        chunks(1, lambda k: ((0, 0), (0, 2)))
    for h in (0, 1):
        for da in (1, -1, 2):
            arrived(h, da, 2)
    if both:
        chunks(2, lambda k: ((2 - k, 3 * k - 1), (2 - 3 * k, 1 + k)))
        chunks(1, lambda k: ((0, 0), (2, 2)))

    def lane_tops():
        for t in range(ROWS // 128):
            rows = slice(t * 128, (t + 1) * 128)
            mrep[rows, :] = jnp.broadcast_to(jnp.max(mrep[rows, :], axis=1, keepdims=True), (128, 128))

    RB = min(32, ROWS)
    bad = jnp.zeros((1, 1), jnp.float32)
    diag = (lax.broadcasted_iota(jnp.int32, (128, 128), 0) == lax.broadcasted_iota(jnp.int32, (128, 128), 1))

    for it in range(ITERS):
        last = it == ITERS - 1

        def term(r):
            return delta[r] if it else None

        shift = None
        if it and not fast:
            def top_of(i, carry):
                rows = pl.ds(pl.multiple_of(i * RB, RB), RB)
                top = jnp.full((RB, 128), -jnp.inf, jnp.float32)
                for r in range(NR):
                    v = zs[r, rows, :] + delta[r]
                    for q in range(0, TW, 128):
                        top = jnp.maximum(top, v[:, q:q + 128])
                mrep[rows, :] = top
                return carry
            lax.fori_loop(0, ROWS // RB, top_of, 0)
        if not (it and fast):
            lane_tops()
        if it and fast:
            shift = jnp.max(jnp.concatenate([delta[r] for r in range(NR)], axis=0), axis=0, keepdims=True)
            shift = jnp.max(shift, axis=1, keepdims=True)
            for r in range(NR):
                delta[r] = jnp.exp2(delta[r] - shift)

        def sum_of(i, carry):
            rows = pl.ds(pl.multiple_of(i * RB, RB), RB)
            top = mrep[rows, :]
            acc = jnp.zeros((RB, 128), jnp.float32)
            for r in range(NR):
                for q in range(0, TW, 128):
                    v = zs[r, rows, q:q + 128]
                    if it and fast:
                        acc = acc + v * delta[r, :, q:q + 128]
                        continue
                    if it:
                        v = v + delta[r, :, q:q + 128]
                    e = jnp.exp2(v - top)
                    if fast:
                        zs[r, rows, q:q + 128] = e
                    acc = acc + e
            sacc[rows, :] = acc
            return carry
        lax.fori_loop(0, ROWS // RB, sum_of, 0)

        packed = []
        least = None
        for t in range(ROWS // 128):
            rows = slice(t * 128, (t + 1) * 128)
            s = jnp.sum(sacc[rows, :], axis=1, keepdims=True)
            part = mrep[rows, :] + jnp.log2(s)
            if it and fast:
                part = part + shift
                least = s if least is None else jnp.minimum(least, s)
            packed.append(jnp.sum(jnp.where(diag, part, 0.0), axis=0, keepdims=True))
        f_buf[it, col] = jnp.concatenate(packed, axis=0)
        if it and fast:
            bad = bad + jnp.max(jnp.where(least >= SMALLEST, 0.0, 1.0), axis=0, keepdims=True)
        if fast:
            if it == 0:
                tops = [
                    jnp.sum(jnp.where(diag, mrep[t * 128:(t + 1) * 128, :], 0.0), axis=0, keepdims=True)
                    for t in range(ROWS // 128)
                ]
                m_rows[...] = jnp.concatenate(tops, axis=0)
        to_all(col_peer, NK, lambda k: f_buf.at[it, col], f_buf.at[it, col], f_sems.at[it, 0], f_sems.at[it, 1])
        wait_bytes(f_buf.at[it], NK - 1, f_sems.at[it, 1])
        parts = f_buf[it]
        top = jnp.max(parts, axis=0)
        whole = top + jnp.log2(jnp.sum(jnp.exp2(parts - top[None]), axis=0))
        if last:
            f_ref[...] = whole * (-NATS)
        term_rows = loga_ref[...] * LOG2E - whole
        level = jnp.zeros((1, 1), jnp.float32)
        if fast:
            term_rows = term_rows + m_rows[...]
            level = jnp.max(jnp.max(term_rows, axis=0, keepdims=True), axis=1, keepdims=True)
            term_rows = jnp.exp2(term_rows - level)
        weights = sacc if fast else mrep
        for t in range(ROWS // 128):
            v = jnp.where(diag, term_rows[t:t + 1, :], 0.0)
            s = jnp.sum(v, axis=1, keepdims=True)
            weights[t * 128:(t + 1) * 128, :] = jnp.broadcast_to(s, (128, 128))

        CB = min(4, NR)

        def columns(i, carry):
            slots = [i * CB + n for n in range(CB)]

            def sums(k, acc):
                rows = pl.ds(pl.multiple_of(k * 128, 128), 128)
                u = weights[rows, :]
                out = []
                for n, r in enumerate(slots):
                    for q in range(0, TW, 128):
                        v = zs[r, rows, q:q + 128] * u
                        out.append(acc[len(out)] + jnp.sum(v.reshape(16, 8, 128), axis=0))
                return tuple(out)
            none = tuple(jnp.zeros((8, 128), jnp.float32) for _ in range(CB * TW // 128))
            found = lax.fori_loop(0, ROWS // 128, sums, none)
            for n, r in enumerate(slots):
                part = [jnp.sum(v, axis=0, keepdims=True) for v in found[n * TW // 128:(n + 1) * TW // 128]]
                c_send[it, r, :, 0:TW] = jnp.log2(jnp.concatenate(part, axis=1)) + level - bias[r]
                c_send[it, r, :, TW:TW + 128] = jnp.broadcast_to(level, (1, 128))
            return carry

        def column(r, carry):
            def tops(i, acc):
                rows = pl.ds(pl.multiple_of(i * 128, 128), 128)
                f = mrep[rows, :]
                out = []
                for n, q in enumerate(range(0, TW, 128)):
                    v = zs[r, rows, q:q + 128] + f
                    out.append(jnp.maximum(acc[n], jnp.max(v.reshape(16, 8, 128), axis=0)))
                return tuple(out)
            low = tuple(jnp.full((8, 128), -jnp.inf, jnp.float32) for _ in range(0, TW, 128))
            tops_ = lax.fori_loop(0, ROWS // 128, tops, low)
            tops_ = [jnp.max(t, axis=0, keepdims=True) for t in tops_]

            def sums(i, acc):
                rows = pl.ds(pl.multiple_of(i * 128, 128), 128)
                f = mrep[rows, :]
                out = []
                for n, q in enumerate(range(0, TW, 128)):
                    v = jnp.exp2((zs[r, rows, q:q + 128] + f) - tops_[n])
                    out.append(acc[n] + jnp.sum(v.reshape(16, 8, 128), axis=0))
                return tuple(out)
            none = tuple(jnp.zeros((8, 128), jnp.float32) for _ in range(0, TW, 128))
            sums_ = lax.fori_loop(0, ROWS // 128, sums, none)
            sums_ = [jnp.sum(s, axis=0, keepdims=True) for s in sums_]
            val = jnp.concatenate([t + jnp.log2(s) for t, s in zip(tops_, sums_)], axis=1)
            c_send[it, r, :, 0:TW] = val - bias[r]
            c_send[it, r, :, TW:TW + 128] = jnp.zeros((1, 128), jnp.float32)
            return carry
        if fast:
            lax.fori_loop(0, NR // CB, columns, 0)
        else:
            lax.fori_loop(0, NR, column, 0)
        c_buf[it, row] = c_send[it, row]
        to_all(
            row_peer, NR, lambda k: c_send.at[it, lax.rem(row + k, NR)], c_buf.at[it, row],
            c_sems.at[it, 0], c_sems.at[it, 1],
        )
        wait_bytes(c_buf.at[it], NR - 1, c_sems.at[it, 1])
        got = [c_buf[it, r, :, 0:TW] for r in range(NR)]
        top = functools.reduce(jnp.maximum, got)
        tot = functools.reduce(jnp.add, [jnp.exp2(v - top) for v in got])
        mapped = top + jnp.log2(tot)
        if fast:
            levels = functools.reduce(jnp.maximum, [c_buf[it, r, :, TW:TW + 128] for r in range(NR)])
            size = mapped + bias[row] - jnp.concatenate([levels] * (TW // 128), axis=1)
            bad = bad + jnp.max(jnp.where(size >= LEAST_BITS, 0.0, 1.0), axis=1, keepdims=True)
        mapped = mapped * (-NATS)

        if it == 0:
            images = [hm_in[k:k + 1, :] for k in range(HIST - 1)] + [mapped]
            base = [hg_ref[k:k + 1, :] for k in range(HIST - 1)] + [g_in[...]]
        else:
            images = images[1:] + [mapped]
            base = base[1:] + [g_own]
        resid = placed(8, [p - q for p, q in zip(images, base)], TW)
        lane = lax.broadcasted_iota(jnp.int32, (8, 128), 1)
        sub = lax.broadcasted_iota(jnp.int32, (8, 128), 0)
        flat = jnp.zeros((8, 128), jnp.float32)
        for b in range(HIST):
            prod = jnp.sum(resid * resid[b:b + 1, :], axis=1, keepdims=True)
            flat = jnp.where(lane == sub * 8 + b, prod, flat)
        flat = jnp.sum(flat, axis=0, keepdims=True)
        line = lax.broadcasted_iota(jnp.int32, (1, 128), 1)
        flat = jnp.where(line == FLAG_LANE, bad, flat)
        m_buf[it, row, :, 0:TW] = mapped
        m_buf[it, row, :, TW:TW + 128] = flat
        to_all(row_peer, NR, lambda k: m_buf.at[it, row], m_buf.at[it, row], m_sems.at[it, 0], m_sems.at[it, 1])
        wait_bytes(m_buf.at[it], NR - 1, m_sems.at[it, 1])
        flat = m_buf[it, 0, :, TW:TW + 128]
        for r in range(1, NR):
            flat = flat + m_buf[it, r, :, TW:TW + 128]
        r_buf[it, col] = flat
        to_all(col_peer, NK, lambda k: r_buf.at[it, col], r_buf.at[it, col], r_sems.at[it, 0], r_sems.at[it, 1])
        wait_bytes(r_buf.at[it], NK - 1, r_sems.at[it, 1])
        flat = r_buf[it, 0]
        for b in range(1, NK):
            flat = flat + r_buf[it, b]
        gram = {
            (a, b): jnp.sum(jnp.where(line == a * 8 + b, flat, 0.0), axis=1, keepdims=True)
            for a in range(HIST) for b in range(a, HIST)
        }
        mix = solve(gram)
        g_own = images[0] * mix[0]
        for k in range(1, HIST):
            g_own = g_own + images[k] * mix[k]
        if last:
            gout_ref[...] = g_own
            flag_ref[...] = jnp.broadcast_to(
                jnp.sum(jnp.where(line == FLAG_LANE, flat, 0.0), axis=1, keepdims=True), (1, 128)
            )
        else:
            def renew(r, carry):
                acc = m_buf[it, r, :, 0:TW] * mix[HIST - 1]
                for k in range(HIST - 1):
                    acc = acc + tgt_all[r, D + 1 + k:D + 2 + k, :] * mix[k]
                b = acc * BITS + logb_ref[r] * LOG2E
                delta[r] = b - bias[r]
                return carry
            lax.fori_loop(0, NR, renew, 0)

    wait_bytes(src_all, NK - 1, src_send)
    wait_bytes(tgt_all, NR - 1, tgt_send)
    for it in range(ITERS):
        wait_bytes(f_buf.at[it], NK - 1, f_sems.at[it, 0])
        wait_bytes(c_buf.at[it], NR - 1, c_sems.at[it, 0])
        wait_bytes(m_buf.at[it], NR - 1, m_sems.at[it, 0])
        wait_bytes(r_buf.at[it], NK - 1, r_sems.at[it, 0])


def shards(dims, src, tgt, log_a, log_b, g, hist_g, hist_maps):
    NZ, NX, NY, NC = dims
    NR, NK = NZ * NX, NY * NC
    D, SW = src.shape
    TW = tgt.shape[1]
    ROWS = NK * SW
    f32 = jnp.float32
    vmem = pl.BlockSpec(memory_space=pltpu.VMEM)
    dma = pltpu.SemaphoreType.DMA
    def call(fast):
        return pl.pallas_call(
        functools.partial(kernel, fast, dims),
        out_shape=(
            jax.ShapeDtypeStruct((ROWS // 128, 128), f32),
            jax.ShapeDtypeStruct((1, TW), f32),
            jax.ShapeDtypeStruct((1, 128), f32),
        ),
        in_specs=[pl.BlockSpec(memory_space=pltpu.HBM)] * 7,
        out_specs=(vmem, vmem, vmem),
        scratch_shapes=[
            pltpu.VMEM((NR, D + 8, TW), f32),
            pltpu.VMEM((NK, D, SW), f32),
            pltpu.VMEM((1, TW), f32),
            pltpu.VMEM((HIST - 1, TW), f32),
            pltpu.VMEM((ROWS // 128, 128), f32),
            pltpu.VMEM((NR, 1, TW), f32),
            pltpu.VMEM((HIST - 1, TW), f32),
            pltpu.VMEM((ROWS, 4 * D), jnp.bfloat16),
            pltpu.VMEM((NR, ROWS, TW), f32),
            pltpu.VMEM((ROWS, 128), f32),
            pltpu.VMEM((ROWS, 128), f32),
            pltpu.VMEM((ROWS // 128, 128), f32),
            pltpu.VMEM((NR, 1, TW), f32),
            pltpu.VMEM((NR, 1, TW), f32),
            pltpu.VMEM((ITERS, NK, ROWS // 128, 128), f32),
            pltpu.VMEM((ITERS, NR, 1, TW + 128), f32),
            pltpu.VMEM((ITERS, NR, 1, TW + 128), f32),
            pltpu.VMEM((ITERS, NR, 1, TW + 128), f32),
            pltpu.VMEM((ITERS, NK, 1, 128), f32),
            dma((7,)), dma, dma((2, NR)), dma, dma((NK,)),
            dma((ITERS, 2)), dma((ITERS, 2)), dma((ITERS, 2)), dma((ITERS, 2)),
        ],
        compiler_params=pltpu.CompilerParams(
            collective_id=0 if fast else 1, has_side_effects=True, vmem_limit_bytes=48 * 1024 * 1024
        ),
        name="sinkhorn" if fast else "sinkhorn_wide",
    )(src, tgt, log_a.reshape(ROWS // 128, 128), log_b.reshape(NR, 1, TW), g.reshape(1, TW), hist_g, hist_maps)

    f, gout, flag = call(True)
    f, gout = lax.cond(flag[0, 0] > 0.5, lambda: call(False)[:2], lambda: (f, gout))
    return f.reshape(-1), gout.reshape(-1)


def solution(mesh, dims=(4, 4, 4, 2)):
    grid = Mesh(mesh.devices.reshape(dims), AXES)
    in_specs = (
        P(None, AXES),
        P(None, ("y", "core", "z", "x")),
        P(("z", "x")),
        P(("y", "core")),
        P(("y", "core", "z", "x")),
        P(None, ("y", "core", "z", "x")),
        P(None, ("y", "core", "z", "x")),
    )
    out_specs = (P(("z", "x")), P(("y", "core", "z", "x")))
    return jax.shard_map(
        functools.partial(shards, dims), mesh=grid, in_specs=in_specs, out_specs=out_specs, check_vma=False
    )
```

```python
import functools

import jax
import jax.numpy as jnp
from jax import lax
from jax.experimental import pallas as pl
from jax.experimental.pallas import tpu as pltpu
from jax.sharding import Mesh
from jax.sharding import PartitionSpec as P

HIST = 5
ITERS = 2
EPS = 0.1
LOG2E = 1.4426950408889634
BITS = LOG2E / EPS
NATS = EPS / LOG2E
LEAST_BITS = -97.0
SMALLEST = 2.0**LEAST_BITS
MESH = pl.DeviceIdType.MESH
AXES = ("z", "x", "y", "core")


def split2(v):
    hi = v.astype(jnp.bfloat16).astype(jnp.float32)
    return hi, v - hi


def split3(v):
    hi = v.astype(jnp.bfloat16).astype(jnp.float32)
    rest = v - hi
    mid = rest.astype(jnp.bfloat16).astype(jnp.float32)
    return hi, mid, rest - mid


def placed(rows, values, width):
    at = lax.broadcasted_iota(jnp.int32, (rows, width), 0)
    out = jnp.zeros((rows, width), jnp.float32)
    for k, v in enumerate(values):
        out = jnp.where(at == k, v, out)
    return out


def solve(gram):
    n = HIST
    trace = gram[0, 0]
    for k in range(1, n):
        trace = trace + gram[k, k]
    shift = 0.001 * trace / n + 1e-6
    a = [[gram[min(p, q), max(p, q)] + (shift if p == q else 0.0) for q in range(n)] for p in range(n)]
    rhs = [jnp.ones((1, 1), jnp.float32) for _ in range(n)]
    for p in range(n):
        for low in range(p + 1, n):
            factor = a[low][p] / a[p][p]
            for q in range(p + 1, n):
                a[low][q] = a[low][q] - factor * a[p][q]
            rhs[low] = rhs[low] - factor * rhs[p]
    out = [None] * n
    for p in reversed(range(n)):
        acc = rhs[p]
        for q in range(p + 1, n):
            acc = acc - a[p][q] * out[q]
        out[p] = acc / a[p][p]
    total = out[0]
    for k in range(1, n):
        total = total + out[k]
    return [o / total for o in out]


def kernel(
    fast, dims,
    src_hbm, tgt_hbm, loga_hbm, logb_hbm, g_hbm, hg_hbm, hm_hbm,
    f_ref, gout_ref, flag_ref,
    src_all, tgt_all, loga_in, logb_in, g_in, hg_in, hm_in,
    left, zs, wacc, vrep, hist, m_rows, a_rows, u_rows, g_tmp,
    f_buf, fo_buf, c_buf, r_buf,
    in_sems, src_send, src_recv, tgt_send, tgt_recv, f_sems, fo_sems, c_sems, r_sems,
):
    NZ, NX, NY, NC = dims
    SIZE = dict(zip(AXES, dims))
    NR, NK = NZ * NX, NY * NC
    D, SW = src_hbm.shape
    TW = tgt_hbm.shape[1]
    COLS = NK * TW
    NT = COLS // 128
    at = {name: lax.axis_index(name) for name in AXES}
    z, x, y, core = (at[name] for name in AXES)
    row, col = z * NX + x, y * NC + core

    def row_peer(k):
        p = lax.rem(row + k, NR)
        return {"z": p // NX, "x": lax.rem(p, NX)}

    def col_peer(k):
        p = lax.rem(col + k, NK)
        return {"y": p // NC, "core": lax.rem(p, NC)}

    def near(axis, d):
        return {axis: lax.rem(at[axis] + d + SIZE[axis], SIZE[axis])}

    def remote(part, ssem, rsem, peer):
        pltpu.make_async_remote_copy(
            src_ref=part, dst_ref=part, send_sem=ssem, recv_sem=rsem, device_id=peer, device_id_type=MESH
        ).start()

    def to_all(peer, count, part, sems):
        def one(k, carry):
            remote(part, sems.at[0], sems.at[1], peer(k))
            return carry
        lax.fori_loop(1, count, one, 0)

    def wait_for(part, sem):
        pltpu.make_async_copy(part, part, sem).wait()

    def wait_bytes(buf, count, sem):
        if count:
            wait_for(buf.at[pl.ds(0, count)], sem)

    barrier = pltpu.get_barrier_semaphore()
    around = [(name, d) for name in ("x", "z", "y") if SIZE[name] > 1 for d in (1, -1)]
    if NC > 1:
        around.append(("core", 1))
    for name, d in around:
        pl.semaphore_signal(barrier, inc=1, device_id=near(name, d), device_id_type=MESH)

    moves = [
        (src_hbm, src_all.at[row, pl.ds(0, D)]), (tgt_hbm, tgt_all.at[col, pl.ds(0, D)]), (loga_hbm, loga_in),
        (logb_hbm.at[row], logb_in), (g_hbm, g_in), (hm_hbm, hm_in), (hg_hbm, hg_in),
    ]
    moves = [pltpu.make_async_copy(s, d, in_sems.at[k]) for k, (s, d) in enumerate(moves)]
    for m in moves:
        m.start()
    for m in moves:
        m.wait()
    KEPT = HIST - 1
    src_all[row, D:D + 8, :] = placed(8, [loga_in[pl.ds(col, 1), :]], SW)
    tgt_all[col, D:D + 16, :] = placed(
        16, [g_in[...], logb_in[...]] + [hm_in[k:k + 1, :] for k in range(KEPT)]
        + [hg_in[k:k + 1, :] for k in range(KEPT)], TW
    )
    pl.semaphore_wait(barrier, len(around))

    HALF, QUART, EXTRA = D // 2, D // 4, 8
    PIECES = {
        (0, None): (0, HALF), (0, 0): (0, QUART), (0, 1): (QUART, QUART),
        (1, None): (HALF, HALF + EXTRA), (1, 0): (HALF, QUART + EXTRA), (1, 1): (HALF + QUART + EXTRA, QUART),
    }
    ORDER = (("x", "z"), ("z", "x"))

    def slot_of(dz, dx):
        return lax.rem(z + dz + NZ, NZ) * NX + lax.rem(x + dx + NX, NX)

    def piece(r, h, sub=None):
        start, count = PIECES[h, sub]
        return src_all.at[r, pl.ds(start, count)]

    def pass_on(r, h, sub, axis, d):
        remote(piece(r, h, sub), src_send, src_recv.at[h, r], near(axis, d))

    def arrived(h, da, db):
        a, b = ORDER[h]
        if (da and SIZE[a] == 1) or (db and SIZE[b] == 1):
            return
        r = slot_of(**{"d" + a: da, "d" + b: db})
        if da or db:
            wait_for(piece(r, h), src_recv.at[h, r])
        if db == 0:
            if da == 0 and SIZE[a] > 1:
                for d in (1, -1):
                    pass_on(r, h, None, a, d)
            elif da in (1, -1):
                pass_on(r, h, 0 if da < 0 else 1, a, -da)
            if SIZE[b] > 1:
                for d in (1, -1):
                    pass_on(r, h, None, b, d)
        elif db in (1, -1):
            pass_on(r, h, 0 if db < 0 else 1, b, -db)

    TROWS = D + 16

    def target(c, sub=None):
        if sub is None:
            return tgt_all.at[c]
        return tgt_all.at[c, pl.ds(sub * (TROWS // 2), TROWS // 2)]

    def tgt_slot(dy, other=0):
        return lax.rem(y + dy + NY, NY) * NC + lax.rem(core + other, NC)

    def tgt_pass(c, sub, axis, d):
        remote(target(c, sub), tgt_send, tgt_recv.at[c], near(axis, d))

    def tgt_arrived(dy):
        if dy and NY == 1:
            return
        c = tgt_slot(dy)
        if dy:
            wait_for(target(c), tgt_recv.at[c])
        if dy == 0 and NY > 1:
            for d in (1, -1):
                tgt_pass(c, None, "y", d)
        elif dy in (1, -1):
            tgt_pass(c, 0 if dy < 0 else 1, "y", -dy)
        if NC > 1:
            tgt_pass(c, None, "core", 1)

    def take_targets(c):
        v = tgt_all[c, 0:D, :]
        norm = jnp.sum(v * v, axis=0, keepdims=True) * (-BITS)
        b = tgt_all[c, D:D + 1, :] * BITS + tgt_all[c, D + 1:D + 2, :] * LOG2E
        hi, lo = split2(v)
        one = jnp.ones((1, TW), jnp.float32)
        tail = placed(D, list(split3(norm)) + list(split3(b)) + [one] * 3, TW)
        full = jnp.concatenate([hi, lo, hi, tail], axis=0)
        left[pl.ds(pl.multiple_of(c * TW, TW), TW), :] = full.T.astype(jnp.bfloat16)

    def sources(r):
        v = src_all[r, 0:D, :]
        norm = jnp.sum(v * v, axis=0, keepdims=True) * (-BITS)
        hi, lo = split2(v * (2.0 * BITS))
        one = jnp.ones((1, SW), jnp.float32)
        tail = placed(D, [one] * 6 + list(split3(norm)), SW)
        return jnp.concatenate([hi, hi, lo, tail], axis=0).astype(jnp.bfloat16)

    EB = min(256, COLS)

    def block(offsets):
        spots = [(lax.rem(z + dz + NZ, NZ), lax.rem(x + dx + NX, NX)) for dz, dx in offsets]
        slots = [zb * NX + xb for zb, xb in spots]
        t = jnp.dot(
            left[...], jnp.concatenate([sources(r) for r in slots], axis=1), preferred_element_type=jnp.float32
        )
        tops = []
        for n, r in enumerate(slots):
            part = t[:, n * SW:(n + 1) * SW]
            zs[r] = part
            tops.append(jnp.max(jnp.max(part.reshape(COLS // 8, 8, SW), axis=0), axis=0, keepdims=True))

        def expo(i, acc):
            rows = pl.ds(pl.multiple_of(i * EB, EB), EB)
            out = []
            for n, r in enumerate(slots):
                e = jnp.exp2(zs[r, rows, :] - tops[n])
                if fast:
                    zs[r, rows, :] = e
                out.append(acc[n] + jnp.sum(e.reshape(EB // 8, 8, SW), axis=0))
            return tuple(out)
        found = lax.fori_loop(0, COLS // EB, expo, tuple(jnp.zeros((8, SW), jnp.float32) for _ in slots))
        for n, (zb, xb) in enumerate(spots):
            f_buf[0, row, zb, pl.ds(xb, 1), :] = tops[n] + jnp.log2(jnp.sum(found[n], axis=0, keepdims=True))
            m_rows[zb, pl.ds(xb, 1), :] = tops[n]
            a_rows[zb, pl.ds(xb, 1), :] = src_all[slots[n], D:D + 1, :] * LOG2E

    def blocks(count, offsets):
        def one(k, carry):
            block(offsets(k))
            return carry
        lax.fori_loop(0, count, one, 0)

    def send_f(it, zb):
        to_all(row_peer, NR, f_buf.at[it, row, zb], f_sems.at[it])

    both = NZ > 1 and NX > 1
    tgt_arrived(0)
    for h in (0, 1):
        arrived(h, 0, 0)
    take_targets(col)
    for dy in (1, -1):
        tgt_arrived(dy)
    for h in (0, 1):
        for da in (1, -1):
            arrived(h, da, 0)
    for h in (0, 1):
        for db in (1, -1):
            arrived(h, 0, db)
    tgt_arrived(2)
    if NY > 1:
        for dy in (1, -1, 2):
            take_targets(tgt_slot(dy))
    for h in (0, 1):
        arrived(h, 2, 0)
        for da in (1, -1):
            for db in (1, -1):
                arrived(h, da, db)
    if NC > 1:
        for dy in ((0, 1, -1, 2) if NY > 1 else (0,)):
            c = tgt_slot(dy, 1)
            wait_for(target(c), tgt_recv.at[c])
            take_targets(c)
    if both:
        blocks(2, lambda k: ((k, 1 - k), (-k, k - 1)))
    for h in (0, 1):
        for db in (1, -1):
            arrived(h, 2, db)
        arrived(h, 0, 2)
    if both:
        blocks(2, lambda k: ((1, 1 - 2 * k), (-1, 1 - 2 * k)))
    block(((0, 0), (0, 2)) if both else ((0, 0),))
    for h in (0, 1):
        for da in (1, -1, 2):
            arrived(h, da, 2)
    send_f(0, z)
    if both:
        blocks(1, lambda k: ((1, 2), (-1, 2)))
        for d in (1, 3):
            send_f(0, lax.rem(z + d, NZ))
        blocks(2, lambda k: ((2, 1 - k), (2, 3 * k - 1)))
        send_f(0, lax.rem(z + 2, NZ))
    for c in range(NK):
        for k in range(2 * KEPT + 2):
            for q in range(TW // 128):
                t = c * (TW // 128) + q
                hist[k, t:t + 1, :] = tgt_all[c, D + k:D + k + 1, q * 128:(q + 1) * 128]

    bad = jnp.zeros((1, 1), jnp.float32)
    g_now = hist[0]
    bias = g_now * BITS + hist[1] * LOG2E
    images = [hist[2 + k] for k in range(KEPT)]
    base = [hist[2 + KEPT + k] for k in range(KEPT)]
    shift = jnp.zeros((1, 1), jnp.float32)
    pairs = [(a, b) for a in range(HIST) for b in range(a, HIST)]
    line = lax.broadcasted_iota(jnp.int32, (1, 128), 1)
    eye = (lax.broadcasted_iota(jnp.int32, (16, 128), 0) == lax.broadcasted_iota(jnp.int32, (16, 128), 1))

    def all_of(v, op):
        return op(op(v, axis=0, keepdims=True), axis=1, keepdims=True)

    def low(v):
        return all_of(jnp.where(v >= SMALLEST, 0.0, 1.0), jnp.max)

    for it in range(ITERS):
        last = it == ITERS - 1
        if it and fast:
            GZ = min(2, NZ)
            SB = min(128, COLS)
            for zg in range(0, NZ, GZ):
                spots = [(zz, xx) for zz in range(zg, zg + GZ) for xx in range(NX)]

                def weigh(i, acc):
                    rows = pl.ds(pl.multiple_of(i * SB, SB), SB)
                    v = vrep[rows, :]
                    return tuple(
                        a + jnp.sum((zs[zz * NX + xx, rows, :] * v).reshape(SB // 8, 8, SW), axis=0)
                        for a, (zz, xx) in zip(acc, spots)
                    )
                found = lax.fori_loop(0, COLS // SB, weigh, tuple(jnp.zeros((8, SW), jnp.float32) for _ in spots))
                found = [jnp.sum(v, axis=0, keepdims=True) for v in found]
                for zz in range(zg, zg + GZ):
                    s = jnp.concatenate(found[(zz - zg) * NX:(zz - zg + 1) * NX], axis=0)
                    bad = bad + low(s)
                    f_buf[it, row, zz] = m_rows[zz] + shift + jnp.log2(s)
                for zz in range(zg, zg + GZ):
                    send_f(it, zz)
        elif it:
            def again(r, carry):
                def tops_of(i, acc):
                    rows = pl.ds(pl.multiple_of(i * EB, EB), EB)
                    v = zs[r, rows, :] + vrep[rows, :]
                    return jnp.maximum(acc, jnp.max(v.reshape(EB // 8, 8, SW), axis=0))
                top = lax.fori_loop(0, COLS // EB, tops_of, jnp.full((8, SW), -jnp.inf, jnp.float32))
                top = jnp.max(top, axis=0, keepdims=True)

                def sums_of(i, acc):
                    rows = pl.ds(pl.multiple_of(i * EB, EB), EB)
                    v = jnp.exp2((zs[r, rows, :] + vrep[rows, :]) - top)
                    return acc + jnp.sum(v.reshape(EB // 8, 8, SW), axis=0)
                s = lax.fori_loop(0, COLS // EB, sums_of, jnp.zeros((8, SW), jnp.float32))
                f_buf[it, row, r // NX, pl.ds(lax.rem(r, NX), 1), :] = top + jnp.log2(
                    jnp.sum(s, axis=0, keepdims=True))
                return carry
            lax.fori_loop(0, NR, again, 0)
            for zz in range(NZ):
                send_f(it, zz)
        wait_bytes(f_buf.at[it], NR - 1, f_sems.at[it, 1])
        parts = [f_buf[it, r] for r in range(NR)]
        top = functools.reduce(jnp.maximum, parts)
        whole = top + jnp.log2(functools.reduce(jnp.add, [jnp.exp2(v - top) for v in parts]))
        term = a_rows[...] - whole
        level = jnp.zeros((1, 1), jnp.float32)
        if fast:
            term = term + m_rows[...]
            level = all_of(jnp.max(term, axis=0), jnp.max)
            u_rows[...] = jnp.exp2(term - level[None])
        else:
            u_rows[...] = term
        TPH = max(NT // 2, 1)
        for half in range(NT // TPH):
            def tile(i, carry):
                rows = pl.ds(pl.multiple_of((half * TPH + i) * 128, 128), 128)

                def scaled(r):
                    return zs[r, rows, :] * u_rows[r // NX, r % NX:r % NX + 1, :]
                acc = scaled(0)
                for r in range(1, NR):
                    acc = acc + scaled(r)
                wacc[rows, :] = acc
                return carry

            def tile_wide(i, carry):
                rows = pl.ds(pl.multiple_of((half * TPH + i) * 128, 128), 128)

                def moved(r):
                    return zs[r, rows, :] + u_rows[r // NX, r % NX:r % NX + 1, :]
                top = functools.reduce(jnp.maximum, [moved(r) for r in range(NR)])
                top = jnp.max(top, axis=1, keepdims=True)
                acc = functools.reduce(jnp.add, [jnp.exp2(moved(r) - top) for r in range(NR)])
                wacc[rows, :] = jnp.broadcast_to(top + jnp.log2(jnp.sum(acc, axis=1, keepdims=True)), (128, 128))
                return carry
            lax.fori_loop(0, TPH, tile if fast else tile_wide, 0)
            found = []
            for i in range(half * TPH, (half + 1) * TPH):
                turned = wacc[i * 128:(i + 1) * 128, :].T
                found.append(jnp.sum(turned, axis=0, keepdims=True) if fast else turned[0:1, :])
            found = jnp.concatenate(found, axis=0)
            lines = slice(half * TPH, (half + 1) * TPH)
            if fast:
                bad = bad + low(found)
                found = jnp.log2(found) + level
            c_buf[it, col, lines, :] = found - bias[lines, :]
            to_all(col_peer, NK, c_buf.at[it, col, pl.ds(half * TPH, TPH)], c_sems.at[it])
        if last:
            g_tmp[...] = whole
            fo_buf[col] = g_tmp[z, pl.ds(x, 1), :] * (-NATS)
            to_all(col_peer, NK, fo_buf.at[col], fo_sems)
        wait_bytes(c_buf.at[it], NK - 1, c_sems.at[it, 1])
        parts = [c_buf[it, c] for c in range(NK)]
        top = functools.reduce(jnp.maximum, parts)
        mapped = (top + jnp.log2(functools.reduce(jnp.add, [jnp.exp2(v - top) for v in parts]))) * (-NATS)
        images = (images + [mapped])[-HIST:]
        base = (base + [g_now])[-HIST:]
        resid = [p - q for p, q in zip(images, base)]
        prods = [jnp.sum(resid[a] * resid[b], axis=0, keepdims=True) for a, b in pairs]
        prods.append(jnp.where(line == 0, bad, 0.0))
        sums = jnp.sum(jnp.concatenate(prods, axis=0), axis=1, keepdims=True)
        r_buf[it, row] = jnp.sum(jnp.where(eye, sums, 0.0), axis=0, keepdims=True)
        to_all(row_peer, NR, r_buf.at[it, row], r_sems.at[it])
        wait_bytes(r_buf.at[it], NR - 1, r_sems.at[it, 1])
        flat = functools.reduce(jnp.add, [r_buf[it, r] for r in range(NR)])

        def entry(k):
            return jnp.sum(jnp.where(line == k, flat, 0.0), axis=1, keepdims=True)
        mix = solve({ab: entry(k) for k, ab in enumerate(pairs)})
        g_next = functools.reduce(jnp.add, [v * m for v, m in zip(images, mix)])
        if last:
            hist[0] = g_next
            for q in range(TW // 128):
                gout_ref[q:q + 1, :] = hist[0, pl.ds(col * (TW // 128) + q, 1), :]
            flag_ref[...] = jnp.broadcast_to(entry(len(pairs)), (1, 128))
        else:
            delta = (g_next - g_now) * BITS
            if fast:
                shift = all_of(delta, jnp.max)
                delta = jnp.exp2(delta - shift)
            for t in range(NT):
                vrep[t * 128:(t + 1) * 128, :] = jnp.broadcast_to(delta[t:t + 1, :], (128, 128)).T
            g_now = g_next

    wait_bytes(fo_buf, NK - 1, fo_sems.at[1])
    for c in range(NK):
        f_ref[c:c + 1, :] = fo_buf[c]
    wait_bytes(src_all, NR - 1, src_send)
    wait_bytes(tgt_all, NK - 1, tgt_send)
    wait_bytes(fo_buf, NK - 1, fo_sems.at[0])
    for it in range(ITERS):
        wait_bytes(f_buf.at[it], NR - 1, f_sems.at[it, 0])
        wait_bytes(c_buf.at[it], NK - 1, c_sems.at[it, 0])
        wait_bytes(r_buf.at[it], NR - 1, r_sems.at[it, 0])


def shards(dims, src, tgt, log_a, log_b, g, hist_g, hist_maps):
    NZ, NX, NY, NC = dims
    NR, NK = NZ * NX, NY * NC
    D, SW = src.shape
    TW = tgt.shape[1]
    COLS = NK * TW
    NT = COLS // 128
    f32 = jnp.float32
    vmem = pl.BlockSpec(memory_space=pltpu.VMEM)
    dma = pltpu.SemaphoreType.DMA

    def call(fast):
        return pl.pallas_call(
            functools.partial(kernel, fast, dims),
            out_shape=(
                jax.ShapeDtypeStruct((NK, SW), f32),
                jax.ShapeDtypeStruct((TW // 128, 128), f32),
                jax.ShapeDtypeStruct((1, 128), f32),
            ),
            in_specs=[pl.BlockSpec(memory_space=pltpu.HBM)] * 7,
            out_specs=(vmem, vmem, vmem),
            scratch_shapes=[
                pltpu.VMEM((NR, D + 8, SW), f32),
                pltpu.VMEM((NK, D + 16, TW), f32),
                pltpu.VMEM((NK, SW), f32),
                pltpu.VMEM((1, TW), f32),
                pltpu.VMEM((1, TW), f32),
                pltpu.VMEM((HIST - 1, TW), f32),
                pltpu.VMEM((HIST - 1, TW), f32),
                pltpu.VMEM((COLS, 4 * D), jnp.bfloat16),
                pltpu.VMEM((NR, COLS, SW), f32),
                pltpu.VMEM((COLS, 128), f32),
                pltpu.VMEM((COLS, 128), f32),
                pltpu.VMEM((2 * HIST, NT, 128), f32),
                pltpu.VMEM((NZ, NX, SW), f32),
                pltpu.VMEM((NZ, NX, SW), f32),
                pltpu.VMEM((NZ, NX, SW), f32),
                pltpu.VMEM((NZ, NX, SW), f32),
                pltpu.VMEM((ITERS, NR, NZ, NX, SW), f32),
                pltpu.VMEM((NK, 1, SW), f32),
                pltpu.VMEM((ITERS, NK, NT, 128), f32),
                pltpu.VMEM((ITERS, NR, 1, 128), f32),
                dma((7,)), dma, dma((2, NR)), dma, dma((NK,)),
                dma((ITERS, 2)), dma((2,)), dma((ITERS, 2)), dma((ITERS, 2)),
            ],
            compiler_params=pltpu.CompilerParams(
                collective_id=0 if fast else 1, has_side_effects=True, vmem_limit_bytes=48 * 1024 * 1024
            ),
            name="sinkhorn" if fast else "sinkhorn_wide",
        )(src, tgt, log_a.reshape(NK, SW), log_b.reshape(NR, 1, TW), g.reshape(1, TW), hist_g, hist_maps)

    f, gout, flag = call(True)
    f, gout = lax.cond(flag[0, 0] > 0.5, lambda: call(False)[:2], lambda: (f, gout))
    return f.reshape(-1), gout.reshape(-1)


def solution(mesh, dims=(4, 4, 4, 2)):
    grid = Mesh(mesh.devices.reshape(dims), AXES)
    in_specs = (
        P(None, AXES),
        P(None, ("y", "core", "z", "x")),
        P(("z", "x")),
        P(("y", "core")),
        P(("y", "core", "z", "x")),
        P(None, ("y", "core", "z", "x")),
        P(None, ("y", "core", "z", "x")),
    )
    out_specs = (P(("z", "x")), P(("y", "core", "z", "x")))
    return jax.shard_map(
        functools.partial(shards, dims), mesh=grid, in_specs=in_specs, out_specs=out_specs, check_vma=False
    )
```

```python
import functools

import jax
import jax.numpy as jnp
from jax import lax
from jax.experimental import pallas as pl
from jax.experimental.pallas import tpu as pltpu
from jax.sharding import Mesh
from jax.sharding import PartitionSpec as P

HIST = 5
ITERS = 2
EPS = 0.1
LOG2E = 1.4426950408889634
BITS = LOG2E / EPS
NATS = EPS / LOG2E
LEAST_BITS = -97.0
SMALLEST = 2.0**LEAST_BITS
MESH = pl.DeviceIdType.MESH
AXES = ("z", "x", "y", "core")


def split2(v):
    hi = v.astype(jnp.bfloat16).astype(jnp.float32)
    return hi, v - hi


def split3(v):
    hi = v.astype(jnp.bfloat16).astype(jnp.float32)
    rest = v - hi
    mid = rest.astype(jnp.bfloat16).astype(jnp.float32)
    return hi, mid, rest - mid


def placed(rows, values, width):
    at = lax.broadcasted_iota(jnp.int32, (rows, width), 0)
    out = jnp.zeros((rows, width), jnp.float32)
    for k, v in enumerate(values):
        out = jnp.where(at == k, v, out)
    return out


def solve(gram):
    n = HIST
    trace = gram[0, 0]
    for k in range(1, n):
        trace = trace + gram[k, k]
    shift = 0.001 * trace / n + 1e-6
    a = [[gram[min(p, q), max(p, q)] + (shift if p == q else 0.0) for q in range(n)] for p in range(n)]
    rhs = [jnp.ones((1, 1), jnp.float32) for _ in range(n)]
    for p in range(n):
        for low in range(p + 1, n):
            factor = a[low][p] / a[p][p]
            for q in range(p + 1, n):
                a[low][q] = a[low][q] - factor * a[p][q]
            rhs[low] = rhs[low] - factor * rhs[p]
    out = [None] * n
    for p in reversed(range(n)):
        acc = rhs[p]
        for q in range(p + 1, n):
            acc = acc - a[p][q] * out[q]
        out[p] = acc / a[p][p]
    total = out[0]
    for k in range(1, n):
        total = total + out[k]
    return [o / total for o in out]


def kernel(
    fast, dims,
    src_hbm, tgt_hbm, loga_hbm, logb_hbm, g_hbm, hg_hbm, hm_hbm,
    f_ref, gout_ref, flag_ref,
    src_all, tgt_all, loga_in, logb_in, g_in, hg_in, hm_in,
    left, staged, tops_buf, zs, wacc, vrep, hist, m_rows, a_rows, u_rows, g_tmp,
    f_buf, fo_buf, c_buf, r_buf,
    in_sems, src_send, src_recv, tgt_send, tgt_recv, f_sems, fo_sems, c_sems, r_sems,
):
    NZ, NX, NY, NC = dims
    SIZE = dict(zip(AXES, dims))
    NR, NK = NZ * NX, NY * NC
    D, SW = src_hbm.shape
    TW = tgt_hbm.shape[1]
    COLS = NK * TW
    NT = COLS // 128
    at = {name: lax.axis_index(name) for name in AXES}
    z, x, y, core = (at[name] for name in AXES)
    row, col = z * NX + x, y * NC + core

    def row_peer(k):
        p = lax.rem(row + k, NR)
        return {"z": p // NX, "x": lax.rem(p, NX)}

    def col_peer(k):
        p = lax.rem(col + k, NK)
        return {"y": p // NC, "core": lax.rem(p, NC)}

    def near(axis, d):
        return {axis: lax.rem(at[axis] + d + SIZE[axis], SIZE[axis])}

    def remote(part, ssem, rsem, peer):
        pltpu.make_async_remote_copy(
            src_ref=part, dst_ref=part, send_sem=ssem, recv_sem=rsem, device_id=peer, device_id_type=MESH
        ).start()

    def to_all(peer, count, part, sems):
        for k in range(1, count):
            remote(part, sems.at[0], sems.at[1], peer(k))

    def wait_for(part, sem):
        pltpu.make_async_copy(part, part, sem).wait()

    def wait_bytes(buf, count, sem):
        if count:
            wait_for(buf.at[pl.ds(0, count)], sem)

    barrier = pltpu.get_barrier_semaphore()
    around = [(name, d) for name in ("x", "z", "y") if SIZE[name] > 1 for d in (1, -1)]
    if NC > 1:
        around.append(("core", 1))
    for name, d in around:
        pl.semaphore_signal(barrier, inc=1, device_id=near(name, d), device_id_type=MESH)

    moves = [
        (src_hbm, src_all.at[row, pl.ds(0, D)]), (tgt_hbm, tgt_all.at[col, pl.ds(0, D)]), (loga_hbm, loga_in),
        (logb_hbm.at[row], logb_in), (g_hbm, g_in), (hm_hbm, hm_in), (hg_hbm, hg_in),
    ]
    moves = [pltpu.make_async_copy(s, d, in_sems.at[k]) for k, (s, d) in enumerate(moves)]
    for m in moves:
        m.start()
    for m in moves:
        m.wait()
    KEPT = HIST - 1
    src_all[row, D:D + 8, :] = placed(8, [loga_in[pl.ds(col, 1), :]], SW)
    tgt_all[col, D:D + 16, :] = placed(
        16, [g_in[...], logb_in[...]] + [hm_in[k:k + 1, :] for k in range(KEPT)]
        + [hg_in[k:k + 1, :] for k in range(KEPT)], TW
    )
    pl.semaphore_wait(barrier, len(around))

    HALF, QUART, EXTRA = D // 2, D // 4, 8
    PIECES = (((0, QUART), (QUART, QUART)), ((HALF, QUART + EXTRA), (HALF + QUART + EXTRA, QUART)))
    ORDER = (("x", "z"), ("z", "x"))
    seen = set()

    def slot_of(dz, dx):
        return lax.rem(z + dz + NZ, NZ) * NX + lax.rem(x + dx + NX, NX)

    def piece(r, h, sub):
        start, count = PIECES[h][sub]
        return src_all.at[r, pl.ds(start, count)]

    def pass_on(r, h, sub, axis, d):
        remote(piece(r, h, sub), src_send, src_recv.at[h, sub, r], near(axis, d))

    def part_for(d):
        return 0 if d < 0 else 1

    def start_sources():
        for phase in (0, 1):
            for first in (True, False):
                for h in (0, 1):
                    axis = ORDER[h][phase]
                    if SIZE[axis] > 1:
                        for d in (1, -1):
                            pass_on(row, h, part_for(-d) if first else part_for(d), axis, d)

    def arrived(h, da, db, sub):
        a, b = ORDER[h]
        if (h, da, db, sub) in seen or (da == 0 and db == 0):
            return
        seen.add((h, da, db, sub))
        r = slot_of(**{"d" + a: da, "d" + b: db})
        wait_for(piece(r, h, sub), src_recv.at[h, sub, r])
        if db == 0:
            if da in (1, -1) and sub == part_for(da):
                pass_on(r, h, sub, a, -da)
            for d in (1, -1):
                pass_on(r, h, sub, b, d)
        elif db in (1, -1) and sub == part_for(db):
            pass_on(r, h, sub, b, -db)

    def complete(*blocks):
        for dz, dx in blocks:
            for h in (0, 1):
                da, db = (dx, dz) if h == 0 else (dz, dx)
                for sub in (0, 1):
                    arrived(h, da, db, sub)

    THALF = (D + 16) // 2

    def target(c, sub):
        return tgt_all.at[c, pl.ds(sub * THALF, THALF)]

    def tgt_slot(dy, other=0):
        return lax.rem(y + dy + NY, NY) * NC + lax.rem(core + other, NC)

    def tgt_pass(c, sub, axis, d):
        remote(target(c, sub), tgt_send, tgt_recv.at[sub, c], near(axis, d))

    def start_targets():
        if NY > 1:
            for first in (True, False):
                for d in (1, -1):
                    tgt_pass(col, part_for(-d) if first else part_for(d), "y", d)
        if NC > 1:
            for sub in (0, 1):
                tgt_pass(col, sub, "core", 1)

    def tgt_arrived(dy, sub):
        c = tgt_slot(dy)
        wait_for(target(c, sub), tgt_recv.at[sub, c])
        if dy in (1, -1) and sub == part_for(dy):
            tgt_pass(c, sub, "y", -dy)
        if NC > 1:
            tgt_pass(c, sub, "core", 1)

    def take_targets(c):
        v = tgt_all[c, 0:D, :]
        norm = jnp.sum(v * v, axis=0, keepdims=True) * (-BITS)
        b = tgt_all[c, D:D + 1, :] * BITS + tgt_all[c, D + 1:D + 2, :] * LOG2E
        hi, lo = split2(v)
        one = jnp.ones((1, TW), jnp.float32)
        tail = placed(D, list(split3(norm)) + list(split3(b)) + [one] * 3, TW)
        full = jnp.concatenate([hi, lo, hi, tail], axis=0)
        left[pl.ds(pl.multiple_of(c * TW, TW), TW), :] = full.T.astype(jnp.bfloat16)

    def sources(r):
        v = src_all[r, 0:D, :]
        norm = jnp.sum(v * v, axis=0, keepdims=True) * (-BITS)
        hi, lo = split2(v * (2.0 * BITS))
        one = jnp.ones((1, SW), jnp.float32)
        tail = placed(D, [one] * 6 + list(split3(norm)), SW)
        return jnp.concatenate([hi, hi, lo, tail], axis=0).astype(jnp.bfloat16)

    QB = min(512, COLS)
    EB = min(256, COLS)

    def spots_of(offsets):
        return [(lax.rem(z + dz + 8 * NZ, NZ), lax.rem(x + dx + 8 * NX, NX)) for dz, dx in offsets]

    def folded(v, op):
        return op(v.reshape(v.shape[0] // 8, 8, v.shape[1]), axis=0)

    def step(done, new):
        if new:
            right = jnp.concatenate([sources(zb * NX + xb) for zb, xb in new], axis=1)
        tops, sums = [None] * len(new), [None] * len(done)
        before = [tops_buf[n] for n in range(len(done))]
        for q in range(COLS // QB):
            rows = slice(q * QB, (q + 1) * QB)
            for n, (zb, xb) in enumerate(done):
                e = jnp.exp2(staged[rows, n * SW:(n + 1) * SW] - before[n])
                if fast:
                    zs[zb * NX + xb, rows, :] = e
                else:
                    zs[zb * NX + xb, rows, :] = staged[rows, n * SW:(n + 1) * SW]
                e = folded(e, jnp.sum)
                sums[n] = e if q == 0 else sums[n] + e
            if new:
                t = jnp.dot(left[rows, :], right, preferred_element_type=jnp.float32)
                staged[rows, 0:len(new) * SW] = t
                for n in range(len(new)):
                    top = folded(t[:, n * SW:(n + 1) * SW], jnp.max)
                    tops[n] = top if q == 0 else jnp.maximum(tops[n], top)
        for n, (zb, xb) in enumerate(done):
            f_buf[0, row, zb, pl.ds(xb, 1), :] = before[n] + jnp.log2(jnp.sum(sums[n], axis=0, keepdims=True))
            m_rows[zb, pl.ds(xb, 1), :] = before[n]
            a_rows[zb, pl.ds(xb, 1), :] = src_all[zb * NX + xb, D:D + 1, :] * LOG2E
        for n in range(len(new)):
            tops_buf[n] = jnp.max(tops[n], axis=0, keepdims=True)

    def steps(count, first, offsets, after=None):
        def one(k, carry):
            p = jnp.minimum(k, 1)
            before = offsets(jnp.maximum(k - 1, 0))
            before = [tuple(p * v + (1 - p) * w for v, w in zip(*pair)) for pair in zip(before, first)]
            step(spots_of(before), spots_of(offsets(k)))
            if after is not None:
                after(k)
            return carry
        lax.fori_loop(0, count, one, 0)

    def send_f(it, zb):
        to_all(row_peer, NR, f_buf.at[it, row, zb], f_sems.at[it])

    both = NZ > 1 and NX > 1
    start_sources()
    start_targets()
    take_targets(col)
    if both:
        for h in (0, 1):
            for d in (1, -1):
                arrived(h, d, 0, part_for(d))
        for h in (0, 1):
            for d in (1, -1):
                arrived(h, d, 0, part_for(-d))
    if NY > 1:
        for d in (1, -1):
            tgt_arrived(d, part_for(d))
        for d in (1, -1):
            tgt_arrived(d, part_for(-d))
    if both:
        for h in (0, 1):
            for d in (1, -1):
                arrived(h, 0, d, part_for(d))
    if both:
        for h in (0, 1):
            for sub in (0, 1):
                arrived(h, 2, 0, sub)
            for da in (1, -1):
                for db in (1, -1):
                    arrived(h, da, db, part_for(db))
    if NY > 1:
        for sub in (0, 1):
            tgt_arrived(2, sub)
        for dy in (1, -1, 2):
            take_targets(tgt_slot(dy))
    if NC > 1:
        for dy in ((0, 1, -1, 2) if NY > 1 else (0,)):
            c = tgt_slot(dy, 1)
            for sub in (0, 1):
                wait_for(target(c, sub), tgt_recv.at[sub, c])
            take_targets(c)
    if both:
        complete((0, 1), (0, -1), (1, 0), (-1, 0))
    PAIR_A, PAIR_B = ((0, 1), (0, -1)), ((1, 0), (-1, 0))
    step([], spots_of(PAIR_A if both else ((0, 0),)))
    if both:
        step(spots_of(PAIR_A), spots_of(PAIR_B))
    if both:
        for h in (0, 1):
            for db in (1, -1):
                arrived(h, 2, db, part_for(db))
    if both:
        complete((1, 1), (1, -1), (-1, 1), (-1, -1), (0, 2))
    if both:
        def mid(k):
            a = 1 - k // 2
            return (a, (1 - 2 * k) * a), (-a, (1 - 2 * k) * a + 2 - 2 * a)
        steps(3, PAIR_B, mid)
    if both:
        complete((1, 2), (-1, 2), (2, 1), (2, -1), (2, 0), (2, 2))
    if both:
        def end(k):
            a = (2 - k) // 2
            return (2 - a, 2 - k), (2 - 3 * a, 2 - 3 * lax.rem(k, 2))

        def ready(k):
            @pl.when(k == 0)
            def _():
                send_f(0, z)

            @pl.when(k == 1)
            def _():
                for d in (1, 3):
                    send_f(0, lax.rem(z + d, NZ))
        steps(3, ((0, 0), (0, 2)), end, ready)
    step(spots_of(((2, 0), (2, 2)) if both else ((0, 0),)), [])
    send_f(0, lax.rem(z + NZ // 2, NZ))
    for c in range(NK):
        for k in range(2 * KEPT + 2):
            for q in range(TW // 128):
                t = c * (TW // 128) + q
                hist[k, t:t + 1, :] = tgt_all[c, D + k:D + k + 1, q * 128:(q + 1) * 128]

    bad = jnp.zeros((1, 1), jnp.float32)
    g_now = hist[0]
    bias = g_now * BITS + hist[1] * LOG2E
    images = [hist[2 + k] for k in range(KEPT)]
    base = [hist[2 + KEPT + k] for k in range(KEPT)]
    shift = jnp.zeros((1, 1), jnp.float32)
    pairs = [(a, b) for a in range(HIST) for b in range(a, HIST)]
    line = lax.broadcasted_iota(jnp.int32, (1, 128), 1)
    eye = (lax.broadcasted_iota(jnp.int32, (16, 128), 0) == lax.broadcasted_iota(jnp.int32, (16, 128), 1))

    def all_of(v, op):
        return op(op(v, axis=0, keepdims=True), axis=1, keepdims=True)

    def low(v):
        return all_of(jnp.where(v >= SMALLEST, 0.0, 1.0), jnp.max)

    for it in range(ITERS):
        last = it == ITERS - 1
        if it and fast:
            GZ = min(2, NZ)
            SB = min(128, COLS)
            for zg in range(0, NZ, GZ):
                spots = [(zz, xx) for zz in range(zg, zg + GZ) for xx in range(NX)]

                def weigh(i, acc):
                    rows = pl.ds(pl.multiple_of(i * SB, SB), SB)
                    v = vrep[rows, :]
                    return tuple(
                        a + jnp.sum((zs[zz * NX + xx, rows, :] * v).reshape(SB // 8, 8, SW), axis=0)
                        for a, (zz, xx) in zip(acc, spots)
                    )
                found = lax.fori_loop(0, COLS // SB, weigh, tuple(jnp.zeros((8, SW), jnp.float32) for _ in spots))
                found = [jnp.sum(v, axis=0, keepdims=True) for v in found]
                for zz in range(zg, zg + GZ):
                    s = jnp.concatenate(found[(zz - zg) * NX:(zz - zg + 1) * NX], axis=0)
                    bad = bad + low(s)
                    f_buf[it, row, zz] = m_rows[zz] + shift + jnp.log2(s)
                for zz in range(zg, zg + GZ):
                    send_f(it, zz)
        elif it:
            def again(r, carry):
                def tops_of(i, acc):
                    rows = pl.ds(pl.multiple_of(i * EB, EB), EB)
                    v = zs[r, rows, :] + vrep[rows, :]
                    return jnp.maximum(acc, jnp.max(v.reshape(EB // 8, 8, SW), axis=0))
                top = lax.fori_loop(0, COLS // EB, tops_of, jnp.full((8, SW), -jnp.inf, jnp.float32))
                top = jnp.max(top, axis=0, keepdims=True)

                def sums_of(i, acc):
                    rows = pl.ds(pl.multiple_of(i * EB, EB), EB)
                    v = jnp.exp2((zs[r, rows, :] + vrep[rows, :]) - top)
                    return acc + jnp.sum(v.reshape(EB // 8, 8, SW), axis=0)
                s = lax.fori_loop(0, COLS // EB, sums_of, jnp.zeros((8, SW), jnp.float32))
                f_buf[it, row, r // NX, pl.ds(lax.rem(r, NX), 1), :] = top + jnp.log2(
                    jnp.sum(s, axis=0, keepdims=True))
                return carry
            lax.fori_loop(0, NR, again, 0)
            for zz in range(NZ):
                send_f(it, zz)
        wait_bytes(f_buf.at[it], NR - 1, f_sems.at[it, 1])
        parts = [f_buf[it, r] for r in range(NR)]
        top = functools.reduce(jnp.maximum, parts)
        whole = top + jnp.log2(functools.reduce(jnp.add, [jnp.exp2(v - top) for v in parts]))
        term = a_rows[...] - whole
        level = jnp.zeros((1, 1), jnp.float32)
        if fast:
            term = term + m_rows[...]
            level = all_of(jnp.max(term, axis=0), jnp.max)
            u_rows[...] = jnp.exp2(term - level[None])
        else:
            u_rows[...] = term
        TPH = max(NT // 2, 1)
        for half in range(NT // TPH):
            def tile(i, carry):
                rows = pl.ds(pl.multiple_of((half * TPH + i) * 128, 128), 128)

                def scaled(r):
                    return zs[r, rows, :] * u_rows[r // NX, r % NX:r % NX + 1, :]
                acc = scaled(0)
                for r in range(1, NR):
                    acc = acc + scaled(r)
                wacc[rows, :] = acc
                return carry

            def tile_wide(i, carry):
                rows = pl.ds(pl.multiple_of((half * TPH + i) * 128, 128), 128)

                def moved(r):
                    return zs[r, rows, :] + u_rows[r // NX, r % NX:r % NX + 1, :]
                top = functools.reduce(jnp.maximum, [moved(r) for r in range(NR)])
                top = jnp.max(top, axis=1, keepdims=True)
                acc = functools.reduce(jnp.add, [jnp.exp2(moved(r) - top) for r in range(NR)])
                wacc[rows, :] = jnp.broadcast_to(top + jnp.log2(jnp.sum(acc, axis=1, keepdims=True)), (128, 128))
                return carry
            lax.fori_loop(0, TPH, tile if fast else tile_wide, 0)
            found = []
            for i in range(half * TPH, (half + 1) * TPH):
                turned = wacc[i * 128:(i + 1) * 128, :].T
                found.append(jnp.sum(turned, axis=0, keepdims=True) if fast else turned[0:1, :])
            found = jnp.concatenate(found, axis=0)
            lines = slice(half * TPH, (half + 1) * TPH)
            if fast:
                bad = bad + low(found)
                found = jnp.log2(found) + level
            c_buf[it, col, lines, :] = found - bias[lines, :]
            to_all(col_peer, NK, c_buf.at[it, col, pl.ds(half * TPH, TPH)], c_sems.at[it])
        if last:
            g_tmp[...] = whole
            fo_buf[col] = g_tmp[z, pl.ds(x, 1), :] * (-NATS)
            to_all(col_peer, NK, fo_buf.at[col], fo_sems)
        wait_bytes(c_buf.at[it], NK - 1, c_sems.at[it, 1])
        parts = [c_buf[it, c] for c in range(NK)]
        top = functools.reduce(jnp.maximum, parts)
        mapped = (top + jnp.log2(functools.reduce(jnp.add, [jnp.exp2(v - top) for v in parts]))) * (-NATS)
        images = (images + [mapped])[-HIST:]
        base = (base + [g_now])[-HIST:]
        resid = [p - q for p, q in zip(images, base)]
        prods = [jnp.sum(resid[a] * resid[b], axis=0, keepdims=True) for a, b in pairs]
        prods.append(jnp.where(line == 0, bad, 0.0))
        sums = jnp.sum(jnp.concatenate(prods, axis=0), axis=1, keepdims=True)
        r_buf[it, row] = jnp.sum(jnp.where(eye, sums, 0.0), axis=0, keepdims=True)
        to_all(row_peer, NR, r_buf.at[it, row], r_sems.at[it])
        wait_bytes(r_buf.at[it], NR - 1, r_sems.at[it, 1])
        flat = functools.reduce(jnp.add, [r_buf[it, r] for r in range(NR)])

        def entry(k):
            return jnp.sum(jnp.where(line == k, flat, 0.0), axis=1, keepdims=True)
        mix = solve({ab: entry(k) for k, ab in enumerate(pairs)})
        g_next = functools.reduce(jnp.add, [v * m for v, m in zip(images, mix)])
        if last:
            hist[0] = g_next
            for q in range(TW // 128):
                gout_ref[q:q + 1, :] = hist[0, pl.ds(col * (TW // 128) + q, 1), :]
            flag_ref[...] = jnp.broadcast_to(entry(len(pairs)), (1, 128))
        else:
            delta = (g_next - g_now) * BITS
            if fast:
                shift = all_of(delta, jnp.max)
                delta = jnp.exp2(delta - shift)
            for t in range(NT):
                vrep[t * 128:(t + 1) * 128, :] = jnp.broadcast_to(delta[t:t + 1, :], (128, 128)).T
            g_now = g_next

    wait_bytes(fo_buf, NK - 1, fo_sems.at[1])
    for c in range(NK):
        f_ref[c:c + 1, :] = fo_buf[c]
    wait_bytes(src_all, NR - 1, src_send)
    wait_bytes(tgt_all, NK - 1, tgt_send)
    wait_bytes(fo_buf, NK - 1, fo_sems.at[0])
    for it in range(ITERS):
        wait_bytes(f_buf.at[it], NR - 1, f_sems.at[it, 0])
        wait_bytes(c_buf.at[it], NK - 1, c_sems.at[it, 0])
        wait_bytes(r_buf.at[it], NR - 1, r_sems.at[it, 0])


def shards(dims, src, tgt, log_a, log_b, g, hist_g, hist_maps):
    NZ, NX, NY, NC = dims
    NR, NK = NZ * NX, NY * NC
    D, SW = src.shape
    TW = tgt.shape[1]
    COLS = NK * TW
    NT = COLS // 128
    f32 = jnp.float32
    vmem = pl.BlockSpec(memory_space=pltpu.VMEM)
    dma = pltpu.SemaphoreType.DMA

    def call(fast):
        return pl.pallas_call(
            functools.partial(kernel, fast, dims),
            out_shape=(
                jax.ShapeDtypeStruct((NK, SW), f32),
                jax.ShapeDtypeStruct((TW // 128, 128), f32),
                jax.ShapeDtypeStruct((1, 128), f32),
            ),
            in_specs=[pl.BlockSpec(memory_space=pltpu.HBM)] * 7,
            out_specs=(vmem, vmem, vmem),
            scratch_shapes=[
                pltpu.VMEM((NR, D + 8, SW), f32),
                pltpu.VMEM((NK, D + 16, TW), f32),
                pltpu.VMEM((NK, SW), f32),
                pltpu.VMEM((1, TW), f32),
                pltpu.VMEM((1, TW), f32),
                pltpu.VMEM((HIST - 1, TW), f32),
                pltpu.VMEM((HIST - 1, TW), f32),
                pltpu.VMEM((COLS, 4 * D), jnp.bfloat16),
                pltpu.VMEM((COLS, 2 * SW), f32),
                pltpu.VMEM((2, 1, SW), f32),
                pltpu.VMEM((NR, COLS, SW), f32),
                pltpu.VMEM((COLS, 128), f32),
                pltpu.VMEM((COLS, 128), f32),
                pltpu.VMEM((2 * HIST, NT, 128), f32),
                pltpu.VMEM((NZ, NX, SW), f32),
                pltpu.VMEM((NZ, NX, SW), f32),
                pltpu.VMEM((NZ, NX, SW), f32),
                pltpu.VMEM((NZ, NX, SW), f32),
                pltpu.VMEM((ITERS, NR, NZ, NX, SW), f32),
                pltpu.VMEM((NK, 1, SW), f32),
                pltpu.VMEM((ITERS, NK, NT, 128), f32),
                pltpu.VMEM((ITERS, NR, 1, 128), f32),
                dma((7,)), dma, dma((2, 2, NR)), dma, dma((2, NK)),
                dma((ITERS, 2)), dma((2,)), dma((ITERS, 2)), dma((ITERS, 2)),
            ],
            compiler_params=pltpu.CompilerParams(
                collective_id=0 if fast else 1, has_side_effects=True, vmem_limit_bytes=48 * 1024 * 1024
            ),
            name="sinkhorn" if fast else "sinkhorn_wide",
        )(src, tgt, log_a.reshape(NK, SW), log_b.reshape(NR, 1, TW), g.reshape(1, TW), hist_g, hist_maps)

    f, gout, flag = call(True)
    f, gout = lax.cond(flag[0, 0] > 0.5, lambda: call(False)[:2], lambda: (f, gout))
    return f.reshape(-1), gout.reshape(-1)


def solution(mesh, dims=(4, 4, 4, 2)):
    grid = Mesh(mesh.devices.reshape(dims), AXES)
    in_specs = (
        P(None, AXES),
        P(None, ("y", "core", "z", "x")),
        P(("z", "x")),
        P(("y", "core")),
        P(("y", "core", "z", "x")),
        P(None, ("y", "core", "z", "x")),
        P(None, ("y", "core", "z", "x")),
    )
    out_specs = (P(("z", "x")), P(("y", "core", "z", "x")))
    return jax.shard_map(
        functools.partial(shards, dims), mesh=grid, in_specs=in_specs, out_specs=out_specs, check_vma=False
    )
```

```python
import functools

import jax
import jax.numpy as jnp
from jax import lax
from jax.experimental import pallas as pl
from jax.experimental.pallas import tpu as pltpu
from jax.sharding import Mesh
from jax.sharding import PartitionSpec as P

HIST = 5
ITERS = 2
EPS = 0.1
LOG2E = 1.4426950408889634
BITS = LOG2E / EPS
NATS = EPS / LOG2E
LEAST_BITS = -97.0
SMALLEST = 2.0**LEAST_BITS
MESH = pl.DeviceIdType.MESH
AXES = ("z", "x", "y", "core")


def split2(v):
    hi = v.astype(jnp.bfloat16).astype(jnp.float32)
    return hi, v - hi


def split3(v):
    hi = v.astype(jnp.bfloat16).astype(jnp.float32)
    rest = v - hi
    mid = rest.astype(jnp.bfloat16).astype(jnp.float32)
    return hi, mid, rest - mid


def placed(rows, values, width):
    at = lax.broadcasted_iota(jnp.int32, (rows, width), 0)
    out = jnp.zeros((rows, width), jnp.float32)
    for k, v in enumerate(values):
        out = jnp.where(at == k, v, out)
    return out


def solve(gram):
    n = HIST
    trace = gram[0, 0]
    for k in range(1, n):
        trace = trace + gram[k, k]
    shift = 0.001 * trace / n + 1e-6
    a = [[gram[min(p, q), max(p, q)] + (shift if p == q else 0.0) for q in range(n)] for p in range(n)]
    rhs = [jnp.ones((1, 1), jnp.float32) for _ in range(n)]
    for p in range(n):
        for low in range(p + 1, n):
            factor = a[low][p] / a[p][p]
            for q in range(p + 1, n):
                a[low][q] = a[low][q] - factor * a[p][q]
            rhs[low] = rhs[low] - factor * rhs[p]
    out = [None] * n
    for p in reversed(range(n)):
        acc = rhs[p]
        for q in range(p + 1, n):
            acc = acc - a[p][q] * out[q]
        out[p] = acc / a[p][p]
    total = out[0]
    for k in range(1, n):
        total = total + out[k]
    return [o / total for o in out]


def kernel(
    fast, dims,
    src_hbm, tgt_hbm, loga_hbm, logb_hbm, g_hbm, hg_hbm, hm_hbm,
    f_ref, gout_ref, flag_ref,
    src_all, tgt_all, loga_in, logb_in, g_in, hg_in, hm_in,
    left, right, staged, tops_buf, zs, wacc, vrep, hist, m_rows, a_rows, u_rows, g_tmp,
    f_buf, fo_buf, c_buf, r_buf,
    in_sems, src_send, src_recv, tgt_send, tgt_recv, f_sems, fo_sems, c_sems, r_sems,
):
    NZ, NX, NY, NC = dims
    SIZE = dict(zip(AXES, dims))
    NR, NK = NZ * NX, NY * NC
    D, SW = src_hbm.shape
    TW = tgt_hbm.shape[1]
    COLS = NK * TW
    NT = COLS // 128
    at = {name: lax.axis_index(name) for name in AXES}
    z, x, y, core = (at[name] for name in AXES)
    row, col = z * NX + x, y * NC + core

    def row_peer(k):
        p = lax.rem(row + k, NR)
        return {"z": p // NX, "x": lax.rem(p, NX)}

    def col_peer(k):
        p = lax.rem(col + k, NK)
        return {"y": p // NC, "core": lax.rem(p, NC)}

    def near(axis, d):
        return {axis: lax.rem(at[axis] + d + SIZE[axis], SIZE[axis])}

    def remote(part, ssem, rsem, peer):
        pltpu.make_async_remote_copy(
            src_ref=part, dst_ref=part, send_sem=ssem, recv_sem=rsem, device_id=peer, device_id_type=MESH
        ).start()

    def to_all(peer, count, part, sems):
        for k in range(1, count):
            remote(part, sems.at[0], sems.at[1], peer(k))

    def wait_for(part, sem):
        pltpu.make_async_copy(part, part, sem).wait()

    def wait_bytes(buf, count, sem):
        if count:
            wait_for(buf.at[pl.ds(0, count)], sem)

    barrier = pltpu.get_barrier_semaphore()
    around = [(name, d) for name in ("x", "z", "y") if SIZE[name] > 1 for d in (1, -1)]
    if NC > 1:
        around.append(("core", 1))
    for name, d in around:
        pl.semaphore_signal(barrier, inc=1, device_id=near(name, d), device_id_type=MESH)

    moves = [
        (src_hbm, src_all.at[row, pl.ds(0, D)]), (tgt_hbm, tgt_all.at[col, pl.ds(0, D)]), (loga_hbm, loga_in),
        (logb_hbm.at[row], logb_in), (g_hbm, g_in), (hm_hbm, hm_in), (hg_hbm, hg_in),
    ]
    moves = [pltpu.make_async_copy(s, d, in_sems.at[k]) for k, (s, d) in enumerate(moves)]
    for m in moves:
        m.start()
    for m in moves:
        m.wait()
    KEPT = HIST - 1
    src_all[row, D:D + 8, :] = placed(8, [loga_in[pl.ds(col, 1), :]], SW)
    tgt_all[col, D:D + 16, :] = placed(
        16, [g_in[...], logb_in[...]] + [hm_in[k:k + 1, :] for k in range(KEPT)]
        + [hg_in[k:k + 1, :] for k in range(KEPT)], TW
    )
    pl.semaphore_wait(barrier, len(around))

    HALF, QUART, EXTRA = D // 2, D // 4, 8
    PIECES = (((0, QUART), (QUART, QUART)), ((HALF, QUART + EXTRA), (HALF + QUART + EXTRA, QUART)))
    ORDER = (("x", "z"), ("z", "x"))
    seen = set()

    def slot_of(dz, dx):
        return lax.rem(z + dz + NZ, NZ) * NX + lax.rem(x + dx + NX, NX)

    def piece(r, h, sub):
        start, count = PIECES[h][sub]
        return src_all.at[r, pl.ds(start, count)]

    def pass_on(r, h, sub, axis, d):
        remote(piece(r, h, sub), src_send, src_recv.at[h, sub, r], near(axis, d))

    def part_for(d):
        return 0 if d < 0 else 1

    def start_sources():
        for phase in (0, 1):
            for first in (True, False):
                for h in (0, 1):
                    axis = ORDER[h][phase]
                    if SIZE[axis] > 1:
                        for d in (1, -1):
                            pass_on(row, h, part_for(-d) if first else part_for(d), axis, d)

    def arrived(h, da, db, sub):
        a, b = ORDER[h]
        if (h, da, db, sub) in seen or (da == 0 and db == 0):
            return
        seen.add((h, da, db, sub))
        r = slot_of(**{"d" + a: da, "d" + b: db})
        wait_for(piece(r, h, sub), src_recv.at[h, sub, r])
        if db == 0:
            if da in (1, -1) and sub == part_for(da):
                pass_on(r, h, sub, a, -da)
            for d in (1, -1):
                pass_on(r, h, sub, b, d)
        elif db in (1, -1) and sub == part_for(db):
            pass_on(r, h, sub, b, -db)

    def complete(*blocks):
        for dz, dx in blocks:
            for h in (0, 1):
                da, db = (dx, dz) if h == 0 else (dz, dx)
                for sub in (0, 1):
                    arrived(h, da, db, sub)

    THALF = (D + 16) // 2

    def target(c, sub):
        return tgt_all.at[c, pl.ds(sub * THALF, THALF)]

    def tgt_slot(dy, other=0):
        return lax.rem(y + dy + NY, NY) * NC + lax.rem(core + other, NC)

    def tgt_pass(c, sub, axis, d):
        remote(target(c, sub), tgt_send, tgt_recv.at[sub, c], near(axis, d))

    def start_targets():
        if NY > 1:
            for first in (True, False):
                for d in (1, -1):
                    tgt_pass(col, part_for(-d) if first else part_for(d), "y", d)
        if NC > 1:
            for sub in (0, 1):
                tgt_pass(col, sub, "core", 1)

    def tgt_arrived(dy, sub):
        c = tgt_slot(dy)
        wait_for(target(c, sub), tgt_recv.at[sub, c])
        if dy in (1, -1) and sub == part_for(dy):
            tgt_pass(c, sub, "y", -dy)
        if NC > 1:
            tgt_pass(c, sub, "core", 1)

    def take_targets(c):
        v = tgt_all[c, 0:D, :]
        norm = jnp.sum(v * v, axis=0, keepdims=True) * (-BITS)
        b = tgt_all[c, D:D + 1, :] * BITS + tgt_all[c, D + 1:D + 2, :] * LOG2E
        hi, lo = split2(v)
        one = jnp.ones((1, TW), jnp.float32)
        tail = placed(D, list(split3(norm)) + list(split3(b)) + [one] * 3, TW)
        full = jnp.concatenate([hi, lo, hi, tail], axis=0)
        left[pl.ds(pl.multiple_of(c * TW, TW), TW), :] = full.T.astype(jnp.bfloat16)

    def take_sources(r):
        v = src_all[r, 0:D, :]
        norm = jnp.sum(v * v, axis=0, keepdims=True) * (-BITS)
        hi, lo = split2(v * (2.0 * BITS))
        one = jnp.ones((1, SW), jnp.float32)
        tail = placed(D, [one] * 6 + list(split3(norm)), SW)
        right[r] = jnp.concatenate([hi, hi, lo, tail], axis=0).astype(jnp.bfloat16)

    QB = min(512, COLS)
    EB = min(256, COLS)

    def spots_of(offsets):
        return [(lax.rem(z + dz + 8 * NZ, NZ), lax.rem(x + dx + 8 * NX, NX)) for dz, dx in offsets]

    def folded(v, op):
        return op(v.reshape(v.shape[0] // 8, 8, v.shape[1]), axis=0)

    def step(done, new):
        if new:
            operand = jnp.concatenate([right[zb * NX + xb] for zb, xb in new], axis=1)
        tops, sums = [None] * len(new), [None] * len(done)
        before = [tops_buf[n] for n in range(len(done))]
        for q in range(COLS // QB):
            rows = slice(q * QB, (q + 1) * QB)
            for n, (zb, xb) in enumerate(done):
                e = jnp.exp2(staged[rows, n * SW:(n + 1) * SW] - before[n])
                if fast:
                    zs[zb * NX + xb, rows, :] = e
                else:
                    zs[zb * NX + xb, rows, :] = staged[rows, n * SW:(n + 1) * SW]
                e = folded(e, jnp.sum)
                sums[n] = e if q == 0 else sums[n] + e
            if new:
                t = jnp.dot(left[rows, :], operand, preferred_element_type=jnp.float32)
                staged[rows, 0:len(new) * SW] = t
                for n in range(len(new)):
                    top = folded(t[:, n * SW:(n + 1) * SW], jnp.max)
                    tops[n] = top if q == 0 else jnp.maximum(tops[n], top)
        for n, (zb, xb) in enumerate(done):
            f_buf[0, row, zb, pl.ds(xb, 1), :] = before[n] + jnp.log2(jnp.sum(sums[n], axis=0, keepdims=True))
            m_rows[zb, pl.ds(xb, 1), :] = before[n]
            a_rows[zb, pl.ds(xb, 1), :] = src_all[zb * NX + xb, D:D + 1, :] * LOG2E
        for n in range(len(new)):
            tops_buf[n] = jnp.max(tops[n], axis=0, keepdims=True)

    TURNS = (
        ((0, 1), (0, -1)), ((1, 0), (-1, 0)), ((1, 1), (-1, 1)), ((1, -1), (-1, -1)), ((0, 0), (0, 2)),
        ((1, 2), (-1, 2)), ((2, 1), (2, -1)), ((2, 0), (2, 2)),
    ) if NZ > 1 and NX > 1 else (((0, 0),),)

    def turn(k):
        out = TURNS[0]
        for t in range(1, len(TURNS)):
            out = tuple(tuple(jnp.where(k == t, v, w) for v, w in zip(*pair)) for pair in zip(TURNS[t], out))
        return spots_of(out)

    def ready(*turns):
        for t in turns:
            complete(*TURNS[t])
            for zb, xb in spots_of(TURNS[t]):
                take_sources(zb * NX + xb)

    def send_f(it, zb):
        to_all(row_peer, NR, f_buf.at[it, row, zb], f_sems.at[it])

    both = NZ > 1 and NX > 1
    start_sources()
    start_targets()
    take_targets(col)
    if both:
        for h in (0, 1):
            for d in (1, -1):
                arrived(h, d, 0, part_for(d))
        for h in (0, 1):
            for d in (1, -1):
                arrived(h, d, 0, part_for(-d))
    if NY > 1:
        for d in (1, -1):
            tgt_arrived(d, part_for(d))
        for d in (1, -1):
            tgt_arrived(d, part_for(-d))
    if both:
        for h in (0, 1):
            for d in (1, -1):
                arrived(h, 0, d, part_for(d))
    if both:
        for h in (0, 1):
            for sub in (0, 1):
                arrived(h, 2, 0, sub)
            for da in (1, -1):
                for db in (1, -1):
                    arrived(h, da, db, part_for(db))
        ready(0, 1)
    else:
        ready(0)
    if NY > 1:
        for sub in (0, 1):
            tgt_arrived(2, sub)
        for dy in (1, -1, 2):
            take_targets(tgt_slot(dy))
    if NC > 1:
        for dy in ((0, 1, -1, 2) if NY > 1 else (0,)):
            c = tgt_slot(dy, 1)
            for sub in (0, 1):
                wait_for(target(c, sub), tgt_recv.at[sub, c])
            take_targets(c)
    if both:
        complete((0, 1), (0, -1), (1, 0), (-1, 0))
    if both:
        def stage(k, carry):
            @pl.when(k == 2)
            def _():
                for h in (0, 1):
                    for db in (1, -1):
                        arrived(h, 2, db, part_for(db))
            for t in range(2, len(TURNS)):
                @pl.when(k == t)
                def _(t=t):
                    ready(t)
            step(turn(jnp.maximum(k - 1, 0)), turn(k))

            @pl.when(k == 5)
            def _():
                send_f(0, z)

            @pl.when(k == 6)
            def _():
                for d in (1, 3):
                    send_f(0, lax.rem(z + d, NZ))
            return carry
        lax.fori_loop(0, len(TURNS) + 1, stage, 0)
    else:
        step([], spots_of(TURNS[0]))
        step(spots_of(TURNS[0]), [])
    send_f(0, lax.rem(z + NZ // 2, NZ))
    for c in range(NK):
        for k in range(2 * KEPT + 2):
            for q in range(TW // 128):
                t = c * (TW // 128) + q
                hist[k, t:t + 1, :] = tgt_all[c, D + k:D + k + 1, q * 128:(q + 1) * 128]

    bad = jnp.zeros((1, 1), jnp.float32)
    g_now = hist[0]
    bias = g_now * BITS + hist[1] * LOG2E
    images = [hist[2 + k] for k in range(KEPT)]
    base = [hist[2 + KEPT + k] for k in range(KEPT)]
    shift = jnp.zeros((1, 1), jnp.float32)
    pairs = [(a, b) for a in range(HIST) for b in range(a, HIST)]
    line = lax.broadcasted_iota(jnp.int32, (1, 128), 1)
    eye = (lax.broadcasted_iota(jnp.int32, (16, 128), 0) == lax.broadcasted_iota(jnp.int32, (16, 128), 1))

    def all_of(v, op):
        return op(op(v, axis=0, keepdims=True), axis=1, keepdims=True)

    def low(v):
        return all_of(jnp.where(v >= SMALLEST, 0.0, 1.0), jnp.max)

    for it in range(ITERS):
        last = it == ITERS - 1
        if it and fast:
            GZ = min(2, NZ)
            SB = min(128, COLS)
            for zg in range(0, NZ, GZ):
                spots = [(zz, xx) for zz in range(zg, zg + GZ) for xx in range(NX)]

                def weigh(i, acc):
                    rows = pl.ds(pl.multiple_of(i * SB, SB), SB)
                    v = vrep[rows, :]
                    return tuple(
                        a + jnp.sum((zs[zz * NX + xx, rows, :] * v).reshape(SB // 8, 8, SW), axis=0)
                        for a, (zz, xx) in zip(acc, spots)
                    )
                found = lax.fori_loop(0, COLS // SB, weigh, tuple(jnp.zeros((8, SW), jnp.float32) for _ in spots))
                found = [jnp.sum(v, axis=0, keepdims=True) for v in found]
                for zz in range(zg, zg + GZ):
                    s = jnp.concatenate(found[(zz - zg) * NX:(zz - zg + 1) * NX], axis=0)
                    bad = bad + low(s)
                    f_buf[it, row, zz] = m_rows[zz] + shift + jnp.log2(s)
                for zz in range(zg, zg + GZ):
                    send_f(it, zz)
        elif it:
            def again(r, carry):
                def tops_of(i, acc):
                    rows = pl.ds(pl.multiple_of(i * EB, EB), EB)
                    v = zs[r, rows, :] + vrep[rows, :]
                    return jnp.maximum(acc, jnp.max(v.reshape(EB // 8, 8, SW), axis=0))
                top = lax.fori_loop(0, COLS // EB, tops_of, jnp.full((8, SW), -jnp.inf, jnp.float32))
                top = jnp.max(top, axis=0, keepdims=True)

                def sums_of(i, acc):
                    rows = pl.ds(pl.multiple_of(i * EB, EB), EB)
                    v = jnp.exp2((zs[r, rows, :] + vrep[rows, :]) - top)
                    return acc + jnp.sum(v.reshape(EB // 8, 8, SW), axis=0)
                s = lax.fori_loop(0, COLS // EB, sums_of, jnp.zeros((8, SW), jnp.float32))
                f_buf[it, row, r // NX, pl.ds(lax.rem(r, NX), 1), :] = top + jnp.log2(
                    jnp.sum(s, axis=0, keepdims=True))
                return carry
            lax.fori_loop(0, NR, again, 0)
            for zz in range(NZ):
                send_f(it, zz)
        wait_bytes(f_buf.at[it], NR - 1, f_sems.at[it, 1])
        parts = [f_buf[it, r] for r in range(NR)]
        top = functools.reduce(jnp.maximum, parts)
        whole = top + jnp.log2(functools.reduce(jnp.add, [jnp.exp2(v - top) for v in parts]))
        term = a_rows[...] - whole
        level = jnp.zeros((1, 1), jnp.float32)
        if fast:
            term = term + m_rows[...]
            level = all_of(jnp.max(term, axis=0), jnp.max)
            u_rows[...] = jnp.exp2(term - level[None])
        else:
            u_rows[...] = term
        TPH = max(NT // 2, 1)
        for half in range(NT // TPH):
            def tile(i, carry):
                rows = pl.ds(pl.multiple_of((half * TPH + i) * 128, 128), 128)

                def scaled(r):
                    return zs[r, rows, :] * u_rows[r // NX, r % NX:r % NX + 1, :]
                acc = scaled(0)
                for r in range(1, NR):
                    acc = acc + scaled(r)
                wacc[rows, :] = acc
                return carry

            def tile_wide(i, carry):
                rows = pl.ds(pl.multiple_of((half * TPH + i) * 128, 128), 128)

                def moved(r):
                    return zs[r, rows, :] + u_rows[r // NX, r % NX:r % NX + 1, :]
                top = functools.reduce(jnp.maximum, [moved(r) for r in range(NR)])
                top = jnp.max(top, axis=1, keepdims=True)
                acc = functools.reduce(jnp.add, [jnp.exp2(moved(r) - top) for r in range(NR)])
                wacc[rows, :] = jnp.broadcast_to(top + jnp.log2(jnp.sum(acc, axis=1, keepdims=True)), (128, 128))
                return carry
            lax.fori_loop(0, TPH, tile if fast else tile_wide, 0)
            found = []
            for i in range(half * TPH, (half + 1) * TPH):
                turned = wacc[i * 128:(i + 1) * 128, :].T
                found.append(jnp.sum(turned, axis=0, keepdims=True) if fast else turned[0:1, :])
            found = jnp.concatenate(found, axis=0)
            lines = slice(half * TPH, (half + 1) * TPH)
            if fast:
                bad = bad + low(found)
                found = jnp.log2(found) + level
            c_buf[it, col, lines, :] = found - bias[lines, :]
            to_all(col_peer, NK, c_buf.at[it, col, pl.ds(half * TPH, TPH)], c_sems.at[it])
        if last:
            g_tmp[...] = whole
            fo_buf[col] = g_tmp[z, pl.ds(x, 1), :] * (-NATS)
            to_all(col_peer, NK, fo_buf.at[col], fo_sems)
        wait_bytes(c_buf.at[it], NK - 1, c_sems.at[it, 1])
        parts = [c_buf[it, c] for c in range(NK)]
        top = functools.reduce(jnp.maximum, parts)
        mapped = (top + jnp.log2(functools.reduce(jnp.add, [jnp.exp2(v - top) for v in parts]))) * (-NATS)
        images = (images + [mapped])[-HIST:]
        base = (base + [g_now])[-HIST:]
        resid = [p - q for p, q in zip(images, base)]
        prods = [jnp.sum(resid[a] * resid[b], axis=0, keepdims=True) for a, b in pairs]
        prods.append(jnp.where(line == 0, bad, 0.0))
        sums = jnp.sum(jnp.concatenate(prods, axis=0), axis=1, keepdims=True)
        r_buf[it, row] = jnp.sum(jnp.where(eye, sums, 0.0), axis=0, keepdims=True)
        to_all(row_peer, NR, r_buf.at[it, row], r_sems.at[it])
        wait_bytes(r_buf.at[it], NR - 1, r_sems.at[it, 1])
        flat = functools.reduce(jnp.add, [r_buf[it, r] for r in range(NR)])

        def entry(k):
            return jnp.sum(jnp.where(line == k, flat, 0.0), axis=1, keepdims=True)
        mix = solve({ab: entry(k) for k, ab in enumerate(pairs)})
        g_next = functools.reduce(jnp.add, [v * m for v, m in zip(images, mix)])
        if last:
            hist[0] = g_next
            for q in range(TW // 128):
                gout_ref[q:q + 1, :] = hist[0, pl.ds(col * (TW // 128) + q, 1), :]
            flag_ref[...] = jnp.broadcast_to(entry(len(pairs)), (1, 128))
        else:
            delta = (g_next - g_now) * BITS
            if fast:
                shift = all_of(delta, jnp.max)
                delta = jnp.exp2(delta - shift)
            for t in range(NT):
                vrep[t * 128:(t + 1) * 128, :] = jnp.broadcast_to(delta[t:t + 1, :], (128, 128)).T
            g_now = g_next

    wait_bytes(fo_buf, NK - 1, fo_sems.at[1])
    for c in range(NK):
        f_ref[c:c + 1, :] = fo_buf[c]
    wait_bytes(src_all, NR - 1, src_send)
    wait_bytes(tgt_all, NK - 1, tgt_send)
    wait_bytes(fo_buf, NK - 1, fo_sems.at[0])
    for it in range(ITERS):
        wait_bytes(f_buf.at[it], NR - 1, f_sems.at[it, 0])
        wait_bytes(c_buf.at[it], NK - 1, c_sems.at[it, 0])
        wait_bytes(r_buf.at[it], NR - 1, r_sems.at[it, 0])


def shards(dims, src, tgt, log_a, log_b, g, hist_g, hist_maps):
    NZ, NX, NY, NC = dims
    NR, NK = NZ * NX, NY * NC
    D, SW = src.shape
    TW = tgt.shape[1]
    COLS = NK * TW
    NT = COLS // 128
    f32 = jnp.float32
    vmem = pl.BlockSpec(memory_space=pltpu.VMEM)
    dma = pltpu.SemaphoreType.DMA

    def call(fast):
        return pl.pallas_call(
            functools.partial(kernel, fast, dims),
            out_shape=(
                jax.ShapeDtypeStruct((NK, SW), f32),
                jax.ShapeDtypeStruct((TW // 128, 128), f32),
                jax.ShapeDtypeStruct((1, 128), f32),
            ),
            in_specs=[pl.BlockSpec(memory_space=pltpu.HBM)] * 7,
            out_specs=(vmem,) * 3,
            scratch_shapes=[
                pltpu.VMEM((NR, D + 8, SW), f32),
                pltpu.VMEM((NK, D + 16, TW), f32),
                pltpu.VMEM((NK, SW), f32),
                pltpu.VMEM((1, TW), f32),
                pltpu.VMEM((1, TW), f32),
                pltpu.VMEM((HIST - 1, TW), f32),
                pltpu.VMEM((HIST - 1, TW), f32),
                pltpu.VMEM((COLS, 4 * D), jnp.bfloat16),
                pltpu.VMEM((NR, 4 * D, SW), jnp.bfloat16),
                pltpu.VMEM((COLS, 2 * SW), f32),
                pltpu.VMEM((2, 1, SW), f32),
                pltpu.VMEM((NR, COLS, SW), f32),
                pltpu.VMEM((COLS, 128), f32),
                pltpu.VMEM((COLS, 128), f32),
                pltpu.VMEM((2 * HIST, NT, 128), f32),
                pltpu.VMEM((NZ, NX, SW), f32),
                pltpu.VMEM((NZ, NX, SW), f32),
                pltpu.VMEM((NZ, NX, SW), f32),
                pltpu.VMEM((NZ, NX, SW), f32),
                pltpu.VMEM((ITERS, NR, NZ, NX, SW), f32),
                pltpu.VMEM((NK, 1, SW), f32),
                pltpu.VMEM((ITERS, NK, NT, 128), f32),
                pltpu.VMEM((ITERS, NR, 1, 128), f32),
                dma((7,)), dma, dma((2, 2, NR)), dma, dma((2, NK)),
                dma((ITERS, 2)), dma((2,)), dma((ITERS, 2)), dma((ITERS, 2)),
            ],
            compiler_params=pltpu.CompilerParams(
                collective_id=0 if fast else 1, has_side_effects=True,
                vmem_limit_bytes=48 * 1024 * 1024
            ),
            name="sinkhorn" if fast else "sinkhorn_wide",
        )(src, tgt, log_a.reshape(NK, SW), log_b.reshape(NR, 1, TW), g.reshape(1, TW), hist_g, hist_maps)

    f, gout, flag = call(True)
    f, gout = lax.cond(flag[0, 0] > 0.5, lambda: call(False)[:2], lambda: (f, gout))
    return f.reshape(-1), gout.reshape(-1)


def solution(mesh, dims=(4, 4, 4, 2)):
    grid = Mesh(mesh.devices.reshape(dims), AXES)
    in_specs = (
        P(None, AXES),
        P(None, ("y", "core", "z", "x")),
        P(("z", "x")),
        P(("y", "core")),
        P(("y", "core", "z", "x")),
        P(None, ("y", "core", "z", "x")),
        P(None, ("y", "core", "z", "x")),
    )
    out_specs = (P(("z", "x")), P(("y", "core", "z", "x")))
    return jax.shard_map(
        functools.partial(shards, dims), mesh=grid, in_specs=in_specs, out_specs=out_specs, check_vma=False
    )
```

```python
import functools

import jax
import jax.numpy as jnp
from jax import lax
from jax.experimental import pallas as pl
from jax.experimental.pallas import tpu as pltpu
from jax.sharding import Mesh
from jax.sharding import PartitionSpec as P

HIST = 5
ITERS = 2
EPS = 0.1
LOG2E = 1.4426950408889634
BITS = LOG2E / EPS
NATS = EPS / LOG2E
LEAST_BITS = -97.0
SMALLEST = 2.0**LEAST_BITS
MESH = pl.DeviceIdType.MESH
AXES = ("z", "x", "y", "core")


def split2(v):
    hi = v.astype(jnp.bfloat16).astype(jnp.float32)
    return hi, v - hi


def split3(v):
    hi = v.astype(jnp.bfloat16).astype(jnp.float32)
    rest = v - hi
    mid = rest.astype(jnp.bfloat16).astype(jnp.float32)
    return hi, mid, rest - mid


def placed(rows, values, width):
    at = lax.broadcasted_iota(jnp.int32, (rows, width), 0)
    out = jnp.zeros((rows, width), jnp.float32)
    for k, v in enumerate(values):
        out = jnp.where(at == k, v, out)
    return out


def solve(gram):
    n = HIST
    trace = gram[0, 0]
    for k in range(1, n):
        trace = trace + gram[k, k]
    shift = 0.001 * trace / n + 1e-6
    a = [[gram[min(p, q), max(p, q)] + (shift if p == q else 0.0) for q in range(n)] for p in range(n)]
    rhs = [jnp.ones((1, 1), jnp.float32) for _ in range(n)]
    for p in range(n):
        for low in range(p + 1, n):
            factor = a[low][p] / a[p][p]
            for q in range(p + 1, n):
                a[low][q] = a[low][q] - factor * a[p][q]
            rhs[low] = rhs[low] - factor * rhs[p]
    out = [None] * n
    for p in reversed(range(n)):
        acc = rhs[p]
        for q in range(p + 1, n):
            acc = acc - a[p][q] * out[q]
        out[p] = acc / a[p][p]
    total = out[0]
    for k in range(1, n):
        total = total + out[k]
    return [o / total for o in out]


def kernel(
    fast, dims,
    src_hbm, tgt_hbm, loga_hbm, logb_hbm, g_hbm, hg_hbm, hm_hbm,
    f_ref, gout_ref, flag_ref,
    src_all, tgt_all, a_all, old_all, loga_in, logb_in, g_in, hg_in, hm_in,
    left, right, staged, tops_buf, zs, wacc, vrep, hist, m_rows, a_rows, u_rows, g_tmp,
    f_buf, fo_buf, c_buf, r_buf,
    in_sems, a_sems, old_sems, src_send, src_recv, tgt_send, tgt_recv, f_sems, fo_sems, c_sems, r_sems,
):
    NZ, NX, NY, NC = dims
    SIZE = dict(zip(AXES, dims))
    NR, NK = NZ * NX, NY * NC
    D, SW = src_hbm.shape
    TW = tgt_hbm.shape[1]
    COLS = NK * TW
    NT = COLS // 128
    at = {name: lax.axis_index(name) for name in AXES}
    z, x, y, core = (at[name] for name in AXES)
    row, col = z * NX + x, y * NC + core

    def row_peer(k):
        p = lax.rem(row + k, NR)
        return {"z": p // NX, "x": lax.rem(p, NX)}

    def col_peer(k):
        p = lax.rem(col + k, NK)
        return {"y": p // NC, "core": lax.rem(p, NC)}

    def near(axis, d):
        return {axis: lax.rem(at[axis] + d + SIZE[axis], SIZE[axis])}

    def remote(part, ssem, rsem, peer):
        pltpu.make_async_remote_copy(
            src_ref=part, dst_ref=part, send_sem=ssem, recv_sem=rsem, device_id=peer, device_id_type=MESH
        ).start()

    def to_all(peer, count, part, sems):
        for k in range(1, count):
            remote(part, sems.at[0], sems.at[1], peer(k))

    def wait_for(part, sem):
        pltpu.make_async_copy(part, part, sem).wait()

    def wait_bytes(buf, count, sem):
        if count:
            wait_for(buf.at[pl.ds(0, count)], sem)

    barrier = pltpu.get_barrier_semaphore()
    around = [(name, d) for name in ("x", "z", "y") if SIZE[name] > 1 for d in (1, -1)]
    if NC > 1:
        around.append(("core", 1))
    for name, d in around:
        pl.semaphore_signal(barrier, inc=1, device_id=near(name, d), device_id_type=MESH)

    greeted = len(around)
    if NC > 1 and NY > 1:
        for d in (1, -1):
            to = {"y": lax.rem(y + d + NY, NY), "core": lax.rem(core + 1, NC)}
            pl.semaphore_signal(barrier, inc=1, device_id=to, device_id_type=MESH)
        greeted += 2

    moves = [
        (src_hbm, src_all.at[row]), (tgt_hbm, tgt_all.at[col, pl.ds(0, D)]), (loga_hbm, loga_in),
        (logb_hbm.at[row], logb_in), (g_hbm, g_in), (hm_hbm, hm_in), (hg_hbm, hg_in),
    ]
    moves = [pltpu.make_async_copy(s, d, in_sems.at[k]) for k, (s, d) in enumerate(moves)]
    for m in moves:
        m.start()
    for m in moves:
        m.wait()
    KEPT = HIST - 1
    a_all[row] = loga_in[pl.ds(col, 1), :]
    tgt_all[col, D:D + 8, :] = placed(8, [g_in[...], logb_in[...]], TW)
    old_all[col] = jnp.concatenate([hm_in[...], hg_in[...]], axis=0)
    pl.semaphore_wait(barrier, greeted)

    HALF, QUART = D // 2, D // 4
    PIECES = (((0, QUART), (QUART, QUART)), ((HALF, QUART), (HALF + QUART, QUART)))
    ORDER = (("x", "z"), ("z", "x"))
    seen = set()

    def slot_of(dz, dx):
        return lax.rem(z + dz + NZ, NZ) * NX + lax.rem(x + dx + NX, NX)

    def piece(r, h, sub):
        start, count = PIECES[h][sub]
        return src_all.at[r, pl.ds(start, count)]

    def pass_on(r, h, sub, axis, d):
        remote(piece(r, h, sub), src_send, src_recv.at[h, sub, r], near(axis, d))

    def part_for(d):
        return 0 if d < 0 else 1

    def start_sources():
        for phase in (0, 1):
            for first in (True, False):
                for h in (0, 1):
                    axis = ORDER[h][phase]
                    if SIZE[axis] > 1:
                        for d in (1, -1):
                            pass_on(row, h, part_for(-d) if first else part_for(d), axis, d)

    def arrived(h, da, db, sub):
        a, b = ORDER[h]
        if (h, da, db, sub) in seen or (da == 0 and db == 0):
            return
        seen.add((h, da, db, sub))
        r = slot_of(**{"d" + a: da, "d" + b: db})
        wait_for(piece(r, h, sub), src_recv.at[h, sub, r])
        if db == 0:
            if da in (1, -1) and sub == part_for(da):
                pass_on(r, h, sub, a, -da)
            for d in (1, -1):
                pass_on(r, h, sub, b, d)
        elif db in (1, -1) and sub == part_for(db):
            pass_on(r, h, sub, b, -db)

    def complete(*blocks):
        for dz, dx in blocks:
            for h in (0, 1):
                da, db = (dx, dz) if h == 0 else (dz, dx)
                for sub in (0, 1):
                    arrived(h, da, db, sub)

    def target(c, sub):
        return tgt_all.at[c, pl.ds(0, HALF + 8) if sub == 0 else pl.ds(HALF + 8, HALF)]

    def tgt_slot(dy, other=0):
        return lax.rem(y + dy + NY, NY) * NC + lax.rem(core + other, NC)

    def tgt_pass(c, sub, axis, d):
        remote(target(c, sub), tgt_send, tgt_recv.at[sub, c], near(axis, d))

    def start_targets():
        if NY > 1:
            for first in (True, False):
                for d in (1, -1):
                    tgt_pass(col, part_for(-d) if first else part_for(d), "y", d)
        if NC > 1:
            for sub in (0, 1):
                tgt_pass(col, sub, "core", 1)

    def tgt_arrived(dy, sub):
        c = tgt_slot(dy)
        wait_for(target(c, sub), tgt_recv.at[sub, c])
        if dy in (1, -1):
            if sub == part_for(dy):
                if NC > 1:
                    to = {"y": lax.rem(y - dy + NY, NY), "core": lax.rem(core + 1, NC)}
                    remote(target(c, sub), tgt_send, tgt_recv.at[sub, c], to)
                tgt_pass(c, sub, "y", -dy)
            if NC > 1:
                tgt_pass(c, sub, "core", 1)

    def take_targets(c):
        v = tgt_all[c, 0:D, :]
        norm = jnp.sum(v * v, axis=0, keepdims=True) * (-BITS)
        b = tgt_all[c, D:D + 1, :] * BITS + tgt_all[c, D + 1:D + 2, :] * LOG2E
        hi, lo = split2(v)
        one = jnp.ones((1, TW), jnp.float32)
        tail = placed(D, list(split3(norm)) + list(split3(b)) + [one] * 3, TW)
        full = jnp.concatenate([hi, lo, hi, tail], axis=0)
        left[pl.ds(pl.multiple_of(c * TW, TW), TW), :] = full.T.astype(jnp.bfloat16)

    def take_sources(r):
        v = src_all[r]
        norm = jnp.sum(v * v, axis=0, keepdims=True) * (-BITS)
        hi, lo = split2(v * (2.0 * BITS))
        one = jnp.ones((1, SW), jnp.float32)
        tail = placed(D, [one] * 6 + list(split3(norm)), SW)
        right[r] = jnp.concatenate([hi, hi, lo, tail], axis=0).astype(jnp.bfloat16)

    QB = min(512, COLS)
    EB = min(256, COLS)

    def spots_of(offsets):
        return [(lax.rem(z + dz + 8 * NZ, NZ), lax.rem(x + dx + 8 * NX, NX)) for dz, dx in offsets]

    def folded(v, op):
        return op(v.reshape(v.shape[0] // 8, 8, v.shape[1]), axis=0)

    def step(done, new):
        if new:
            operand = jnp.concatenate([right[zb * NX + xb] for zb, xb in new], axis=1)
        tops, sums = [None] * len(new), [None] * len(done)
        before = [tops_buf[n] for n in range(len(done))]
        for q in range(COLS // QB):
            rows = slice(q * QB, (q + 1) * QB)
            for n, (zb, xb) in enumerate(done):
                e = jnp.exp2(staged[rows, n * SW:(n + 1) * SW] - before[n])
                if fast:
                    zs[zb * NX + xb, rows, :] = e
                else:
                    zs[zb * NX + xb, rows, :] = staged[rows, n * SW:(n + 1) * SW]
                e = folded(e, jnp.sum)
                sums[n] = e if q == 0 else sums[n] + e
            if new:
                t = jnp.dot(left[rows, :], operand, preferred_element_type=jnp.float32)
                staged[rows, 0:len(new) * SW] = t
                for n in range(len(new)):
                    top = folded(t[:, n * SW:(n + 1) * SW], jnp.max)
                    tops[n] = top if q == 0 else jnp.maximum(tops[n], top)
        for n, (zb, xb) in enumerate(done):
            f_buf[0, row, zb, pl.ds(xb, 1), :] = before[n] + jnp.log2(jnp.sum(sums[n], axis=0, keepdims=True))
            m_rows[zb, pl.ds(xb, 1), :] = before[n]
        for n in range(len(new)):
            tops_buf[n] = jnp.max(tops[n], axis=0, keepdims=True)

    TURNS = (
        ((0, 1), (0, -1)), ((1, 0), (-1, 0)), ((1, 1), (-1, 1)), ((1, -1), (-1, -1)), ((0, 0), (0, 2)),
        ((1, 2), (-1, 2)), ((2, 1), (2, -1)), ((2, 0), (2, 2)),
    ) if NZ > 1 and NX > 1 else (((0, 0),),)

    def turn(k):
        out = TURNS[0]
        for t in range(1, len(TURNS)):
            out = tuple(tuple(jnp.where(k == t, v, w) for v, w in zip(*pair)) for pair in zip(TURNS[t], out))
        return spots_of(out)

    def ready(*turns):
        for t in turns:
            complete(*TURNS[t])
            for zb, xb in spots_of(TURNS[t]):
                take_sources(zb * NX + xb)

    SPLIT = fast and NZ > 1

    def send_f(it, zb):
        late = it if it and SPLIT and zb < NZ // 2 else 0
        to_all(row_peer, NR, f_buf.at[it, row, zb], f_sems.at[it + late])

    both = NZ > 1 and NX > 1
    start_sources()
    start_targets()
    take_targets(col)
    if both:
        for h in (0, 1):
            for d in (1, -1):
                arrived(h, d, 0, part_for(d))
        for h in (0, 1):
            for d in (1, -1):
                arrived(h, d, 0, part_for(-d))
    if NY > 1:
        for d in (1, -1):
            tgt_arrived(d, part_for(d))
        for d in (1, -1):
            tgt_arrived(d, part_for(-d))
    if both:
        for h in (0, 1):
            for d in (1, -1):
                arrived(h, 0, d, part_for(d))
    if both:
        for h in (0, 1):
            for sub in (0, 1):
                arrived(h, 2, 0, sub)
            for da in (1, -1):
                for db in (1, -1):
                    arrived(h, da, db, part_for(db))
        ready(0, 1, 2, 3)
    else:
        ready(0)
    if NY > 1:
        for sub in (0, 1):
            tgt_arrived(2, sub)
        for dy in (1, -1, 2):
            take_targets(tgt_slot(dy))
    if NC > 1:
        for dy in ((0, 1, -1, 2) if NY > 1 else (0,)):
            c = tgt_slot(dy, 1)
            for sub in (0, 1):
                wait_for(target(c, sub), tgt_recv.at[sub, c])
            take_targets(c)
    if both:
        complete((0, 1), (0, -1), (1, 0), (-1, 0))
    if both:
        def stage(k, carry):
            @pl.when(k == 2)
            def _():
                for h in (0, 1):
                    for db in (1, -1):
                        arrived(h, 2, db, part_for(db))
            for t in range(4, len(TURNS)):
                @pl.when(k == t)
                def _(t=t):
                    ready(t)
            step(turn(jnp.maximum(k - 1, 0)), turn(k))

            @pl.when(k == 5)
            def _():
                send_f(0, z)

            @pl.when(k == 6)
            def _():
                for d in (1, 3):
                    send_f(0, lax.rem(z + d, NZ))
            return carry
        lax.fori_loop(0, len(TURNS) + 1, stage, 0)
    else:
        step([], spots_of(TURNS[0]))
        step(spots_of(TURNS[0]), [])
    send_f(0, lax.rem(z + NZ // 2, NZ))
    to_all(row_peer, NR, a_all.at[row], a_sems)
    to_all(col_peer, NK, old_all.at[col], old_sems)
    wait_bytes(a_all, NR - 1, a_sems.at[1])
    wait_bytes(old_all, NK - 1, old_sems.at[1])
    for r in range(NR):
        a_rows[r // NX, r % NX:r % NX + 1, :] = a_all[r] * LOG2E
    for c in range(NK):
        for q in range(TW // 128):
            t, lanes = c * (TW // 128) + q, slice(q * 128, (q + 1) * 128)
            for k in range(2):
                hist[k, t:t + 1, :] = tgt_all[c, D + k:D + k + 1, lanes]
            for k in range(2 * KEPT):
                hist[2 + k, t:t + 1, :] = old_all[c, k:k + 1, lanes]

    bad = jnp.zeros((1, 1), jnp.float32)
    g_now = hist[0]
    bias = g_now * BITS + hist[1] * LOG2E
    images = [hist[2 + k] for k in range(KEPT)]
    base = [hist[2 + KEPT + k] for k in range(KEPT)]
    shift = jnp.zeros((1, 1), jnp.float32)
    pairs = [(a, b) for a in range(HIST) for b in range(a, HIST)]
    line = lax.broadcasted_iota(jnp.int32, (1, 128), 1)
    eye = (lax.broadcasted_iota(jnp.int32, (16, 128), 0) == lax.broadcasted_iota(jnp.int32, (16, 128), 1))

    def all_of(v, op):
        return op(op(v, axis=0, keepdims=True), axis=1, keepdims=True)

    def low(v):
        return all_of(jnp.where(v >= SMALLEST, 0.0, 1.0), jnp.max)

    for it in range(ITERS):
        last = it == ITERS - 1
        if it and fast:
            GZ = min(2, NZ)
            SB = min(128, COLS)
            for zg in range(0, NZ, GZ):
                spots = [(zz, xx) for zz in range(zg, zg + GZ) for xx in range(NX)]

                def weigh(i, acc):
                    rows = pl.ds(pl.multiple_of(i * SB, SB), SB)
                    v = vrep[rows, :]
                    return tuple(
                        a + jnp.sum((zs[zz * NX + xx, rows, :] * v).reshape(SB // 8, 8, SW), axis=0)
                        for a, (zz, xx) in zip(acc, spots)
                    )
                found = lax.fori_loop(0, COLS // SB, weigh, tuple(jnp.zeros((8, SW), jnp.float32) for _ in spots))
                found = [jnp.sum(v, axis=0, keepdims=True) for v in found]
                for zz in range(zg, zg + GZ):
                    s = jnp.concatenate(found[(zz - zg) * NX:(zz - zg + 1) * NX], axis=0)
                    bad = bad + low(s)
                    f_buf[it, row, zz] = m_rows[zz] + shift + jnp.log2(s)
                for zz in range(zg, zg + GZ):
                    send_f(it, zz)
        elif it:
            def again(r, carry):
                def tops_of(i, acc):
                    rows = pl.ds(pl.multiple_of(i * EB, EB), EB)
                    v = zs[r, rows, :] + vrep[rows, :]
                    return jnp.maximum(acc, jnp.max(v.reshape(EB // 8, 8, SW), axis=0))
                top = lax.fori_loop(0, COLS // EB, tops_of, jnp.full((8, SW), -jnp.inf, jnp.float32))
                top = jnp.max(top, axis=0, keepdims=True)

                def sums_of(i, acc):
                    rows = pl.ds(pl.multiple_of(i * EB, EB), EB)
                    v = jnp.exp2((zs[r, rows, :] + vrep[rows, :]) - top)
                    return acc + jnp.sum(v.reshape(EB // 8, 8, SW), axis=0)
                s = lax.fori_loop(0, COLS // EB, sums_of, jnp.zeros((8, SW), jnp.float32))
                f_buf[it, row, r // NX, pl.ds(lax.rem(r, NX), 1), :] = top + jnp.log2(
                    jnp.sum(s, axis=0, keepdims=True))
                return carry
            lax.fori_loop(0, NR, again, 0)
            for zz in range(NZ):
                send_f(it, zz)
        level = jnp.zeros((1, 1), jnp.float32)
        early = it > 0 and SPLIT
        HZ = NZ // 2

        def joined(lines):
            parts = [f_buf[it, r, lines] for r in range(NR)]
            top = functools.reduce(jnp.maximum, parts)
            return top + jnp.log2(functools.reduce(jnp.add, [jnp.exp2(v - top) for v in parts]))

        def half_sent(sem, lines):
            wait_for(f_buf.at[it, pl.ds(0, NR - 1), lines], sem)

        if early:
            half_sent(f_sems.at[it + 1, 1], pl.ds(0, HZ))
            whole = joined(slice(0, HZ))
            g_tmp[0:HZ] = whole
            term = a_rows[0:HZ] - whole + m_rows[0:HZ]
            level = all_of(jnp.max(term, axis=0), jnp.max)
            u_rows[0:HZ] = jnp.exp2(term - level[None])

            def first_half(i, carry):
                rows = pl.ds(pl.multiple_of(i * 128, 128), 128)
                wacc[rows, :] = functools.reduce(jnp.add, [
                    zs[r, rows, :] * u_rows[r // NX, r % NX:r % NX + 1, :] for r in range(HZ * NX)
                ])
                return carry
            lax.fori_loop(0, NT, first_half, 0)
            half_sent(f_sems.at[it, 1], pl.ds(0, HZ))
            whole = joined(slice(HZ, NZ))
            g_tmp[HZ:NZ] = whole
            term = a_rows[HZ:NZ] - whole + m_rows[HZ:NZ] - level[None]
            bad = bad + all_of(jnp.max(jnp.where(term <= 60.0, 0.0, 1.0), axis=0), jnp.max)
            u_rows[HZ:NZ] = jnp.exp2(term)
        else:
            wait_bytes(f_buf.at[it], NR - 1, f_sems.at[it, 1])
            whole = joined(slice(0, NZ))
            g_tmp[...] = whole
            term = a_rows[...] - whole
            if fast:
                term = term + m_rows[...]
                level = all_of(jnp.max(term, axis=0), jnp.max)
                u_rows[...] = jnp.exp2(term - level[None])
            else:
                u_rows[...] = term
        TPH = max(NT // 2, 1)
        for half in range(NT // TPH):
            def tile(i, carry):
                rows = pl.ds(pl.multiple_of((half * TPH + i) * 128, 128), 128)

                def scaled(r):
                    return zs[r, rows, :] * u_rows[r // NX, r % NX:r % NX + 1, :]
                if early:
                    acc = functools.reduce(jnp.add, [scaled(r) for r in range(HZ * NX, NR)])
                    wacc[rows, :] = acc + wacc[rows, :]
                else:
                    wacc[rows, :] = functools.reduce(jnp.add, [scaled(r) for r in range(NR)])
                return carry

            def tile_wide(i, carry):
                rows = pl.ds(pl.multiple_of((half * TPH + i) * 128, 128), 128)

                def moved(r):
                    return zs[r, rows, :] + u_rows[r // NX, r % NX:r % NX + 1, :]
                top = functools.reduce(jnp.maximum, [moved(r) for r in range(NR)])
                top = jnp.max(top, axis=1, keepdims=True)
                acc = functools.reduce(jnp.add, [jnp.exp2(moved(r) - top) for r in range(NR)])
                wacc[rows, :] = jnp.broadcast_to(top + jnp.log2(jnp.sum(acc, axis=1, keepdims=True)), (128, 128))
                return carry
            lax.fori_loop(0, TPH, tile if fast else tile_wide, 0)
            found = []
            for i in range(half * TPH, (half + 1) * TPH):
                turned = wacc[i * 128:(i + 1) * 128, :].T
                found.append(jnp.sum(turned, axis=0, keepdims=True) if fast else turned[0:1, :])
            found = jnp.concatenate(found, axis=0)
            lines = slice(half * TPH, (half + 1) * TPH)
            if fast:
                bad = bad + low(found)
                found = jnp.log2(found) + level
            c_buf[it, col, lines, :] = found - bias[lines, :]
            to_all(col_peer, NK, c_buf.at[it, col, pl.ds(half * TPH, TPH)], c_sems.at[it])
        if last:
            fo_buf[col] = g_tmp[z, pl.ds(x, 1), :] * (-NATS)
            to_all(col_peer, NK, fo_buf.at[col], fo_sems)
        wait_bytes(c_buf.at[it], NK - 1, c_sems.at[it, 1])
        parts = [c_buf[it, c] for c in range(NK)]
        top = functools.reduce(jnp.maximum, parts)
        mapped = (top + jnp.log2(functools.reduce(jnp.add, [jnp.exp2(v - top) for v in parts]))) * (-NATS)
        images = (images + [mapped])[-HIST:]
        base = (base + [g_now])[-HIST:]
        resid = [p - q for p, q in zip(images, base)]
        prods = [jnp.sum(resid[a] * resid[b], axis=0, keepdims=True) for a, b in pairs]
        prods.append(jnp.where(line == 0, bad, 0.0))
        sums = jnp.sum(jnp.concatenate(prods, axis=0), axis=1, keepdims=True)
        r_buf[it, row] = jnp.sum(jnp.where(eye, sums, 0.0), axis=0, keepdims=True)
        to_all(row_peer, NR, r_buf.at[it, row], r_sems.at[it])
        wait_bytes(r_buf.at[it], NR - 1, r_sems.at[it, 1])
        flat = functools.reduce(jnp.add, [r_buf[it, r] for r in range(NR)])

        def entry(k):
            return jnp.sum(jnp.where(line == k, flat, 0.0), axis=1, keepdims=True)
        mix = solve({ab: entry(k) for k, ab in enumerate(pairs)})
        g_next = functools.reduce(jnp.add, [v * m for v, m in zip(images, mix)])
        if last:
            hist[0] = g_next
            for q in range(TW // 128):
                gout_ref[q:q + 1, :] = hist[0, pl.ds(col * (TW // 128) + q, 1), :]
            flag_ref[...] = jnp.broadcast_to(entry(len(pairs)), (1, 128))
        else:
            delta = (g_next - g_now) * BITS
            if fast:
                shift = all_of(delta, jnp.max)
                delta = jnp.exp2(delta - shift)
            for t in range(NT):
                vrep[t * 128:(t + 1) * 128, :] = jnp.broadcast_to(delta[t:t + 1, :], (128, 128)).T
            g_now = g_next

    wait_bytes(fo_buf, NK - 1, fo_sems.at[1])
    for c in range(NK):
        f_ref[c:c + 1, :] = fo_buf[c]
    wait_bytes(src_all, NR - 1, src_send)
    wait_bytes(tgt_all, NK - 1, tgt_send)
    wait_bytes(fo_buf, NK - 1, fo_sems.at[0])
    wait_bytes(a_all, NR - 1, a_sems.at[0])
    wait_bytes(old_all, NK - 1, old_sems.at[0])
    for it in range(ITERS):
        if it and SPLIT:
            half_sent(f_sems.at[it, 0], pl.ds(0, HZ))
            half_sent(f_sems.at[it + 1, 0], pl.ds(0, HZ))
        else:
            wait_bytes(f_buf.at[it], NR - 1, f_sems.at[it, 0])
        wait_bytes(c_buf.at[it], NK - 1, c_sems.at[it, 0])
        wait_bytes(r_buf.at[it], NR - 1, r_sems.at[it, 0])


def shards(dims, src, tgt, log_a, log_b, g, hist_g, hist_maps):
    NZ, NX, NY, NC = dims
    NR, NK = NZ * NX, NY * NC
    D, SW = src.shape
    TW = tgt.shape[1]
    COLS = NK * TW
    NT = COLS // 128
    f32 = jnp.float32
    vmem = pl.BlockSpec(memory_space=pltpu.VMEM)
    dma = pltpu.SemaphoreType.DMA

    def call(fast):
        return pl.pallas_call(
            functools.partial(kernel, fast, dims),
            out_shape=(
                jax.ShapeDtypeStruct((NK, SW), f32),
                jax.ShapeDtypeStruct((TW // 128, 128), f32),
                jax.ShapeDtypeStruct((1, 128), f32),
            ),
            in_specs=[pl.BlockSpec(memory_space=pltpu.HBM)] * 7,
            out_specs=(vmem,) * 3,
            scratch_shapes=[
                pltpu.VMEM((NR, D, SW), f32),
                pltpu.VMEM((NK, D + 8, TW), f32),
                pltpu.VMEM((NR, 1, SW), f32),
                pltpu.VMEM((NK, 2 * (HIST - 1), TW), f32),
                pltpu.VMEM((NK, SW), f32),
                pltpu.VMEM((1, TW), f32),
                pltpu.VMEM((1, TW), f32),
                pltpu.VMEM((HIST - 1, TW), f32),
                pltpu.VMEM((HIST - 1, TW), f32),
                pltpu.VMEM((COLS, 4 * D), jnp.bfloat16),
                pltpu.VMEM((NR, 4 * D, SW), jnp.bfloat16),
                pltpu.VMEM((COLS, 2 * SW), f32),
                pltpu.VMEM((2, 1, SW), f32),
                pltpu.VMEM((NR, COLS, SW), f32),
                pltpu.VMEM((COLS, 128), f32),
                pltpu.VMEM((COLS, 128), f32),
                pltpu.VMEM((2 * HIST, NT, 128), f32),
                pltpu.VMEM((NZ, NX, SW), f32),
                pltpu.VMEM((NZ, NX, SW), f32),
                pltpu.VMEM((NZ, NX, SW), f32),
                pltpu.VMEM((NZ, NX, SW), f32),
                pltpu.VMEM((ITERS, NR, NZ, NX, SW), f32),
                pltpu.VMEM((NK, 1, SW), f32),
                pltpu.VMEM((ITERS, NK, NT, 128), f32),
                pltpu.VMEM((ITERS, NR, 1, 128), f32),
                dma((7,)), dma((2,)), dma((2,)), dma, dma((2, 2, NR)), dma, dma((2, NK)),
                dma((ITERS + 1, 2)), dma((2,)), dma((ITERS, 2)), dma((ITERS, 2)),
            ],
            compiler_params=pltpu.CompilerParams(
                collective_id=0 if fast else 1, has_side_effects=True,
                vmem_limit_bytes=48 * 1024 * 1024
            ),
            name="sinkhorn" if fast else "sinkhorn_wide",
        )(src, tgt, log_a.reshape(NK, SW), log_b.reshape(NR, 1, TW), g.reshape(1, TW), hist_g, hist_maps)

    f, gout, flag = call(True)
    f, gout = lax.cond(flag[0, 0] > 0.5, lambda: call(False)[:2], lambda: (f, gout))
    return f.reshape(-1), gout.reshape(-1)


def solution(mesh, dims=(4, 4, 4, 2)):
    grid = Mesh(mesh.devices.reshape(dims), AXES)
    in_specs = (
        P(None, AXES),
        P(None, ("y", "core", "z", "x")),
        P(("z", "x")),
        P(("y", "core")),
        P(("y", "core", "z", "x")),
        P(None, ("y", "core", "z", "x")),
        P(None, ("y", "core", "z", "x")),
    )
    out_specs = (P(("z", "x")), P(("y", "core", "z", "x")))
    return jax.shard_map(
        functools.partial(shards, dims), mesh=grid, in_specs=in_specs, out_specs=out_specs, check_vma=False
    )
```

```python
import functools

import jax
import jax.numpy as jnp
from jax import lax
from jax.experimental import pallas as pl
from jax.experimental.pallas import tpu as pltpu
from jax.sharding import Mesh
from jax.sharding import PartitionSpec as P

HIST = 5
ITERS = 2
EPS = 0.1
LOG2E = 1.4426950408889634
BITS = LOG2E / EPS
NATS = EPS / LOG2E
LEAST_BITS = -97.0
SMALLEST = 2.0**LEAST_BITS
MESH = pl.DeviceIdType.MESH
AXES = ("z", "x", "y", "core")


def split2(v):
    hi = v.astype(jnp.bfloat16).astype(jnp.float32)
    return hi, v - hi


def split3(v):
    hi = v.astype(jnp.bfloat16).astype(jnp.float32)
    rest = v - hi
    mid = rest.astype(jnp.bfloat16).astype(jnp.float32)
    return hi, mid, rest - mid


def placed(rows, values, width):
    at = lax.broadcasted_iota(jnp.int32, (rows, width), 0)
    out = jnp.zeros((rows, width), jnp.float32)
    for k, v in enumerate(values):
        out = jnp.where(at == k, v, out)
    return out


def solve(gram):
    n = HIST
    trace = gram[0, 0]
    for k in range(1, n):
        trace = trace + gram[k, k]
    shift = 0.001 * trace / n + 1e-6
    a = [[gram[min(p, q), max(p, q)] + (shift if p == q else 0.0) for q in range(n)] for p in range(n)]
    rhs = [jnp.ones((1, 1), jnp.float32) for _ in range(n)]
    for p in range(n):
        for low in range(p + 1, n):
            factor = a[low][p] / a[p][p]
            for q in range(p + 1, n):
                a[low][q] = a[low][q] - factor * a[p][q]
            rhs[low] = rhs[low] - factor * rhs[p]
    out = [None] * n
    for p in reversed(range(n)):
        acc = rhs[p]
        for q in range(p + 1, n):
            acc = acc - a[p][q] * out[q]
        out[p] = acc / a[p][p]
    total = out[0]
    for k in range(1, n):
        total = total + out[k]
    return [o / total for o in out]


def kernel(
    fast, dims,
    src_hbm, tgt_hbm, loga_hbm, logb_hbm, g_hbm, hg_hbm, hm_hbm,
    f_ref, gout_ref, flag_ref,
    src_all, tgt_all, a_all, old_all, loga_in, logb_in, g_in, hg_in, hm_in,
    left, right, staged, tops_buf, zs, wacc, vrep, hist, m_rows, a_rows, u_rows, g_tmp,
    f_buf, fo_buf, c_buf, r_buf,
    in_sems, a_sems, old_sems, src_send, src_recv, tgt_send, tgt_recv, f_sems, fo_sems, c_sems, r_sems,
):
    NZ, NX, NY, NC = dims
    SIZE = dict(zip(AXES, dims))
    NR, NK = NZ * NX, NY * NC
    D, SW = src_hbm.shape
    TW = tgt_hbm.shape[1]
    COLS = NK * TW
    NT = COLS // 128
    at = {name: lax.axis_index(name) for name in AXES}
    z, x, y, core = (at[name] for name in AXES)
    row, col = z * NX + x, y * NC + core

    def row_peer(k):
        p = lax.rem(row + k, NR)
        return {"z": p // NX, "x": lax.rem(p, NX)}

    def col_peer(k):
        p = lax.rem(col + k, NK)
        return {"y": p // NC, "core": lax.rem(p, NC)}

    def near(axis, d):
        return {axis: lax.rem(at[axis] + d + SIZE[axis], SIZE[axis])}

    def remote(part, ssem, rsem, peer):
        pltpu.make_async_remote_copy(
            src_ref=part, dst_ref=part, send_sem=ssem, recv_sem=rsem, device_id=peer, device_id_type=MESH
        ).start()

    def to_all(peer, count, part, sems):
        for k in range(1, count):
            remote(part, sems.at[0], sems.at[1], peer(k))

    def wait_for(part, sem):
        pltpu.make_async_copy(part, part, sem).wait()

    def wait_bytes(buf, count, sem):
        if count:
            wait_for(buf.at[pl.ds(0, count)], sem)

    barrier = pltpu.get_barrier_semaphore()
    around = [(name, d) for name in ("x", "z", "y") if SIZE[name] > 1 for d in (1, -1)]
    if NC > 1:
        around.append(("core", 1))
    for name, d in around:
        pl.semaphore_signal(barrier, inc=1, device_id=near(name, d), device_id_type=MESH)

    greeted = len(around)
    if NC > 1 and NY > 1:
        for d in (1, -1):
            to = {"y": lax.rem(y + d + NY, NY), "core": lax.rem(core + 1, NC)}
            pl.semaphore_signal(barrier, inc=1, device_id=to, device_id_type=MESH)
        greeted += 2

    moves = [
        (src_hbm, src_all.at[row]), (tgt_hbm, tgt_all.at[col, pl.ds(0, D)]), (loga_hbm, loga_in),
        (logb_hbm.at[row], logb_in), (g_hbm, g_in), (hm_hbm, hm_in), (hg_hbm, hg_in),
    ]
    moves = [pltpu.make_async_copy(s, d, in_sems.at[k]) for k, (s, d) in enumerate(moves)]
    for m in moves:
        m.start()
    for m in moves:
        m.wait()
    KEPT = HIST - 1
    a_all[row] = loga_in[pl.ds(col, 1), :]
    tgt_all[col, D:D + 8, :] = placed(8, [g_in[...], logb_in[...]], TW)
    old_all[col] = jnp.concatenate([hm_in[...], hg_in[...]], axis=0)
    pl.semaphore_wait(barrier, greeted)

    HALF, QUART = D // 2, D // 4
    PIECES = (((0, QUART), (QUART, QUART)), ((HALF, QUART), (HALF + QUART, QUART)))
    ORDER = (("x", "z"), ("z", "x"))
    seen = set()

    def slot_of(dz, dx):
        return lax.rem(z + dz + NZ, NZ) * NX + lax.rem(x + dx + NX, NX)

    def piece(r, h, sub):
        start, count = PIECES[h][sub]
        return src_all.at[r, pl.ds(start, count)]

    def pass_on(r, h, sub, axis, d):
        remote(piece(r, h, sub), src_send, src_recv.at[h, sub, r], near(axis, d))

    def part_for(d):
        return 0 if d < 0 else 1

    def start_sources():
        for phase in (0, 1):
            for first in (True, False):
                for h in (0, 1):
                    axis = ORDER[h][phase]
                    if SIZE[axis] > 1:
                        for d in (1, -1):
                            pass_on(row, h, part_for(-d) if first else part_for(d), axis, d)

    def arrived(h, da, db, sub):
        a, b = ORDER[h]
        if (h, da, db, sub) in seen or (da == 0 and db == 0):
            return
        seen.add((h, da, db, sub))
        r = slot_of(**{"d" + a: da, "d" + b: db})
        wait_for(piece(r, h, sub), src_recv.at[h, sub, r])
        if db == 0:
            if da in (1, -1) and sub == part_for(da):
                pass_on(r, h, sub, a, -da)
            for d in (1, -1):
                pass_on(r, h, sub, b, d)
        elif db in (1, -1) and sub == part_for(db):
            pass_on(r, h, sub, b, -db)

    def complete(*blocks):
        for dz, dx in blocks:
            for h in (0, 1):
                da, db = (dx, dz) if h == 0 else (dz, dx)
                for sub in (0, 1):
                    arrived(h, da, db, sub)

    def target(c, sub):
        return tgt_all.at[c, pl.ds(0, HALF + 8) if sub == 0 else pl.ds(HALF + 8, HALF)]

    def tgt_slot(dy, other=0):
        return lax.rem(y + dy + NY, NY) * NC + lax.rem(core + other, NC)

    def tgt_pass(c, sub, axis, d):
        remote(target(c, sub), tgt_send, tgt_recv.at[sub, c], near(axis, d))

    def start_targets():
        if NY > 1:
            for first in (True, False):
                for d in (1, -1):
                    tgt_pass(col, part_for(-d) if first else part_for(d), "y", d)
        if NC > 1:
            for sub in (0, 1):
                tgt_pass(col, sub, "core", 1)

    def tgt_arrived(dy, sub):
        c = tgt_slot(dy)
        wait_for(target(c, sub), tgt_recv.at[sub, c])
        if dy in (1, -1):
            if sub == part_for(dy):
                if NC > 1:
                    to = {"y": lax.rem(y - dy + NY, NY), "core": lax.rem(core + 1, NC)}
                    remote(target(c, sub), tgt_send, tgt_recv.at[sub, c], to)
                tgt_pass(c, sub, "y", -dy)
            if NC > 1:
                tgt_pass(c, sub, "core", 1)

    def take_targets(c):
        v = tgt_all[c, 0:D, :]
        norm = jnp.sum(v * v, axis=0, keepdims=True) * (-BITS)
        b = tgt_all[c, D:D + 1, :] * BITS + tgt_all[c, D + 1:D + 2, :] * LOG2E
        hi, lo = split2(v)
        one = jnp.ones((1, TW), jnp.float32)
        tail = placed(D, list(split3(norm)) + list(split3(b)) + [one] * 3, TW)
        full = jnp.concatenate([hi, lo, hi, tail], axis=0)
        left[pl.ds(pl.multiple_of(c * TW, TW), TW), :] = full.T.astype(jnp.bfloat16)

    def take_sources(r):
        v = src_all[r]
        norm = jnp.sum(v * v, axis=0, keepdims=True) * (-BITS)
        hi, lo = split2(v * (2.0 * BITS))
        one = jnp.ones((1, SW), jnp.float32)
        tail = placed(D, [one] * 6 + list(split3(norm)), SW)
        right[r] = jnp.concatenate([hi, hi, lo, tail], axis=0).astype(jnp.bfloat16)

    QB = min(256, COLS)
    EB = min(256, COLS)

    def spots_of(offsets):
        return [(lax.rem(z + dz + 8 * NZ, NZ), lax.rem(x + dx + 8 * NX, NX)) for dz, dx in offsets]

    def folded(v, op):
        return op(v.reshape(v.shape[0] // 8, 8, v.shape[1]), axis=0)

    def step(done, new):
        if new:
            operand = jnp.concatenate([right[zb * NX + xb] for zb, xb in new], axis=1)
        tops, sums = [None] * len(new), [None] * len(done)
        before = [tops_buf[n] for n in range(len(done))]
        for q in range(COLS // QB):
            rows = slice(q * QB, (q + 1) * QB)
            for n, (zb, xb) in enumerate(done):
                e = jnp.exp2(staged[rows, n * SW:(n + 1) * SW] - before[n])
                if fast:
                    zs[zb * NX + xb, rows, :] = e
                else:
                    zs[zb * NX + xb, rows, :] = staged[rows, n * SW:(n + 1) * SW]
                e = folded(e, jnp.sum)
                sums[n] = e if q == 0 else sums[n] + e
            if new:
                t = jnp.dot(left[rows, :], operand, preferred_element_type=jnp.float32)
                staged[rows, 0:len(new) * SW] = t
                for n in range(len(new)):
                    top = folded(t[:, n * SW:(n + 1) * SW], jnp.max)
                    tops[n] = top if q == 0 else jnp.maximum(tops[n], top)
        for n, (zb, xb) in enumerate(done):
            f_buf[0, row, zb, pl.ds(xb, 1), :] = before[n] + jnp.log2(jnp.sum(sums[n], axis=0, keepdims=True))
            m_rows[zb, pl.ds(xb, 1), :] = before[n]
        for n in range(len(new)):
            tops_buf[n] = jnp.max(tops[n], axis=0, keepdims=True)

    TURNS = (
        ((0, 1), (0, -1)), ((1, 0), (-1, 0)), ((1, 1), (-1, 1)), ((1, -1), (-1, -1)), ((0, 0), (0, 2)),
        ((1, 2), (-1, 2)), ((2, 1), (2, -1)), ((2, 0), (2, 2)),
    ) if NZ > 1 and NX > 1 else (((0, 0),),)

    def turn(k):
        out = TURNS[0]
        for t in range(1, len(TURNS)):
            out = tuple(tuple(jnp.where(k == t, v, w) for v, w in zip(*pair)) for pair in zip(TURNS[t], out))
        return spots_of(out)

    def ready(*turns):
        for t in turns:
            complete(*TURNS[t])
            for zb, xb in spots_of(TURNS[t]):
                take_sources(zb * NX + xb)

    SPLIT = fast and NZ > 1

    def send_f(it, zb):
        late = it if it and SPLIT and zb < NZ // 2 else 0
        to_all(row_peer, NR, f_buf.at[it, row, zb], f_sems.at[it + late])

    both = NZ > 1 and NX > 1
    start_sources()
    start_targets()
    take_targets(col)
    if both:
        for h in (0, 1):
            for d in (1, -1):
                arrived(h, d, 0, part_for(d))
        for h in (0, 1):
            for d in (1, -1):
                arrived(h, d, 0, part_for(-d))
    if NY > 1:
        for d in (1, -1):
            tgt_arrived(d, part_for(d))
        for d in (1, -1):
            tgt_arrived(d, part_for(-d))
    if both:
        for h in (0, 1):
            for d in (1, -1):
                arrived(h, 0, d, part_for(d))
    if both:
        for h in (0, 1):
            for sub in (0, 1):
                arrived(h, 2, 0, sub)
            for da in (1, -1):
                for db in (1, -1):
                    arrived(h, da, db, part_for(db))
        ready(0, 1, 2, 3)
    else:
        ready(0)
    if NY > 1:
        for sub in (0, 1):
            tgt_arrived(2, sub)
        for dy in (1, -1, 2):
            take_targets(tgt_slot(dy))
    if NC > 1:
        for dy in ((0, 1, -1, 2) if NY > 1 else (0,)):
            c = tgt_slot(dy, 1)
            for sub in (0, 1):
                wait_for(target(c, sub), tgt_recv.at[sub, c])
            take_targets(c)
    if both:
        complete((0, 1), (0, -1), (1, 0), (-1, 0))
    if both:
        def stage(k, carry):
            @pl.when(k == 2)
            def _():
                for h in (0, 1):
                    for db in (1, -1):
                        arrived(h, 2, db, part_for(db))
            for t in range(4, len(TURNS)):
                @pl.when(k == t)
                def _(t=t):
                    ready(t)
            step(turn(jnp.maximum(k - 1, 0)), turn(k))

            @pl.when(k == 5)
            def _():
                send_f(0, z)

            @pl.when(k == 6)
            def _():
                for d in (1, 3):
                    send_f(0, lax.rem(z + d, NZ))
            return carry
        lax.fori_loop(0, len(TURNS) + 1, stage, 0)
    else:
        step([], spots_of(TURNS[0]))
        step(spots_of(TURNS[0]), [])
    send_f(0, lax.rem(z + NZ // 2, NZ))
    to_all(row_peer, NR, a_all.at[row], a_sems)
    to_all(col_peer, NK, old_all.at[col], old_sems)
    wait_bytes(a_all, NR - 1, a_sems.at[1])
    wait_bytes(old_all, NK - 1, old_sems.at[1])
    for r in range(NR):
        a_rows[r // NX, r % NX:r % NX + 1, :] = a_all[r] * LOG2E
    for c in range(NK):
        for q in range(TW // 128):
            t, lanes = c * (TW // 128) + q, slice(q * 128, (q + 1) * 128)
            for k in range(2):
                hist[k, t:t + 1, :] = tgt_all[c, D + k:D + k + 1, lanes]
            for k in range(2 * KEPT):
                hist[2 + k, t:t + 1, :] = old_all[c, k:k + 1, lanes]

    bad = jnp.zeros((1, 1), jnp.float32)
    g_now = hist[0]
    bias = g_now * BITS + hist[1] * LOG2E
    images = [hist[2 + k] for k in range(KEPT)]
    base = [hist[2 + KEPT + k] for k in range(KEPT)]
    shift = jnp.zeros((1, 1), jnp.float32)
    pairs = [(a, b) for a in range(HIST) for b in range(a, HIST)]
    line = lax.broadcasted_iota(jnp.int32, (1, 128), 1)
    eye = (lax.broadcasted_iota(jnp.int32, (16, 128), 0) == lax.broadcasted_iota(jnp.int32, (16, 128), 1))

    def all_of(v, op):
        return op(op(v, axis=0, keepdims=True), axis=1, keepdims=True)

    def low(v):
        return all_of(jnp.where(v >= SMALLEST, 0.0, 1.0), jnp.max)

    for it in range(ITERS):
        last = it == ITERS - 1
        if it and fast:
            GZ = min(2, NZ)
            SB = min(128, COLS)
            for zg in range(0, NZ, GZ):
                spots = [(zz, xx) for zz in range(zg, zg + GZ) for xx in range(NX)]

                def weigh(i, acc):
                    rows = pl.ds(pl.multiple_of(i * SB, SB), SB)
                    v = vrep[rows, :]
                    return tuple(
                        a + jnp.sum((zs[zz * NX + xx, rows, :] * v).reshape(SB // 8, 8, SW), axis=0)
                        for a, (zz, xx) in zip(acc, spots)
                    )
                found = lax.fori_loop(0, COLS // SB, weigh, tuple(jnp.zeros((8, SW), jnp.float32) for _ in spots))
                found = [jnp.sum(v, axis=0, keepdims=True) for v in found]
                for zz in range(zg, zg + GZ):
                    s = jnp.concatenate(found[(zz - zg) * NX:(zz - zg + 1) * NX], axis=0)
                    bad = bad + low(s)
                    f_buf[it, row, zz] = m_rows[zz] + shift + jnp.log2(s)
                for zz in range(zg, zg + GZ):
                    send_f(it, zz)
        elif it:
            def again(r, carry):
                def tops_of(i, acc):
                    rows = pl.ds(pl.multiple_of(i * EB, EB), EB)
                    v = zs[r, rows, :] + vrep[rows, :]
                    return jnp.maximum(acc, jnp.max(v.reshape(EB // 8, 8, SW), axis=0))
                top = lax.fori_loop(0, COLS // EB, tops_of, jnp.full((8, SW), -jnp.inf, jnp.float32))
                top = jnp.max(top, axis=0, keepdims=True)

                def sums_of(i, acc):
                    rows = pl.ds(pl.multiple_of(i * EB, EB), EB)
                    v = jnp.exp2((zs[r, rows, :] + vrep[rows, :]) - top)
                    return acc + jnp.sum(v.reshape(EB // 8, 8, SW), axis=0)
                s = lax.fori_loop(0, COLS // EB, sums_of, jnp.zeros((8, SW), jnp.float32))
                f_buf[it, row, r // NX, pl.ds(lax.rem(r, NX), 1), :] = top + jnp.log2(
                    jnp.sum(s, axis=0, keepdims=True))
                return carry
            lax.fori_loop(0, NR, again, 0)
            for zz in range(NZ):
                send_f(it, zz)
        level = jnp.zeros((1, 1), jnp.float32)
        early = it > 0 and SPLIT
        HZ = NZ // 2

        def joined(lines):
            parts = [f_buf[it, r, lines] for r in range(NR)]
            top = functools.reduce(jnp.maximum, parts)
            return top + jnp.log2(functools.reduce(jnp.add, [jnp.exp2(v - top) for v in parts]))

        def half_sent(sem, lines):
            wait_for(f_buf.at[it, pl.ds(0, NR - 1), lines], sem)

        if early:
            half_sent(f_sems.at[it + 1, 1], pl.ds(0, HZ))
            whole = joined(slice(0, HZ))
            g_tmp[0:HZ] = whole
            term = a_rows[0:HZ] - whole + m_rows[0:HZ]
            level = all_of(jnp.max(term, axis=0), jnp.max)
            u_rows[0:HZ] = jnp.exp2(term - level[None])

            def first_half(i, carry):
                rows = pl.ds(pl.multiple_of(i * 128, 128), 128)
                wacc[rows, :] = functools.reduce(jnp.add, [
                    zs[r, rows, :] * u_rows[r // NX, r % NX:r % NX + 1, :] for r in range(HZ * NX)
                ])
                return carry
            lax.fori_loop(0, NT, first_half, 0)
            half_sent(f_sems.at[it, 1], pl.ds(0, HZ))
            whole = joined(slice(HZ, NZ))
            g_tmp[HZ:NZ] = whole
            term = a_rows[HZ:NZ] - whole + m_rows[HZ:NZ] - level[None]
            bad = bad + all_of(jnp.max(jnp.where(term <= 60.0, 0.0, 1.0), axis=0), jnp.max)
            u_rows[HZ:NZ] = jnp.exp2(term)
        else:
            wait_bytes(f_buf.at[it], NR - 1, f_sems.at[it, 1])
            whole = joined(slice(0, NZ))
            g_tmp[...] = whole
            term = a_rows[...] - whole
            if fast:
                term = term + m_rows[...]
                level = all_of(jnp.max(term, axis=0), jnp.max)
                u_rows[...] = jnp.exp2(term - level[None])
            else:
                u_rows[...] = term
        TPH = max(NT // 2, 1)
        for half in range(NT // TPH):
            def tile(i, carry):
                rows = pl.ds(pl.multiple_of((half * TPH + i) * 128, 128), 128)

                def scaled(r):
                    return zs[r, rows, :] * u_rows[r // NX, r % NX:r % NX + 1, :]
                if early:
                    acc = functools.reduce(jnp.add, [scaled(r) for r in range(HZ * NX, NR)])
                    wacc[rows, :] = acc + wacc[rows, :]
                else:
                    wacc[rows, :] = functools.reduce(jnp.add, [scaled(r) for r in range(NR)])
                return carry

            def tile_wide(i, carry):
                rows = pl.ds(pl.multiple_of((half * TPH + i) * 128, 128), 128)

                def moved(r):
                    return zs[r, rows, :] + u_rows[r // NX, r % NX:r % NX + 1, :]
                top = functools.reduce(jnp.maximum, [moved(r) for r in range(NR)])
                top = jnp.max(top, axis=1, keepdims=True)
                acc = functools.reduce(jnp.add, [jnp.exp2(moved(r) - top) for r in range(NR)])
                wacc[rows, :] = jnp.broadcast_to(top + jnp.log2(jnp.sum(acc, axis=1, keepdims=True)), (128, 128))
                return carry
            lax.fori_loop(0, TPH, tile if fast else tile_wide, 0)
            found = []
            for i in range(half * TPH, (half + 1) * TPH):
                turned = wacc[i * 128:(i + 1) * 128, :].T
                found.append(jnp.sum(turned, axis=0, keepdims=True) if fast else turned[0:1, :])
            found = jnp.concatenate(found, axis=0)
            lines = slice(half * TPH, (half + 1) * TPH)
            if fast:
                bad = bad + low(found)
                found = jnp.log2(found) + level
            c_buf[it, col, lines, :] = found - bias[lines, :]
            to_all(col_peer, NK, c_buf.at[it, col, pl.ds(half * TPH, TPH)], c_sems.at[it])
        if last:
            fo_buf[col] = g_tmp[z, pl.ds(x, 1), :] * (-NATS)
            to_all(col_peer, NK, fo_buf.at[col], fo_sems)
        wait_bytes(c_buf.at[it], NK - 1, c_sems.at[it, 1])
        parts = [c_buf[it, c] for c in range(NK)]
        top = functools.reduce(jnp.maximum, parts)
        mapped = (top + jnp.log2(functools.reduce(jnp.add, [jnp.exp2(v - top) for v in parts]))) * (-NATS)
        images = (images + [mapped])[-HIST:]
        base = (base + [g_now])[-HIST:]
        resid = [p - q for p, q in zip(images, base)]
        prods = [jnp.sum(resid[a] * resid[b], axis=0, keepdims=True) for a, b in pairs]
        prods.append(jnp.where(line == 0, bad, 0.0))
        sums = jnp.sum(jnp.concatenate(prods, axis=0), axis=1, keepdims=True)
        r_buf[it, row] = jnp.sum(jnp.where(eye, sums, 0.0), axis=0, keepdims=True)
        to_all(row_peer, NR, r_buf.at[it, row], r_sems.at[it])
        wait_bytes(r_buf.at[it], NR - 1, r_sems.at[it, 1])
        flat = functools.reduce(jnp.add, [r_buf[it, r] for r in range(NR)])

        def entry(k):
            return jnp.sum(jnp.where(line == k, flat, 0.0), axis=1, keepdims=True)
        mix = solve({ab: entry(k) for k, ab in enumerate(pairs)})
        g_next = functools.reduce(jnp.add, [v * m for v, m in zip(images, mix)])
        if last:
            hist[0] = g_next
            for q in range(TW // 128):
                gout_ref[q:q + 1, :] = hist[0, pl.ds(col * (TW // 128) + q, 1), :]
            flag_ref[...] = jnp.broadcast_to(entry(len(pairs)), (1, 128))
        else:
            delta = (g_next - g_now) * BITS
            if fast:
                shift = all_of(delta, jnp.max)
                delta = jnp.exp2(delta - shift)
            for t in range(NT):
                vrep[t * 128:(t + 1) * 128, :] = jnp.broadcast_to(delta[t:t + 1, :], (128, 128)).T
            g_now = g_next

    wait_bytes(fo_buf, NK - 1, fo_sems.at[1])
    for c in range(NK):
        f_ref[c:c + 1, :] = fo_buf[c]
    wait_bytes(src_all, NR - 1, src_send)
    wait_bytes(tgt_all, NK - 1, tgt_send)
    wait_bytes(fo_buf, NK - 1, fo_sems.at[0])
    wait_bytes(a_all, NR - 1, a_sems.at[0])
    wait_bytes(old_all, NK - 1, old_sems.at[0])
    for it in range(ITERS):
        if it and SPLIT:
            half_sent(f_sems.at[it, 0], pl.ds(0, HZ))
            half_sent(f_sems.at[it + 1, 0], pl.ds(0, HZ))
        else:
            wait_bytes(f_buf.at[it], NR - 1, f_sems.at[it, 0])
        wait_bytes(c_buf.at[it], NK - 1, c_sems.at[it, 0])
        wait_bytes(r_buf.at[it], NR - 1, r_sems.at[it, 0])


def shards(dims, src, tgt, log_a, log_b, g, hist_g, hist_maps):
    NZ, NX, NY, NC = dims
    NR, NK = NZ * NX, NY * NC
    D, SW = src.shape
    TW = tgt.shape[1]
    COLS = NK * TW
    NT = COLS // 128
    f32 = jnp.float32
    vmem = pl.BlockSpec(memory_space=pltpu.VMEM)
    dma = pltpu.SemaphoreType.DMA

    def call(fast):
        return pl.pallas_call(
            functools.partial(kernel, fast, dims),
            out_shape=(
                jax.ShapeDtypeStruct((NK, SW), f32),
                jax.ShapeDtypeStruct((TW // 128, 128), f32),
                jax.ShapeDtypeStruct((1, 128), f32),
            ),
            in_specs=[pl.BlockSpec(memory_space=pltpu.HBM)] * 7,
            out_specs=(vmem,) * 3,
            scratch_shapes=[
                pltpu.VMEM((NR, D, SW), f32),
                pltpu.VMEM((NK, D + 8, TW), f32),
                pltpu.VMEM((NR, 1, SW), f32),
                pltpu.VMEM((NK, 2 * (HIST - 1), TW), f32),
                pltpu.VMEM((NK, SW), f32),
                pltpu.VMEM((1, TW), f32),
                pltpu.VMEM((1, TW), f32),
                pltpu.VMEM((HIST - 1, TW), f32),
                pltpu.VMEM((HIST - 1, TW), f32),
                pltpu.VMEM((COLS, 4 * D), jnp.bfloat16),
                pltpu.VMEM((NR, 4 * D, SW), jnp.bfloat16),
                pltpu.VMEM((COLS, 2 * SW), f32),
                pltpu.VMEM((2, 1, SW), f32),
                pltpu.VMEM((NR, COLS, SW), f32),
                pltpu.VMEM((COLS, 128), f32),
                pltpu.VMEM((COLS, 128), f32),
                pltpu.VMEM((2 * HIST, NT, 128), f32),
                pltpu.VMEM((NZ, NX, SW), f32),
                pltpu.VMEM((NZ, NX, SW), f32),
                pltpu.VMEM((NZ, NX, SW), f32),
                pltpu.VMEM((NZ, NX, SW), f32),
                pltpu.VMEM((ITERS, NR, NZ, NX, SW), f32),
                pltpu.VMEM((NK, 1, SW), f32),
                pltpu.VMEM((ITERS, NK, NT, 128), f32),
                pltpu.VMEM((ITERS, NR, 1, 128), f32),
                dma((7,)), dma((2,)), dma((2,)), dma, dma((2, 2, NR)), dma, dma((2, NK)),
                dma((ITERS + 1, 2)), dma((2,)), dma((ITERS, 2)), dma((ITERS, 2)),
            ],
            compiler_params=pltpu.CompilerParams(
                collective_id=0 if fast else 1, has_side_effects=True,
                vmem_limit_bytes=48 * 1024 * 1024
            ),
            name="sinkhorn" if fast else "sinkhorn_wide",
        )(src, tgt, log_a.reshape(NK, SW), log_b.reshape(NR, 1, TW), g.reshape(1, TW), hist_g, hist_maps)

    f, gout, flag = call(True)
    f, gout = lax.cond(flag[0, 0] > 0.5, lambda: call(False)[:2], lambda: (f, gout))
    return f.reshape(-1), gout.reshape(-1)


def solution(mesh, dims=(4, 4, 4, 2)):
    grid = Mesh(mesh.devices.reshape(dims), AXES)
    in_specs = (
        P(None, AXES),
        P(None, ("y", "core", "z", "x")),
        P(("z", "x")),
        P(("y", "core")),
        P(("y", "core", "z", "x")),
        P(None, ("y", "core", "z", "x")),
        P(None, ("y", "core", "z", "x")),
    )
    out_specs = (P(("z", "x")), P(("y", "core", "z", "x")))
    return jax.shard_map(
        functools.partial(shards, dims), mesh=grid, in_specs=in_specs, out_specs=out_specs, check_vma=False
    )
```

```python
import functools

import jax
import jax.numpy as jnp
from jax import lax
from jax.experimental import pallas as pl
from jax.experimental.pallas import tpu as pltpu
from jax.sharding import Mesh
from jax.sharding import PartitionSpec as P

HIST = 5
ITERS = 2
EPS = 0.1
LOG2E = 1.4426950408889634
BITS = LOG2E / EPS
NATS = EPS / LOG2E
LEAST_BITS = -97.0
SMALLEST = 2.0**LEAST_BITS
MESH = pl.DeviceIdType.MESH
AXES = ("z", "x", "y", "core")


def split2(v):
    hi = v.astype(jnp.bfloat16).astype(jnp.float32)
    return hi, v - hi


def split3(v):
    hi = v.astype(jnp.bfloat16).astype(jnp.float32)
    rest = v - hi
    mid = rest.astype(jnp.bfloat16).astype(jnp.float32)
    return hi, mid, rest - mid


def placed(rows, values, width):
    at = lax.broadcasted_iota(jnp.int32, (rows, width), 0)
    out = jnp.zeros((rows, width), jnp.float32)
    for k, v in enumerate(values):
        out = jnp.where(at == k, v, out)
    return out


def solve(gram):
    n = HIST
    trace = gram[0, 0]
    for k in range(1, n):
        trace = trace + gram[k, k]
    shift = 0.001 * trace / n + 1e-6
    a = [[gram[min(p, q), max(p, q)] + (shift if p == q else 0.0) for q in range(n)] for p in range(n)]
    rhs = [jnp.ones((1, 1), jnp.float32) for _ in range(n)]
    for p in range(n):
        for low in range(p + 1, n):
            factor = a[low][p] / a[p][p]
            for q in range(p + 1, n):
                a[low][q] = a[low][q] - factor * a[p][q]
            rhs[low] = rhs[low] - factor * rhs[p]
    out = [None] * n
    for p in reversed(range(n)):
        acc = rhs[p]
        for q in range(p + 1, n):
            acc = acc - a[p][q] * out[q]
        out[p] = acc / a[p][p]
    total = out[0]
    for k in range(1, n):
        total = total + out[k]
    return [o / total for o in out]


def kernel(
    fast, dims,
    src_hbm, tgt_hbm, loga_hbm, logb_hbm, g_hbm, hg_hbm, hm_hbm,
    f_ref, gout_ref, flag_ref,
    src_all, tgt_all, a_all, old_all, loga_in, logb_in, g_in, hg_in, hm_in,
    left, right, staged, tops_buf, zs, wacc, vrep, hist, m_rows, a_rows, u_rows, g_tmp,
    f_buf, fo_buf, c_buf, r_buf,
    in_sems, a_sems, old_sems, src_send, src_recv, tgt_send, tgt_recv, f_sems, fo_sems, c_sems, r_sems,
):
    NZ, NX, NY, NC = dims
    SIZE = dict(zip(AXES, dims))
    NR, NK = NZ * NX, NY * NC
    D, SW = src_hbm.shape
    TW = tgt_hbm.shape[1]
    COLS = NK * TW
    NT = COLS // 128
    at = {name: lax.axis_index(name) for name in AXES}
    z, x, y, core = (at[name] for name in AXES)
    row, col = z * NX + x, y * NC + core

    def row_peer(k):
        p = lax.rem(row + k, NR)
        return {"z": p // NX, "x": lax.rem(p, NX)}

    def col_peer(k):
        p = lax.rem(col + k, NK)
        return {"y": p // NC, "core": lax.rem(p, NC)}

    def near(axis, d):
        return {axis: lax.rem(at[axis] + d + SIZE[axis], SIZE[axis])}

    def remote(part, ssem, rsem, peer):
        pltpu.make_async_remote_copy(
            src_ref=part, dst_ref=part, send_sem=ssem, recv_sem=rsem, device_id=peer, device_id_type=MESH
        ).start()

    def to_all(peer, count, part, sems):
        for k in range(1, count):
            remote(part, sems.at[0], sems.at[1], peer(k))

    def wait_for(part, sem):
        pltpu.make_async_copy(part, part, sem).wait()

    def wait_bytes(buf, count, sem):
        if count:
            wait_for(buf.at[pl.ds(0, count)], sem)

    barrier = pltpu.get_barrier_semaphore()
    around = [(name, d) for name in ("x", "z", "y") if SIZE[name] > 1 for d in (1, -1)]
    if NC > 1:
        around.append(("core", 1))
    for name, d in around:
        pl.semaphore_signal(barrier, inc=1, device_id=near(name, d), device_id_type=MESH)

    greeted = len(around)
    if NC > 1 and NY > 1:
        for d in (1, -1):
            to = {"y": lax.rem(y + d + NY, NY), "core": lax.rem(core + 1, NC)}
            pl.semaphore_signal(barrier, inc=1, device_id=to, device_id_type=MESH)
        greeted += 2

    moves = [
        (src_hbm, src_all.at[row]), (tgt_hbm, tgt_all.at[col, pl.ds(0, D)]), (loga_hbm, loga_in),
        (logb_hbm.at[row], logb_in), (g_hbm, g_in), (hm_hbm, hm_in), (hg_hbm, hg_in),
    ]
    moves = [pltpu.make_async_copy(s, d, in_sems.at[k]) for k, (s, d) in enumerate(moves)]
    for m in moves:
        m.start()
    for m in moves:
        m.wait()
    KEPT = HIST - 1
    a_all[row] = loga_in[pl.ds(col, 1), :]
    tgt_all[col, D:D + 8, :] = placed(8, [g_in[...], logb_in[...]], TW)
    old_all[col] = jnp.concatenate([hm_in[...], hg_in[...]], axis=0)
    pl.semaphore_wait(barrier, greeted)

    HALF, QUART = D // 2, D // 4
    PIECES = (((0, QUART), (QUART, QUART)), ((HALF, QUART), (HALF + QUART, QUART)))
    ORDER = (("x", "z"), ("z", "x"))
    seen = set()

    def slot_of(dz, dx):
        return lax.rem(z + dz + NZ, NZ) * NX + lax.rem(x + dx + NX, NX)

    def piece(r, h, sub):
        start, count = PIECES[h][sub]
        return src_all.at[r, pl.ds(start, count)]

    def pass_on(r, h, sub, axis, d):
        remote(piece(r, h, sub), src_send, src_recv.at[h, sub, r], near(axis, d))

    def part_for(d):
        return 0 if d < 0 else 1

    def start_sources():
        for phase in (0, 1):
            for first in (True, False):
                for h in (0, 1):
                    axis = ORDER[h][phase]
                    if SIZE[axis] > 1:
                        for d in (1, -1):
                            pass_on(row, h, part_for(-d) if first else part_for(d), axis, d)

    def arrived(h, da, db, sub):
        a, b = ORDER[h]
        if (h, da, db, sub) in seen or (da == 0 and db == 0):
            return
        seen.add((h, da, db, sub))
        r = slot_of(**{"d" + a: da, "d" + b: db})
        wait_for(piece(r, h, sub), src_recv.at[h, sub, r])
        if db == 0:
            if da in (1, -1) and sub == part_for(da):
                pass_on(r, h, sub, a, -da)
            for d in (1, -1):
                pass_on(r, h, sub, b, d)
        elif db in (1, -1) and sub == part_for(db):
            pass_on(r, h, sub, b, -db)

    def complete(*blocks):
        for dz, dx in blocks:
            for h in (0, 1):
                da, db = (dx, dz) if h == 0 else (dz, dx)
                for sub in (0, 1):
                    arrived(h, da, db, sub)

    def target(c, sub):
        return tgt_all.at[c, pl.ds(0, HALF + 8) if sub == 0 else pl.ds(HALF + 8, HALF)]

    def tgt_slot(dy, other=0):
        return lax.rem(y + dy + NY, NY) * NC + lax.rem(core + other, NC)

    def tgt_pass(c, sub, axis, d):
        remote(target(c, sub), tgt_send, tgt_recv.at[sub, c], near(axis, d))

    def start_targets():
        if NY > 1:
            for first in (True, False):
                for d in (1, -1):
                    tgt_pass(col, part_for(-d) if first else part_for(d), "y", d)
        if NC > 1:
            for sub in (0, 1):
                tgt_pass(col, sub, "core", 1)

    def tgt_arrived(dy, sub):
        c = tgt_slot(dy)
        wait_for(target(c, sub), tgt_recv.at[sub, c])
        if dy in (1, -1):
            if sub == part_for(dy):
                if NC > 1:
                    to = {"y": lax.rem(y - dy + NY, NY), "core": lax.rem(core + 1, NC)}
                    remote(target(c, sub), tgt_send, tgt_recv.at[sub, c], to)
                tgt_pass(c, sub, "y", -dy)
            if NC > 1:
                tgt_pass(c, sub, "core", 1)

    def take_targets(c):
        v = tgt_all[c, 0:D, :]
        norm = jnp.sum(v * v, axis=0, keepdims=True) * (-BITS)
        b = tgt_all[c, D:D + 1, :] * BITS + tgt_all[c, D + 1:D + 2, :] * LOG2E
        hi, lo = split2(v)
        one = jnp.ones((1, TW), jnp.float32)
        tail = placed(D, list(split3(norm)) + list(split3(b)) + [one] * 3, TW)
        full = jnp.concatenate([hi, lo, hi, tail], axis=0)
        left[pl.ds(pl.multiple_of(c * TW, TW), TW), :] = full.T.astype(jnp.bfloat16)

    def take_sources(r):
        v = src_all[r]
        norm = jnp.sum(v * v, axis=0, keepdims=True) * (-BITS)
        hi, lo = split2(v * (2.0 * BITS))
        one = jnp.ones((1, SW), jnp.float32)
        tail = placed(D, [one] * 6 + list(split3(norm)), SW)
        right[r] = jnp.concatenate([hi, hi, lo, tail], axis=0).astype(jnp.bfloat16)

    QB = min(256, COLS)
    EB = min(256, COLS)

    def spots_of(offsets):
        return [(lax.rem(z + dz + 8 * NZ, NZ), lax.rem(x + dx + 8 * NX, NX)) for dz, dx in offsets]

    def folded(v, op):
        return op(v.reshape(v.shape[0] // 8, 8, v.shape[1]), axis=0)

    def step(done, new):
        if new:
            operand = jnp.concatenate([right[zb * NX + xb] for zb, xb in new], axis=1)
        tops, sums = [None] * len(new), [None] * len(done)
        before = [tops_buf[n] for n in range(len(done))]
        for q in range(COLS // QB):
            rows = slice(q * QB, (q + 1) * QB)
            for n, (zb, xb) in enumerate(done):
                e = jnp.exp2(staged[rows, n * SW:(n + 1) * SW] - before[n])
                if fast:
                    zs[zb * NX + xb, rows, :] = e
                else:
                    zs[zb * NX + xb, rows, :] = staged[rows, n * SW:(n + 1) * SW]
                e = folded(e, jnp.sum)
                sums[n] = e if q == 0 else sums[n] + e
            if new:
                t = jnp.dot(left[rows, :], operand, preferred_element_type=jnp.float32)
                staged[rows, 0:len(new) * SW] = t
                for n in range(len(new)):
                    top = folded(t[:, n * SW:(n + 1) * SW], jnp.max)
                    tops[n] = top if q == 0 else jnp.maximum(tops[n], top)
        for n, (zb, xb) in enumerate(done):
            f_buf[0, row, zb, pl.ds(xb, 1), :] = before[n] + jnp.log2(jnp.sum(sums[n], axis=0, keepdims=True))
            m_rows[zb, pl.ds(xb, 1), :] = before[n]
        for n in range(len(new)):
            tops_buf[n] = jnp.max(tops[n], axis=0, keepdims=True)

    TURNS = (
        ((0, 1), (0, -1)), ((1, 0), (-1, 0)), ((1, 1), (-1, 1)), ((1, -1), (-1, -1)), ((0, 0), (0, 2)),
        ((1, 2), (-1, 2)), ((2, 1), (2, -1)), ((2, 0), (2, 2)),
    ) if NZ > 1 and NX > 1 else (((0, 0),),)

    def turn(k):
        out = TURNS[0]
        for t in range(1, len(TURNS)):
            out = tuple(tuple(jnp.where(k == t, v, w) for v, w in zip(*pair)) for pair in zip(TURNS[t], out))
        return spots_of(out)

    def ready(*turns):
        for t in turns:
            complete(*TURNS[t])
            for zb, xb in spots_of(TURNS[t]):
                take_sources(zb * NX + xb)

    SPLIT = fast and NZ > 1

    def send_f(it, zb):
        late = it if it and SPLIT and zb < NZ // 2 else 0
        to_all(row_peer, NR, f_buf.at[it, row, zb], f_sems.at[it + late])

    def send_rest():
        to_all(row_peer, NR, a_all.at[row], a_sems)
        to_all(col_peer, NK, old_all.at[col], old_sems)

    both = NZ > 1 and NX > 1
    start_sources()
    start_targets()
    take_targets(col)
    if both:
        for h in (0, 1):
            for d in (1, -1):
                arrived(h, d, 0, part_for(d))
        for h in (0, 1):
            for d in (1, -1):
                arrived(h, d, 0, part_for(-d))
    if NY > 1:
        for d in (1, -1):
            tgt_arrived(d, part_for(d))
        for d in (1, -1):
            tgt_arrived(d, part_for(-d))
    if both:
        for h in (0, 1):
            for d in (1, -1):
                arrived(h, 0, d, part_for(d))
    if both:
        for h in (0, 1):
            for sub in (0, 1):
                arrived(h, 2, 0, sub)
            for da in (1, -1):
                for db in (1, -1):
                    arrived(h, da, db, part_for(db))
        ready(0, 1, 2, 3)
    else:
        ready(0)
    if NY > 1:
        for sub in (0, 1):
            tgt_arrived(2, sub)
        for dy in (1, -1, 2):
            take_targets(tgt_slot(dy))
    if NC > 1:
        for dy in ((0, 1, -1, 2) if NY > 1 else (0,)):
            c = tgt_slot(dy, 1)
            for sub in (0, 1):
                wait_for(target(c, sub), tgt_recv.at[sub, c])
            take_targets(c)
    if both:
        complete((0, 1), (0, -1), (1, 0), (-1, 0))
    if both:
        def stage(k, carry):
            @pl.when(k == 2)
            def _():
                for h in (0, 1):
                    for db in (1, -1):
                        arrived(h, 2, db, part_for(db))
            for t in range(4, len(TURNS)):
                @pl.when(k == t)
                def _(t=t):
                    ready(t)
            step(turn(jnp.maximum(k - 1, 0)), turn(k))

            @pl.when(k == 5)
            def _():
                send_f(0, z)

            @pl.when(k == 6)
            def _():
                for d in (1, 3):
                    send_f(0, lax.rem(z + d, NZ))

            @pl.when(k == len(TURNS) - 1)
            def _():
                send_rest()
            return carry
        lax.fori_loop(0, len(TURNS) + 1, stage, 0)
    else:
        step([], spots_of(TURNS[0]))
        step(spots_of(TURNS[0]), [])
        send_rest()
    send_f(0, lax.rem(z + NZ // 2, NZ))
    wait_bytes(a_all, NR - 1, a_sems.at[1])
    wait_bytes(old_all, NK - 1, old_sems.at[1])
    for r in range(NR):
        a_rows[r // NX, r % NX:r % NX + 1, :] = a_all[r] * LOG2E
    for c in range(NK):
        for q in range(TW // 128):
            t, lanes = c * (TW // 128) + q, slice(q * 128, (q + 1) * 128)
            for k in range(2):
                hist[k, t:t + 1, :] = tgt_all[c, D + k:D + k + 1, lanes]
            for k in range(2 * KEPT):
                hist[2 + k, t:t + 1, :] = old_all[c, k:k + 1, lanes]

    bad = jnp.zeros((1, 1), jnp.float32)
    g_now = hist[0]
    bias = g_now * BITS + hist[1] * LOG2E
    images = [hist[2 + k] for k in range(KEPT)]
    base = [hist[2 + KEPT + k] for k in range(KEPT)]
    shift = jnp.zeros((1, 1), jnp.float32)
    pairs = [(a, b) for a in range(HIST) for b in range(a, HIST)]
    line = lax.broadcasted_iota(jnp.int32, (1, 128), 1)
    eye = (lax.broadcasted_iota(jnp.int32, (16, 128), 0) == lax.broadcasted_iota(jnp.int32, (16, 128), 1))

    def all_of(v, op):
        return op(op(v, axis=0, keepdims=True), axis=1, keepdims=True)

    def low(v):
        return all_of(jnp.where(v >= SMALLEST, 0.0, 1.0), jnp.max)

    for it in range(ITERS):
        last = it == ITERS - 1
        if it and fast:
            GZ = min(2, NZ)
            SB = min(128, COLS)
            for zg in range(0, NZ, GZ):
                spots = [(zz, xx) for zz in range(zg, zg + GZ) for xx in range(NX)]

                def weigh(i, acc):
                    rows = pl.ds(pl.multiple_of(i * SB, SB), SB)
                    v = vrep[rows, :]
                    return tuple(
                        a + jnp.sum((zs[zz * NX + xx, rows, :] * v).reshape(SB // 8, 8, SW), axis=0)
                        for a, (zz, xx) in zip(acc, spots)
                    )
                found = lax.fori_loop(0, COLS // SB, weigh, tuple(jnp.zeros((8, SW), jnp.float32) for _ in spots))
                found = [jnp.sum(v, axis=0, keepdims=True) for v in found]
                for zz in range(zg, zg + GZ):
                    s = jnp.concatenate(found[(zz - zg) * NX:(zz - zg + 1) * NX], axis=0)
                    bad = bad + low(s)
                    f_buf[it, row, zz] = m_rows[zz] + shift + jnp.log2(s)
                for zz in range(zg, zg + GZ):
                    send_f(it, zz)
        elif it:
            def again(r, carry):
                def tops_of(i, acc):
                    rows = pl.ds(pl.multiple_of(i * EB, EB), EB)
                    v = zs[r, rows, :] + vrep[rows, :]
                    return jnp.maximum(acc, jnp.max(v.reshape(EB // 8, 8, SW), axis=0))
                top = lax.fori_loop(0, COLS // EB, tops_of, jnp.full((8, SW), -jnp.inf, jnp.float32))
                top = jnp.max(top, axis=0, keepdims=True)

                def sums_of(i, acc):
                    rows = pl.ds(pl.multiple_of(i * EB, EB), EB)
                    v = jnp.exp2((zs[r, rows, :] + vrep[rows, :]) - top)
                    return acc + jnp.sum(v.reshape(EB // 8, 8, SW), axis=0)
                s = lax.fori_loop(0, COLS // EB, sums_of, jnp.zeros((8, SW), jnp.float32))
                f_buf[it, row, r // NX, pl.ds(lax.rem(r, NX), 1), :] = top + jnp.log2(
                    jnp.sum(s, axis=0, keepdims=True))
                return carry
            lax.fori_loop(0, NR, again, 0)
            for zz in range(NZ):
                send_f(it, zz)
        level = jnp.zeros((1, 1), jnp.float32)
        early = it > 0 and SPLIT
        HZ = NZ // 2

        def joined(lines):
            parts = [f_buf[it, r, lines] for r in range(NR)]
            top = functools.reduce(jnp.maximum, parts)
            return top + jnp.log2(functools.reduce(jnp.add, [jnp.exp2(v - top) for v in parts]))

        def half_sent(sem, lines):
            wait_for(f_buf.at[it, pl.ds(0, NR - 1), lines], sem)

        if early:
            half_sent(f_sems.at[it + 1, 1], pl.ds(0, HZ))
            whole = joined(slice(0, HZ))
            g_tmp[0:HZ] = whole
            term = a_rows[0:HZ] - whole + m_rows[0:HZ]
            level = all_of(jnp.max(term, axis=0), jnp.max)
            u_rows[0:HZ] = jnp.exp2(term - level[None])

            def first_half(i, carry):
                rows = pl.ds(pl.multiple_of(i * 128, 128), 128)
                wacc[rows, :] = functools.reduce(jnp.add, [
                    zs[r, rows, :] * u_rows[r // NX, r % NX:r % NX + 1, :] for r in range(HZ * NX)
                ])
                return carry
            lax.fori_loop(0, NT, first_half, 0)
            half_sent(f_sems.at[it, 1], pl.ds(0, HZ))
            whole = joined(slice(HZ, NZ))
            g_tmp[HZ:NZ] = whole
            term = a_rows[HZ:NZ] - whole + m_rows[HZ:NZ] - level[None]
            bad = bad + all_of(jnp.max(jnp.where(term <= 60.0, 0.0, 1.0), axis=0), jnp.max)
            u_rows[HZ:NZ] = jnp.exp2(term)
        else:
            wait_bytes(f_buf.at[it], NR - 1, f_sems.at[it, 1])
            whole = joined(slice(0, NZ))
            g_tmp[...] = whole
            term = a_rows[...] - whole
            if fast:
                term = term + m_rows[...]
                level = all_of(jnp.max(term, axis=0), jnp.max)
                u_rows[...] = jnp.exp2(term - level[None])
            else:
                u_rows[...] = term
        TPH = max(NT // 2, 1)
        for half in range(NT // TPH):
            def tile(i, carry):
                rows = pl.ds(pl.multiple_of((half * TPH + i) * 128, 128), 128)

                def scaled(r):
                    return zs[r, rows, :] * u_rows[r // NX, r % NX:r % NX + 1, :]
                if early:
                    acc = functools.reduce(jnp.add, [scaled(r) for r in range(HZ * NX, NR)])
                    wacc[rows, :] = acc + wacc[rows, :]
                else:
                    wacc[rows, :] = functools.reduce(jnp.add, [scaled(r) for r in range(NR)])
                return carry

            def tile_wide(i, carry):
                rows = pl.ds(pl.multiple_of((half * TPH + i) * 128, 128), 128)

                def moved(r):
                    return zs[r, rows, :] + u_rows[r // NX, r % NX:r % NX + 1, :]
                top = functools.reduce(jnp.maximum, [moved(r) for r in range(NR)])
                top = jnp.max(top, axis=1, keepdims=True)
                acc = functools.reduce(jnp.add, [jnp.exp2(moved(r) - top) for r in range(NR)])
                wacc[rows, :] = jnp.broadcast_to(top + jnp.log2(jnp.sum(acc, axis=1, keepdims=True)), (128, 128))
                return carry
            lax.fori_loop(0, TPH, tile if fast else tile_wide, 0)
            found = []
            for i in range(half * TPH, (half + 1) * TPH):
                turned = wacc[i * 128:(i + 1) * 128, :].T
                found.append(jnp.sum(turned, axis=0, keepdims=True) if fast else turned[0:1, :])
            found = jnp.concatenate(found, axis=0)
            lines = slice(half * TPH, (half + 1) * TPH)
            if fast:
                bad = bad + low(found)
                found = jnp.log2(found) + level
            c_buf[it, col, lines, :] = found - bias[lines, :]
            to_all(col_peer, NK, c_buf.at[it, col, pl.ds(half * TPH, TPH)], c_sems.at[it])
        if last:
            fo_buf[col] = g_tmp[z, pl.ds(x, 1), :] * (-NATS)
            to_all(col_peer, NK, fo_buf.at[col], fo_sems)
        wait_bytes(c_buf.at[it], NK - 1, c_sems.at[it, 1])
        parts = [c_buf[it, c] for c in range(NK)]
        top = functools.reduce(jnp.maximum, parts)
        mapped = (top + jnp.log2(functools.reduce(jnp.add, [jnp.exp2(v - top) for v in parts]))) * (-NATS)
        images = (images + [mapped])[-HIST:]
        base = (base + [g_now])[-HIST:]
        resid = [p - q for p, q in zip(images, base)]
        prods = [jnp.sum(resid[a] * resid[b], axis=0, keepdims=True) for a, b in pairs]
        prods.append(jnp.where(line == 0, bad, 0.0))
        sums = jnp.sum(jnp.concatenate(prods, axis=0), axis=1, keepdims=True)
        r_buf[it, row] = jnp.sum(jnp.where(eye, sums, 0.0), axis=0, keepdims=True)
        to_all(row_peer, NR, r_buf.at[it, row], r_sems.at[it])
        wait_bytes(r_buf.at[it], NR - 1, r_sems.at[it, 1])
        flat = functools.reduce(jnp.add, [r_buf[it, r] for r in range(NR)])

        def entry(k):
            return jnp.sum(jnp.where(line == k, flat, 0.0), axis=1, keepdims=True)
        mix = solve({ab: entry(k) for k, ab in enumerate(pairs)})
        g_next = functools.reduce(jnp.add, [v * m for v, m in zip(images, mix)])
        if last:
            hist[0] = g_next
            for q in range(TW // 128):
                gout_ref[q:q + 1, :] = hist[0, pl.ds(col * (TW // 128) + q, 1), :]
            flag_ref[...] = jnp.broadcast_to(entry(len(pairs)), (1, 128))
        else:
            delta = (g_next - g_now) * BITS
            if fast:
                shift = all_of(delta, jnp.max)
                delta = jnp.exp2(delta - shift)
            for t in range(NT):
                vrep[t * 128:(t + 1) * 128, :] = jnp.broadcast_to(delta[t:t + 1, :], (128, 128)).T
            g_now = g_next

    wait_bytes(fo_buf, NK - 1, fo_sems.at[1])
    for c in range(NK):
        f_ref[c:c + 1, :] = fo_buf[c]
    wait_bytes(src_all, NR - 1, src_send)
    wait_bytes(tgt_all, NK - 1, tgt_send)
    wait_bytes(fo_buf, NK - 1, fo_sems.at[0])
    wait_bytes(a_all, NR - 1, a_sems.at[0])
    wait_bytes(old_all, NK - 1, old_sems.at[0])
    for it in range(ITERS):
        if it and SPLIT:
            half_sent(f_sems.at[it, 0], pl.ds(0, HZ))
            half_sent(f_sems.at[it + 1, 0], pl.ds(0, HZ))
        else:
            wait_bytes(f_buf.at[it], NR - 1, f_sems.at[it, 0])
        wait_bytes(c_buf.at[it], NK - 1, c_sems.at[it, 0])
        wait_bytes(r_buf.at[it], NR - 1, r_sems.at[it, 0])


def shards(dims, src, tgt, log_a, log_b, g, hist_g, hist_maps):
    NZ, NX, NY, NC = dims
    NR, NK = NZ * NX, NY * NC
    D, SW = src.shape
    TW = tgt.shape[1]
    COLS = NK * TW
    NT = COLS // 128
    f32 = jnp.float32
    vmem = pl.BlockSpec(memory_space=pltpu.VMEM)
    dma = pltpu.SemaphoreType.DMA

    def call(fast):
        return pl.pallas_call(
            functools.partial(kernel, fast, dims),
            out_shape=(
                jax.ShapeDtypeStruct((NK, SW), f32),
                jax.ShapeDtypeStruct((TW // 128, 128), f32),
                jax.ShapeDtypeStruct((1, 128), f32),
            ),
            in_specs=[pl.BlockSpec(memory_space=pltpu.HBM)] * 7,
            out_specs=(vmem,) * 3,
            scratch_shapes=[
                pltpu.VMEM((NR, D, SW), f32),
                pltpu.VMEM((NK, D + 8, TW), f32),
                pltpu.VMEM((NR, 1, SW), f32),
                pltpu.VMEM((NK, 2 * (HIST - 1), TW), f32),
                pltpu.VMEM((NK, SW), f32),
                pltpu.VMEM((1, TW), f32),
                pltpu.VMEM((1, TW), f32),
                pltpu.VMEM((HIST - 1, TW), f32),
                pltpu.VMEM((HIST - 1, TW), f32),
                pltpu.VMEM((COLS, 4 * D), jnp.bfloat16),
                pltpu.VMEM((NR, 4 * D, SW), jnp.bfloat16),
                pltpu.VMEM((COLS, 2 * SW), f32),
                pltpu.VMEM((2, 1, SW), f32),
                pltpu.VMEM((NR, COLS, SW), f32),
                pltpu.VMEM((COLS, 128), f32),
                pltpu.VMEM((COLS, 128), f32),
                pltpu.VMEM((2 * HIST, NT, 128), f32),
                pltpu.VMEM((NZ, NX, SW), f32),
                pltpu.VMEM((NZ, NX, SW), f32),
                pltpu.VMEM((NZ, NX, SW), f32),
                pltpu.VMEM((NZ, NX, SW), f32),
                pltpu.VMEM((ITERS, NR, NZ, NX, SW), f32),
                pltpu.VMEM((NK, 1, SW), f32),
                pltpu.VMEM((ITERS, NK, NT, 128), f32),
                pltpu.VMEM((ITERS, NR, 1, 128), f32),
                dma((7,)), dma((2,)), dma((2,)), dma, dma((2, 2, NR)), dma, dma((2, NK)),
                dma((ITERS + 1, 2)), dma((2,)), dma((ITERS, 2)), dma((ITERS, 2)),
            ],
            compiler_params=pltpu.CompilerParams(
                collective_id=0 if fast else 1, has_side_effects=True,
                vmem_limit_bytes=48 * 1024 * 1024
            ),
            name="sinkhorn" if fast else "sinkhorn_wide",
        )(src, tgt, log_a.reshape(NK, SW), log_b.reshape(NR, 1, TW), g.reshape(1, TW), hist_g, hist_maps)

    f, gout, flag = call(True)
    f, gout = lax.cond(flag[0, 0] > 0.5, lambda: call(False)[:2], lambda: (f, gout))
    return f.reshape(-1), gout.reshape(-1)


def solution(mesh, dims=(4, 4, 4, 2)):
    grid = Mesh(mesh.devices.reshape(dims), AXES)
    in_specs = (
        P(None, AXES),
        P(None, ("y", "core", "z", "x")),
        P(("z", "x")),
        P(("y", "core")),
        P(("y", "core", "z", "x")),
        P(None, ("y", "core", "z", "x")),
        P(None, ("y", "core", "z", "x")),
    )
    out_specs = (P(("z", "x")), P(("y", "core", "z", "x")))
    return jax.shard_map(
        functools.partial(shards, dims), mesh=grid, in_specs=in_specs, out_specs=out_specs, check_vma=False
    )
```

```python
import functools

import jax
import jax.numpy as jnp
from jax import lax
from jax.experimental import pallas as pl
from jax.experimental.pallas import tpu as pltpu
from jax.sharding import Mesh
from jax.sharding import PartitionSpec as P

HIST = 5
ITERS = 2
EPS = 0.1
LOG2E = 1.4426950408889634
BITS = LOG2E / EPS
NATS = EPS / LOG2E
LEAST_BITS = -97.0
SMALLEST = 2.0**LEAST_BITS
MESH = pl.DeviceIdType.MESH
AXES = ("z", "x", "y", "core")


def split2(v):
    hi = v.astype(jnp.bfloat16).astype(jnp.float32)
    return hi, v - hi


def split3(v):
    hi = v.astype(jnp.bfloat16).astype(jnp.float32)
    rest = v - hi
    mid = rest.astype(jnp.bfloat16).astype(jnp.float32)
    return hi, mid, rest - mid


def placed(rows, values, width):
    at = lax.broadcasted_iota(jnp.int32, (rows, width), 0)
    out = jnp.zeros((rows, width), jnp.float32)
    for k, v in enumerate(values):
        out = jnp.where(at == k, v, out)
    return out


def solve(gram):
    n = HIST
    trace = gram[0, 0]
    for k in range(1, n):
        trace = trace + gram[k, k]
    shift = 0.001 * trace / n + 1e-6
    a = [[gram[min(p, q), max(p, q)] + (shift if p == q else 0.0) for q in range(n)] for p in range(n)]
    rhs = [jnp.ones((1, 1), jnp.float32) for _ in range(n)]
    for p in range(n):
        for low in range(p + 1, n):
            factor = a[low][p] / a[p][p]
            for q in range(p + 1, n):
                a[low][q] = a[low][q] - factor * a[p][q]
            rhs[low] = rhs[low] - factor * rhs[p]
    out = [None] * n
    for p in reversed(range(n)):
        acc = rhs[p]
        for q in range(p + 1, n):
            acc = acc - a[p][q] * out[q]
        out[p] = acc / a[p][p]
    total = out[0]
    for k in range(1, n):
        total = total + out[k]
    return [o / total for o in out]


def kernel(
    fast, dims,
    src_hbm, tgt_hbm, loga_hbm, logb_hbm, g_hbm, hg_hbm, hm_hbm,
    f_ref, gout_ref, flag_ref,
    src_all, tgt_all, a_all, old_all, loga_in, logb_in, g_in, hg_in, hm_in,
    left, right, staged, tops_buf, zs, wacc, vrep, hist, m_rows, a_rows, u_rows, g_tmp,
    f_buf, fo_buf, c_buf, r_buf,
    in_sems, a_sems, old_sems, src_send, src_recv, tgt_send, tgt_recv, f_sems, fo_sems, c_sems, r_sems,
):
    NZ, NX, NY, NC = dims
    SIZE = dict(zip(AXES, dims))
    NR, NK = NZ * NX, NY * NC
    D, SW = src_hbm.shape
    TW = tgt_hbm.shape[1]
    COLS = NK * TW
    NT = COLS // 128
    at = {name: lax.axis_index(name) for name in AXES}
    z, x, y, core = (at[name] for name in AXES)
    row, col = z * NX + x, y * NC + core

    def row_peer(k):
        p = lax.rem(row + k, NR)
        return {"z": p // NX, "x": lax.rem(p, NX)}

    def col_peer(k):
        p = lax.rem(col + k, NK)
        return {"y": p // NC, "core": lax.rem(p, NC)}

    def near(axis, d):
        return {axis: lax.rem(at[axis] + d + SIZE[axis], SIZE[axis])}

    def remote(part, ssem, rsem, peer):
        pltpu.make_async_remote_copy(
            src_ref=part, dst_ref=part, send_sem=ssem, recv_sem=rsem, device_id=peer, device_id_type=MESH
        ).start()

    def to_all(peer, count, part, sems):
        for k in range(1, count):
            remote(part, sems.at[0], sems.at[1], peer(k))

    def wait_for(part, sem):
        pltpu.make_async_copy(part, part, sem).wait()

    def wait_bytes(buf, count, sem):
        if count:
            wait_for(buf.at[pl.ds(0, count)], sem)

    barrier = pltpu.get_barrier_semaphore()
    around = [(name, d) for name in ("x", "z", "y") if SIZE[name] > 1 for d in (1, -1)]
    if NC > 1:
        around.append(("core", 1))
    for name, d in around:
        pl.semaphore_signal(barrier, inc=1, device_id=near(name, d), device_id_type=MESH)

    greeted = len(around)
    if NC > 1 and NY > 1:
        for d in (1, -1):
            to = {"y": lax.rem(y + d + NY, NY), "core": lax.rem(core + 1, NC)}
            pl.semaphore_signal(barrier, inc=1, device_id=to, device_id_type=MESH)
        greeted += 2

    moves = [
        (src_hbm, src_all.at[row]), (tgt_hbm, tgt_all.at[col, pl.ds(0, D)]), (loga_hbm, loga_in),
        (logb_hbm.at[row], logb_in), (g_hbm, g_in), (hm_hbm, hm_in), (hg_hbm, hg_in),
    ]
    moves = [pltpu.make_async_copy(s, d, in_sems.at[k]) for k, (s, d) in enumerate(moves)]
    for m in moves:
        m.start()
    for m in moves:
        m.wait()
    KEPT = HIST - 1
    a_all[row] = loga_in[pl.ds(col, 1), :]
    tgt_all[col, D:D + 8, :] = placed(8, [g_in[...], logb_in[...]], TW)
    old_all[col] = jnp.concatenate([hm_in[...], hg_in[...]], axis=0)
    pl.semaphore_wait(barrier, greeted)

    HALF, QUART = D // 2, D // 4
    PIECES = (((0, QUART), (QUART, QUART)), ((HALF, QUART), (HALF + QUART, QUART)))
    ORDER = (("x", "z"), ("z", "x"))
    seen = set()

    def slot_of(dz, dx):
        return lax.rem(z + dz + NZ, NZ) * NX + lax.rem(x + dx + NX, NX)

    def piece(r, h, sub):
        start, count = PIECES[h][sub]
        return src_all.at[r, pl.ds(start, count)]

    def pass_on(r, h, sub, axis, d):
        remote(piece(r, h, sub), src_send, src_recv.at[h, sub, r], near(axis, d))

    def part_for(d):
        return 0 if d < 0 else 1

    def start_sources():
        for phase in (0, 1):
            for first in (True, False):
                for h in (0, 1):
                    axis = ORDER[h][phase]
                    if SIZE[axis] > 1:
                        for d in (1, -1):
                            pass_on(row, h, part_for(-d) if first else part_for(d), axis, d)

    def arrived(h, da, db, sub):
        a, b = ORDER[h]
        if (h, da, db, sub) in seen or (da == 0 and db == 0):
            return
        seen.add((h, da, db, sub))
        r = slot_of(**{"d" + a: da, "d" + b: db})
        wait_for(piece(r, h, sub), src_recv.at[h, sub, r])
        if db == 0:
            if da in (1, -1) and sub == part_for(da):
                pass_on(r, h, sub, a, -da)
            for d in (1, -1):
                pass_on(r, h, sub, b, d)
        elif db in (1, -1) and sub == part_for(db):
            pass_on(r, h, sub, b, -db)

    def complete(*blocks):
        for dz, dx in blocks:
            for h in (0, 1):
                da, db = (dx, dz) if h == 0 else (dz, dx)
                for sub in (0, 1):
                    arrived(h, da, db, sub)

    def target(c, sub):
        return tgt_all.at[c, pl.ds(0, HALF + 8) if sub == 0 else pl.ds(HALF + 8, HALF)]

    def tgt_slot(dy, other=0):
        return lax.rem(y + dy + NY, NY) * NC + lax.rem(core + other, NC)

    def tgt_pass(c, sub, axis, d):
        remote(target(c, sub), tgt_send, tgt_recv.at[sub, c], near(axis, d))

    def start_targets():
        if NY > 1:
            for first in (True, False):
                for d in (1, -1):
                    tgt_pass(col, part_for(-d) if first else part_for(d), "y", d)
        if NC > 1:
            for sub in (0, 1):
                tgt_pass(col, sub, "core", 1)

    def tgt_arrived(dy, sub):
        c = tgt_slot(dy)
        wait_for(target(c, sub), tgt_recv.at[sub, c])
        if dy in (1, -1):
            if sub == part_for(dy):
                if NC > 1:
                    to = {"y": lax.rem(y - dy + NY, NY), "core": lax.rem(core + 1, NC)}
                    remote(target(c, sub), tgt_send, tgt_recv.at[sub, c], to)
                tgt_pass(c, sub, "y", -dy)
            if NC > 1:
                tgt_pass(c, sub, "core", 1)

    def take_targets(c):
        v = tgt_all[c, 0:D, :]
        norm = jnp.sum(v * v, axis=0, keepdims=True) * (-BITS)
        b = tgt_all[c, D:D + 1, :] * BITS + tgt_all[c, D + 1:D + 2, :] * LOG2E
        hi, lo = split2(v)
        one = jnp.ones((1, TW), jnp.float32)
        tail = placed(D, list(split3(norm)) + list(split3(b)) + [one] * 3, TW)
        full = jnp.concatenate([hi, lo, hi, tail], axis=0)
        left[pl.ds(pl.multiple_of(c * TW, TW), TW), :] = full.T.astype(jnp.bfloat16)

    def take_sources(r):
        v = src_all[r]
        norm = jnp.sum(v * v, axis=0, keepdims=True) * (-BITS)
        hi, lo = split2(v * (2.0 * BITS))
        one = jnp.ones((1, SW), jnp.float32)
        tail = placed(D, [one] * 6 + list(split3(norm)), SW)
        right[r] = jnp.concatenate([hi, hi, lo, tail], axis=0).astype(jnp.bfloat16)

    QB = min(256, COLS)
    EB = min(256, COLS)

    def spots_of(offsets):
        return [(lax.rem(z + dz + 8 * NZ, NZ), lax.rem(x + dx + 8 * NX, NX)) for dz, dx in offsets]

    def folded(v, op):
        return op(v.reshape(v.shape[0] // 8, 8, v.shape[1]), axis=0)

    def step(done, new):
        if new:
            operand = jnp.concatenate([right[zb * NX + xb] for zb, xb in new], axis=1)
        tops, sums = [None] * len(new), [None] * len(done)
        before = [tops_buf[n] for n in range(len(done))]
        for q in range(COLS // QB):
            rows = slice(q * QB, (q + 1) * QB)
            for n, (zb, xb) in enumerate(done):
                e = jnp.exp2(staged[rows, n * SW:(n + 1) * SW] - before[n])
                if fast:
                    zs[zb * NX + xb, rows, :] = e
                else:
                    zs[zb * NX + xb, rows, :] = staged[rows, n * SW:(n + 1) * SW]
                e = folded(e, jnp.sum)
                sums[n] = e if q == 0 else sums[n] + e
            if new:
                t = jnp.dot(left[rows, :], operand, preferred_element_type=jnp.float32)
                staged[rows, 0:len(new) * SW] = t
                for n in range(len(new)):
                    top = folded(t[:, n * SW:(n + 1) * SW], jnp.max)
                    tops[n] = top if q == 0 else jnp.maximum(tops[n], top)
        for n, (zb, xb) in enumerate(done):
            f_buf[0, row, zb, pl.ds(xb, 1), :] = before[n] + jnp.log2(jnp.sum(sums[n], axis=0, keepdims=True))
            m_rows[zb, pl.ds(xb, 1), :] = before[n]
        for n in range(len(new)):
            tops_buf[n] = jnp.max(tops[n], axis=0, keepdims=True)

    TURNS = (
        ((0, 1), (0, -1)), ((1, 0), (-1, 0)), ((1, 1), (-1, 1)), ((1, -1), (-1, -1)), ((0, 0), (0, 2)),
        ((1, 2), (-1, 2)), ((2, 1), (2, -1)), ((2, 0), (2, 2)),
    ) if NZ > 1 and NX > 1 else (((0, 0),),)

    def turn(k):
        out = TURNS[0]
        for t in range(1, len(TURNS)):
            out = tuple(tuple(jnp.where(k == t, v, w) for v, w in zip(*pair)) for pair in zip(TURNS[t], out))
        return spots_of(out)

    def ready(*turns):
        for t in turns:
            complete(*TURNS[t])
            for zb, xb in spots_of(TURNS[t]):
                take_sources(zb * NX + xb)

    SPLIT = fast and NZ > 1

    def send_f(it, zb):
        late = it if it and SPLIT and zb < NZ // 2 else 0
        to_all(row_peer, NR, f_buf.at[it, row, zb], f_sems.at[it + late])

    both = NZ > 1 and NX > 1
    start_sources()
    start_targets()
    take_targets(col)
    if both:
        for h in (0, 1):
            for d in (1, -1):
                arrived(h, d, 0, part_for(d))
        for h in (0, 1):
            for d in (1, -1):
                arrived(h, d, 0, part_for(-d))
    if NY > 1:
        for d in (1, -1):
            tgt_arrived(d, part_for(d))
        for d in (1, -1):
            tgt_arrived(d, part_for(-d))
    if both:
        for h in (0, 1):
            for d in (1, -1):
                arrived(h, 0, d, part_for(d))
    if both:
        for h in (0, 1):
            for sub in (0, 1):
                arrived(h, 2, 0, sub)
            for da in (1, -1):
                for db in (1, -1):
                    arrived(h, da, db, part_for(db))
        ready(0, 1, 2, 3)
    else:
        ready(0)
    if NY > 1:
        for sub in (0, 1):
            tgt_arrived(2, sub)
        for dy in (1, -1, 2):
            take_targets(tgt_slot(dy))
    if NC > 1:
        for dy in ((0, 1, -1, 2) if NY > 1 else (0,)):
            c = tgt_slot(dy, 1)
            for sub in (0, 1):
                wait_for(target(c, sub), tgt_recv.at[sub, c])
            take_targets(c)
    if both:
        complete((0, 1), (0, -1), (1, 0), (-1, 0))
    if both:
        def stage(k, carry):
            @pl.when(k == 2)
            def _():
                for h in (0, 1):
                    for db in (1, -1):
                        arrived(h, 2, db, part_for(db))
            for t in range(4, len(TURNS)):
                @pl.when(k == t)
                def _(t=t):
                    ready(t)
            step(turn(jnp.maximum(k - 1, 0)), turn(k))

            @pl.when(k == 5)
            def _():
                send_f(0, z)

            @pl.when(k == 6)
            def _():
                for d in (1, 3):
                    send_f(0, lax.rem(z + d, NZ))
            return carry
        lax.fori_loop(0, len(TURNS) + 1, stage, 0)
    else:
        step([], spots_of(TURNS[0]))
        step(spots_of(TURNS[0]), [])
    send_f(0, lax.rem(z + NZ // 2, NZ))
    to_all(row_peer, NR, a_all.at[row], a_sems)
    to_all(col_peer, NK, old_all.at[col], old_sems)
    wait_bytes(a_all, NR - 1, a_sems.at[1])
    wait_bytes(old_all, NK - 1, old_sems.at[1])
    for r in range(NR):
        a_rows[r // NX, r % NX:r % NX + 1, :] = a_all[r] * LOG2E
    for c in range(NK):
        for q in range(TW // 128):
            t, lanes = c * (TW // 128) + q, slice(q * 128, (q + 1) * 128)
            for k in range(2):
                hist[k, t:t + 1, :] = tgt_all[c, D + k:D + k + 1, lanes]
            for k in range(2 * KEPT):
                hist[2 + k, t:t + 1, :] = old_all[c, k:k + 1, lanes]

    bad = jnp.zeros((1, 1), jnp.float32)
    g_now = hist[0]
    bias = g_now * BITS + hist[1] * LOG2E
    images = [hist[2 + k] for k in range(KEPT)]
    base = [hist[2 + KEPT + k] for k in range(KEPT)]
    shift = jnp.zeros((1, 1), jnp.float32)
    pairs = [(a, b) for a in range(HIST) for b in range(a, HIST)]
    line = lax.broadcasted_iota(jnp.int32, (1, 128), 1)
    eye = (lax.broadcasted_iota(jnp.int32, (16, 128), 0) == lax.broadcasted_iota(jnp.int32, (16, 128), 1))

    def all_of(v, op):
        return op(op(v, axis=0, keepdims=True), axis=1, keepdims=True)

    def low(v):
        return all_of(jnp.where(v >= SMALLEST, 0.0, 1.0), jnp.max)

    for it in range(ITERS):
        last = it == ITERS - 1
        if it and fast:
            GZ = min(2, NZ)
            SB = min(256, COLS)
            for zg in range(0, NZ, GZ):
                spots = [(zz, xx) for zz in range(zg, zg + GZ) for xx in range(NX)]

                def weigh(i, acc):
                    rows = pl.ds(pl.multiple_of(i * SB, SB), SB)
                    v = vrep[rows, :]
                    return tuple(
                        a + jnp.sum((zs[zz * NX + xx, rows, :] * v).reshape(SB // 8, 8, SW), axis=0)
                        for a, (zz, xx) in zip(acc, spots)
                    )
                found = lax.fori_loop(0, COLS // SB, weigh, tuple(jnp.zeros((8, SW), jnp.float32) for _ in spots))
                found = [jnp.sum(v, axis=0, keepdims=True) for v in found]
                for zz in range(zg, zg + GZ):
                    s = jnp.concatenate(found[(zz - zg) * NX:(zz - zg + 1) * NX], axis=0)
                    bad = bad + low(s)
                    f_buf[it, row, zz] = m_rows[zz] + shift + jnp.log2(s)
                for zz in range(zg, zg + GZ):
                    send_f(it, zz)
        elif it:
            def again(r, carry):
                def tops_of(i, acc):
                    rows = pl.ds(pl.multiple_of(i * EB, EB), EB)
                    v = zs[r, rows, :] + vrep[rows, :]
                    return jnp.maximum(acc, jnp.max(v.reshape(EB // 8, 8, SW), axis=0))
                top = lax.fori_loop(0, COLS // EB, tops_of, jnp.full((8, SW), -jnp.inf, jnp.float32))
                top = jnp.max(top, axis=0, keepdims=True)

                def sums_of(i, acc):
                    rows = pl.ds(pl.multiple_of(i * EB, EB), EB)
                    v = jnp.exp2((zs[r, rows, :] + vrep[rows, :]) - top)
                    return acc + jnp.sum(v.reshape(EB // 8, 8, SW), axis=0)
                s = lax.fori_loop(0, COLS // EB, sums_of, jnp.zeros((8, SW), jnp.float32))
                f_buf[it, row, r // NX, pl.ds(lax.rem(r, NX), 1), :] = top + jnp.log2(
                    jnp.sum(s, axis=0, keepdims=True))
                return carry
            lax.fori_loop(0, NR, again, 0)
            for zz in range(NZ):
                send_f(it, zz)
        level = jnp.zeros((1, 1), jnp.float32)
        early = it > 0 and SPLIT
        HZ = NZ // 2

        def joined(lines):
            parts = [f_buf[it, r, lines] for r in range(NR)]
            top = functools.reduce(jnp.maximum, parts)
            return top + jnp.log2(functools.reduce(jnp.add, [jnp.exp2(v - top) for v in parts]))

        def half_sent(sem, lines):
            wait_for(f_buf.at[it, pl.ds(0, NR - 1), lines], sem)

        if early:
            half_sent(f_sems.at[it + 1, 1], pl.ds(0, HZ))
            whole = joined(slice(0, HZ))
            g_tmp[0:HZ] = whole
            term = a_rows[0:HZ] - whole + m_rows[0:HZ]
            level = all_of(jnp.max(term, axis=0), jnp.max)
            u_rows[0:HZ] = jnp.exp2(term - level[None])

            def first_half(i, carry):
                rows = pl.ds(pl.multiple_of(i * 128, 128), 128)
                wacc[rows, :] = functools.reduce(jnp.add, [
                    zs[r, rows, :] * u_rows[r // NX, r % NX:r % NX + 1, :] for r in range(HZ * NX)
                ])
                return carry
            lax.fori_loop(0, NT, first_half, 0)
            half_sent(f_sems.at[it, 1], pl.ds(0, HZ))
            whole = joined(slice(HZ, NZ))
            g_tmp[HZ:NZ] = whole
            term = a_rows[HZ:NZ] - whole + m_rows[HZ:NZ] - level[None]
            bad = bad + all_of(jnp.max(jnp.where(term <= 60.0, 0.0, 1.0), axis=0), jnp.max)
            u_rows[HZ:NZ] = jnp.exp2(term)
        else:
            wait_bytes(f_buf.at[it], NR - 1, f_sems.at[it, 1])
            whole = joined(slice(0, NZ))
            g_tmp[...] = whole
            term = a_rows[...] - whole
            if fast:
                term = term + m_rows[...]
                level = all_of(jnp.max(term, axis=0), jnp.max)
                u_rows[...] = jnp.exp2(term - level[None])
            else:
                u_rows[...] = term
        TPH = max(NT // 2, 1)
        for half in range(NT // TPH):
            def tile(i, carry):
                rows = pl.ds(pl.multiple_of((half * TPH + i) * 128, 128), 128)

                def scaled(r):
                    return zs[r, rows, :] * u_rows[r // NX, r % NX:r % NX + 1, :]
                if early:
                    acc = functools.reduce(jnp.add, [scaled(r) for r in range(HZ * NX, NR)])
                    wacc[rows, :] = acc + wacc[rows, :]
                else:
                    wacc[rows, :] = functools.reduce(jnp.add, [scaled(r) for r in range(NR)])
                return carry

            def tile_wide(i, carry):
                rows = pl.ds(pl.multiple_of((half * TPH + i) * 128, 128), 128)

                def moved(r):
                    return zs[r, rows, :] + u_rows[r // NX, r % NX:r % NX + 1, :]
                top = functools.reduce(jnp.maximum, [moved(r) for r in range(NR)])
                top = jnp.max(top, axis=1, keepdims=True)
                acc = functools.reduce(jnp.add, [jnp.exp2(moved(r) - top) for r in range(NR)])
                wacc[rows, :] = jnp.broadcast_to(top + jnp.log2(jnp.sum(acc, axis=1, keepdims=True)), (128, 128))
                return carry
            lax.fori_loop(0, TPH, tile if fast else tile_wide, 0)
            found = []
            for i in range(half * TPH, (half + 1) * TPH):
                turned = wacc[i * 128:(i + 1) * 128, :].T
                found.append(jnp.sum(turned, axis=0, keepdims=True) if fast else turned[0:1, :])
            found = jnp.concatenate(found, axis=0)
            lines = slice(half * TPH, (half + 1) * TPH)
            if fast:
                bad = bad + low(found)
                found = jnp.log2(found) + level
            c_buf[it, col, lines, :] = found - bias[lines, :]
            to_all(col_peer, NK, c_buf.at[it, col, pl.ds(half * TPH, TPH)], c_sems.at[it])
        if last:
            fo_buf[col] = g_tmp[z, pl.ds(x, 1), :] * (-NATS)
            to_all(col_peer, NK, fo_buf.at[col], fo_sems)
        wait_bytes(c_buf.at[it], NK - 1, c_sems.at[it, 1])
        parts = [c_buf[it, c] for c in range(NK)]
        top = functools.reduce(jnp.maximum, parts)
        mapped = (top + jnp.log2(functools.reduce(jnp.add, [jnp.exp2(v - top) for v in parts]))) * (-NATS)
        images = (images + [mapped])[-HIST:]
        base = (base + [g_now])[-HIST:]
        resid = [p - q for p, q in zip(images, base)]
        prods = [jnp.sum(resid[a] * resid[b], axis=0, keepdims=True) for a, b in pairs]
        prods.append(jnp.where(line == 0, bad, 0.0))
        sums = jnp.sum(jnp.concatenate(prods, axis=0), axis=1, keepdims=True)
        r_buf[it, row] = jnp.sum(jnp.where(eye, sums, 0.0), axis=0, keepdims=True)
        to_all(row_peer, NR, r_buf.at[it, row], r_sems.at[it])
        wait_bytes(r_buf.at[it], NR - 1, r_sems.at[it, 1])
        flat = functools.reduce(jnp.add, [r_buf[it, r] for r in range(NR)])

        def entry(k):
            return jnp.sum(jnp.where(line == k, flat, 0.0), axis=1, keepdims=True)
        mix = solve({ab: entry(k) for k, ab in enumerate(pairs)})
        g_next = functools.reduce(jnp.add, [v * m for v, m in zip(images, mix)])
        if last:
            hist[0] = g_next
            for q in range(TW // 128):
                gout_ref[q:q + 1, :] = hist[0, pl.ds(col * (TW // 128) + q, 1), :]
            flag_ref[...] = jnp.broadcast_to(entry(len(pairs)), (1, 128))
        else:
            delta = (g_next - g_now) * BITS
            if fast:
                shift = all_of(delta, jnp.max)
                delta = jnp.exp2(delta - shift)
            for t in range(NT):
                vrep[t * 128:(t + 1) * 128, :] = jnp.broadcast_to(delta[t:t + 1, :], (128, 128)).T
            g_now = g_next

    wait_bytes(fo_buf, NK - 1, fo_sems.at[1])
    for c in range(NK):
        f_ref[c:c + 1, :] = fo_buf[c]
    wait_bytes(src_all, NR - 1, src_send)
    wait_bytes(tgt_all, NK - 1, tgt_send)
    wait_bytes(fo_buf, NK - 1, fo_sems.at[0])
    wait_bytes(a_all, NR - 1, a_sems.at[0])
    wait_bytes(old_all, NK - 1, old_sems.at[0])
    for it in range(ITERS):
        if it and SPLIT:
            half_sent(f_sems.at[it, 0], pl.ds(0, HZ))
            half_sent(f_sems.at[it + 1, 0], pl.ds(0, HZ))
        else:
            wait_bytes(f_buf.at[it], NR - 1, f_sems.at[it, 0])
        wait_bytes(c_buf.at[it], NK - 1, c_sems.at[it, 0])
        wait_bytes(r_buf.at[it], NR - 1, r_sems.at[it, 0])


def shards(dims, src, tgt, log_a, log_b, g, hist_g, hist_maps):
    NZ, NX, NY, NC = dims
    NR, NK = NZ * NX, NY * NC
    D, SW = src.shape
    TW = tgt.shape[1]
    COLS = NK * TW
    NT = COLS // 128
    f32 = jnp.float32
    vmem = pl.BlockSpec(memory_space=pltpu.VMEM)
    dma = pltpu.SemaphoreType.DMA

    def call(fast):
        return pl.pallas_call(
            functools.partial(kernel, fast, dims),
            out_shape=(
                jax.ShapeDtypeStruct((NK, SW), f32),
                jax.ShapeDtypeStruct((TW // 128, 128), f32),
                jax.ShapeDtypeStruct((1, 128), f32),
            ),
            in_specs=[pl.BlockSpec(memory_space=pltpu.HBM)] * 7,
            out_specs=(vmem,) * 3,
            scratch_shapes=[
                pltpu.VMEM((NR, D, SW), f32),
                pltpu.VMEM((NK, D + 8, TW), f32),
                pltpu.VMEM((NR, 1, SW), f32),
                pltpu.VMEM((NK, 2 * (HIST - 1), TW), f32),
                pltpu.VMEM((NK, SW), f32),
                pltpu.VMEM((1, TW), f32),
                pltpu.VMEM((1, TW), f32),
                pltpu.VMEM((HIST - 1, TW), f32),
                pltpu.VMEM((HIST - 1, TW), f32),
                pltpu.VMEM((COLS, 4 * D), jnp.bfloat16),
                pltpu.VMEM((NR, 4 * D, SW), jnp.bfloat16),
                pltpu.VMEM((COLS, 2 * SW), f32),
                pltpu.VMEM((2, 1, SW), f32),
                pltpu.VMEM((NR, COLS, SW), f32),
                pltpu.VMEM((COLS, 128), f32),
                pltpu.VMEM((COLS, 128), f32),
                pltpu.VMEM((2 * HIST, NT, 128), f32),
                pltpu.VMEM((NZ, NX, SW), f32),
                pltpu.VMEM((NZ, NX, SW), f32),
                pltpu.VMEM((NZ, NX, SW), f32),
                pltpu.VMEM((NZ, NX, SW), f32),
                pltpu.VMEM((ITERS, NR, NZ, NX, SW), f32),
                pltpu.VMEM((NK, 1, SW), f32),
                pltpu.VMEM((ITERS, NK, NT, 128), f32),
                pltpu.VMEM((ITERS, NR, 1, 128), f32),
                dma((7,)), dma((2,)), dma((2,)), dma, dma((2, 2, NR)), dma, dma((2, NK)),
                dma((ITERS + 1, 2)), dma((2,)), dma((ITERS, 2)), dma((ITERS, 2)),
            ],
            compiler_params=pltpu.CompilerParams(
                collective_id=0 if fast else 1, has_side_effects=True,
                vmem_limit_bytes=48 * 1024 * 1024
            ),
            name="sinkhorn" if fast else "sinkhorn_wide",
        )(src, tgt, log_a.reshape(NK, SW), log_b.reshape(NR, 1, TW), g.reshape(1, TW), hist_g, hist_maps)

    f, gout, flag = call(True)
    f, gout = lax.cond(flag[0, 0] > 0.5, lambda: call(False)[:2], lambda: (f, gout))
    return f.reshape(-1), gout.reshape(-1)


def solution(mesh, dims=(4, 4, 4, 2)):
    grid = Mesh(mesh.devices.reshape(dims), AXES)
    in_specs = (
        P(None, AXES),
        P(None, ("y", "core", "z", "x")),
        P(("z", "x")),
        P(("y", "core")),
        P(("y", "core", "z", "x")),
        P(None, ("y", "core", "z", "x")),
        P(None, ("y", "core", "z", "x")),
    )
    out_specs = (P(("z", "x")), P(("y", "core", "z", "x")))
    return jax.shard_map(
        functools.partial(shards, dims), mesh=grid, in_specs=in_specs, out_specs=out_specs, check_vma=False
    )
```
